32 devices in a mesh: data: 4 (over y, z), dap: 8 (over x, core).
Axes of the slice: x: 4, y: 2, z: 2, core: 2. Of those that a mesh axis runs over, the one named last changes fastest.
The devices are a block of a 4x4x8 slice.
Arguments:
- msa_act: bfloat16 [3072, 128, 64], P(('data', 'dap')), parts along dimension 0
- pair_act: bfloat16 [512, 128, 128], P(('data', 'dap')), parts along dimension 0
- msa_mask: int32 [3072, 128], P('data'), parts along dimension 0
- res_mask: int32 [512], P('data'), parts along dimension 0
- row_bias_w: bfloat16 [128, 8], replicated
- row_qkvg_w: bfloat16 [64, 4, 8, 8], replicated
- row_out_w: bfloat16 [8, 8, 64], replicated
- col_query_w: bfloat16 [64, 8, 8], replicated
- col_kv_w: bfloat16 [64, 2, 8], replicated
- col_gate_w: bfloat16 [64, 8, 8], replicated
- col_out_w: bfloat16 [8, 8, 64], replicated
- opm_proj_w: bfloat16 [64, 2, 32], replicated
- opm_out_w: bfloat16 [32, 32, 128], replicated
- start_bias_w: bfloat16 [128, 4], replicated
- start_qkvg_w: bfloat16 [128, 4, 4, 32], replicated
- start_out_w: bfloat16 [4, 32, 128], replicated
- end_bias_w: bfloat16 [128, 4], replicated
- end_qkvg_w: bfloat16 [128, 4, 4, 32], replicated
- end_out_w: bfloat16 [4, 32, 128], replicated
Outputs:
- output 1: bfloat16 [3072, 128, 64], P(('data', 'dap')), parts along dimension 0
- output 2: bfloat16 [512, 128, 128], P(('data', 'dap')), parts along dimension 0
There are 4 independent parts. The reference program is written for one: setup_inputs(seed, part) draws one part's arguments, and reference() takes and returns one part's arrays. A program takes and returns all parts, laid end to end along the dimension named above; an argument that names none is the same for every part.
All inputs are finite; a program needn't handle non-finite values.
Results may differ from the reference program's by a relative error of at most 0.0142.
Values are sent between devices in bfloat16 or wider.
A program may use at most 768 MiB of HBM per device.

```python
import jax
import jax.numpy as jnp
from jax import lax

NUM_SEQ = 768
NUM_RES = 128
MSA_DIM = 64
PAIR_DIM = 128
MSA_HEADS = 8
MSA_HEAD_DIM = 8
TRI_HEADS = 4
TRI_HEAD_DIM = 32
OPM_DIM = 32


def draw_weight(rng_key, arr_shape, fan_in, gain_val):
    return (jax.random.normal(rng_key, arr_shape, jnp.float32) * (gain_val * fan_in ** -0.5)).astype(jnp.bfloat16)


def setup_inputs(seed: int = 0, part: int = 0) -> dict:
    part_key = jax.random.fold_in(jax.random.key(seed), part)
    part_keys = jax.random.split(part_key, 6)
    common = jax.random.normal(part_keys[0], (NUM_RES, MSA_DIM), jnp.float32)
    seq_noise = jax.random.normal(part_keys[1], (NUM_SEQ, NUM_RES, MSA_DIM), jnp.float32)
    msa_act = (0.8 * common[None] + 0.6 * seq_noise).astype(jnp.bfloat16)
    pair_act = jax.random.normal(part_keys[2], (NUM_RES, NUM_RES, PAIR_DIM), jnp.float32).astype(jnp.bfloat16)
    msa_mask = (jax.random.randint(part_keys[3], (NUM_SEQ, NUM_RES), 0, 5) != 0).astype(jnp.int32)
    res_mask = (jax.random.randint(part_keys[4], (NUM_RES,), 0, 4) != 0).astype(jnp.int32)
    weight_keys = jax.random.split(jax.random.key(seed + 1), 15)
    msa_width = MSA_HEADS * MSA_HEAD_DIM
    tri_width = TRI_HEADS * TRI_HEAD_DIM
    return {
        'msa_act': msa_act,
        'pair_act': pair_act,
        'msa_mask': msa_mask,
        'res_mask': res_mask,
        'row_bias_w': draw_weight(weight_keys[0], (PAIR_DIM, MSA_HEADS), PAIR_DIM, 1.5),
        'row_qkvg_w': draw_weight(weight_keys[1], (MSA_DIM, 4, MSA_HEADS, MSA_HEAD_DIM), MSA_DIM, 1.25),
        'row_out_w': draw_weight(weight_keys[2], (MSA_HEADS, MSA_HEAD_DIM, MSA_DIM), msa_width, 1.0),
        'col_query_w': draw_weight(weight_keys[3], (MSA_DIM, MSA_HEADS, MSA_HEAD_DIM), MSA_DIM, 2.0),
        'col_kv_w': draw_weight(weight_keys[4], (MSA_DIM, 2, MSA_HEAD_DIM), MSA_DIM, 1.25),
        'col_gate_w': draw_weight(weight_keys[5], (MSA_DIM, MSA_HEADS, MSA_HEAD_DIM), MSA_DIM, 1.0),
        'col_out_w': draw_weight(weight_keys[6], (MSA_HEADS, MSA_HEAD_DIM, MSA_DIM), msa_width, 1.0),
        'opm_proj_w': draw_weight(weight_keys[7], (MSA_DIM, 2, OPM_DIM), MSA_DIM, 1.0),
        'opm_out_w': draw_weight(weight_keys[8], (OPM_DIM, OPM_DIM, PAIR_DIM), OPM_DIM * OPM_DIM, 0.5),
        'start_bias_w': draw_weight(weight_keys[9], (PAIR_DIM, TRI_HEADS), PAIR_DIM, 1.5),
        'start_qkvg_w': draw_weight(weight_keys[10], (PAIR_DIM, 4, TRI_HEADS, TRI_HEAD_DIM), PAIR_DIM, 1.25),
        'start_out_w': draw_weight(weight_keys[11], (TRI_HEADS, TRI_HEAD_DIM, PAIR_DIM), tri_width, 1.0),
        'end_bias_w': draw_weight(weight_keys[12], (PAIR_DIM, TRI_HEADS), PAIR_DIM, 1.5),
        'end_qkvg_w': draw_weight(weight_keys[13], (PAIR_DIM, 4, TRI_HEADS, TRI_HEAD_DIM), PAIR_DIM, 1.25),
        'end_out_w': draw_weight(weight_keys[14], (TRI_HEADS, TRI_HEAD_DIM, PAIR_DIM), tri_width, 1.0),
    }


def layer_norm(values):
    widened = values.astype(jnp.float32)
    mean_val = jnp.mean(widened, axis=-1, keepdims=True)
    centered = widened - mean_val
    variance = jnp.mean(centered * centered, axis=-1, keepdims=True)
    return (centered * lax.rsqrt(variance + 1e-5)).astype(jnp.bfloat16)


def project(einsum_form, activations, weight):
    return jnp.einsum(einsum_form, activations.astype(jnp.float32), weight.astype(jnp.float32)).astype(jnp.bfloat16)


def mask_bias(mask_vals):
    return (mask_vals.astype(jnp.float32) - 1.0) * 1e4


def gated_out(einsum_form, gate_proj, attended, out_w):
    gated_vals = (jax.nn.sigmoid(gate_proj.astype(jnp.float32)) * attended).astype(jnp.bfloat16)
    return jnp.einsum(einsum_form, gated_vals.astype(jnp.float32), out_w.astype(jnp.float32))


def row_attention(msa_act, pair_act, msa_mask, row_bias_w, row_qkvg_w, row_out_w):
    pair_bias = project('ijc,ch->hij', layer_norm(pair_act), row_bias_w).astype(jnp.float32)
    logit_scale = MSA_HEAD_DIM ** -0.5

    def one_seq(seq_inputs):
        seq_ln, seq_mask = seq_inputs
        projected = project('ic,cahd->aihd', seq_ln, row_qkvg_w)
        logits = jnp.einsum('ihd,jhd->hij', projected[0].astype(jnp.float32), projected[1].astype(jnp.float32)) * logit_scale + pair_bias + mask_bias(seq_mask)[None, None, :]
        attn_probs = jax.nn.softmax(logits, axis=-1).astype(jnp.bfloat16)
        attended = jnp.einsum('hij,jhd->ihd', attn_probs.astype(jnp.float32), projected[2].astype(jnp.float32))
        return gated_out('ihd,hdc->ic', projected[3], attended, row_out_w)

    updates = lax.map(one_seq, (layer_norm(msa_act), msa_mask))
    return (msa_act.astype(jnp.float32) + updates).astype(jnp.bfloat16)


def column_attention(msa_act, msa_mask, col_query_w, col_kv_w, col_gate_w, col_out_w):
    msa_ln = layer_norm(msa_act)
    mask_f = msa_mask.astype(jnp.float32)
    mask_count = jnp.sum(mask_f, axis=0) + 1e-10
    mean_query = (jnp.einsum('sr,src->rc', mask_f, msa_ln.astype(jnp.float32)) / mask_count[:, None]).astype(jnp.bfloat16)
    query_proj = project('rc,chd->rhd', mean_query, col_query_w)
    key_val = project('src,cad->asrd', msa_ln, col_kv_w)
    gate_proj = project('src,chd->srhd', msa_ln, col_gate_w)
    logits = jnp.einsum('rhd,srd->rhs', query_proj.astype(jnp.float32), key_val[0].astype(jnp.float32)) * (MSA_HEAD_DIM ** -0.5) + mask_bias(msa_mask).T[:, None, :]
    attn_probs = jax.nn.softmax(logits, axis=-1).astype(jnp.bfloat16)
    attended = jnp.einsum('rhs,srd->rhd', attn_probs.astype(jnp.float32), key_val[1].astype(jnp.float32))
    update = gated_out('srhd,hdc->src', gate_proj, attended[None], col_out_w)
    return (msa_act.astype(jnp.float32) + update).astype(jnp.bfloat16)


def outer_product_mean(msa_act, pair_act, msa_mask, opm_proj_w, opm_out_w):
    mask_f = msa_mask.astype(jnp.float32)
    projected = project('src,cae->asre', layer_norm(msa_act), opm_proj_w) * msa_mask.astype(jnp.bfloat16)[None, :, :, None]
    counts = jnp.einsum('si,sj->ij', mask_f, mask_f)
    right_proj = projected[1].astype(jnp.float32)
    out_f = opm_out_w.astype(jnp.float32)

    def one_row(row_inputs):
        left_row, count_row = row_inputs
        outer_sum = jnp.einsum('se,sjf->jef', left_row.astype(jnp.float32), right_proj).astype(jnp.bfloat16)
        return jnp.einsum('jef,efc->jc', outer_sum.astype(jnp.float32), out_f) / (1e-3 + count_row)[:, None]

    updates = lax.map(one_row, (jnp.swapaxes(projected[0], 0, 1), counts))
    return (pair_act.astype(jnp.float32) + updates).astype(jnp.bfloat16)


def triangle_start(pair_act, res_mask, bias_w, qkvg_w, out_w):
    pair_ln = layer_norm(pair_act)
    tri_bias = project('jkc,ch->hjk', pair_ln, bias_w).astype(jnp.float32)
    key_bias = mask_bias(res_mask)[None, None, :]
    logit_scale = TRI_HEAD_DIM ** -0.5

    def one_row(row_ln):
        projected = project('jc,cahd->ajhd', row_ln, qkvg_w)
        logits = jnp.einsum('jhd,khd->hjk', projected[0].astype(jnp.float32), projected[1].astype(jnp.float32)) * logit_scale + tri_bias + key_bias
        attn_probs = jax.nn.softmax(logits, axis=-1).astype(jnp.bfloat16)
        attended = jnp.einsum('hjk,khd->jhd', attn_probs.astype(jnp.float32), projected[2].astype(jnp.float32))
        return gated_out('jhd,hdc->jc', projected[3], attended, out_w)

    updates = lax.map(one_row, pair_ln)
    return (pair_act.astype(jnp.float32) + updates).astype(jnp.bfloat16)


def reference(msa_act, pair_act, msa_mask, res_mask, row_bias_w, row_qkvg_w, row_out_w, col_query_w, col_kv_w, col_gate_w, col_out_w, opm_proj_w, opm_out_w, start_bias_w, start_qkvg_w, start_out_w, end_bias_w, end_qkvg_w, end_out_w):
    msa_act = row_attention(msa_act, pair_act, msa_mask, row_bias_w, row_qkvg_w, row_out_w)
    msa_act = column_attention(msa_act, msa_mask, col_query_w, col_kv_w, col_gate_w, col_out_w)
    pair_act = outer_product_mean(msa_act, pair_act, msa_mask, opm_proj_w, opm_out_w)
    pair_act = triangle_start(pair_act, res_mask, start_bias_w, start_qkvg_w, start_out_w)
    pair_act = jnp.swapaxes(triangle_start(jnp.swapaxes(pair_act, 0, 1), res_mask, end_bias_w, end_qkvg_w, end_out_w), 0, 1)
    return (msa_act, pair_act)
```

```python
import functools
import math

import jax
import jax.numpy as jnp
import numpy as np
from jax import lax
from jax.experimental import pallas as pl
from jax.experimental.pallas import tpu as pltpu
from jax.sharding import PartitionSpec as P

BF = jnp.bfloat16
F32 = jnp.float32
MESH = pl.DeviceIdType.MESH
LOG2E = math.log2(math.e)
VM = pl.BlockSpec(memory_space=pltpu.VMEM)


def dot(a, b):
    return lax.dot_general(a, b, (((1,), (0,)), ((), ())), preferred_element_type=F32)


def dot_nt(a, b):
    return lax.dot_general(a, b, (((1,), (1,)), ((), ())), preferred_element_type=F32)


def rnd(v):
    return v.astype(BF).astype(F32)


def norm(v, axis):
    mean = jnp.mean(v, axis=axis, keepdims=True)
    cen = v - mean
    var = jnp.mean(cen * cen, axis=axis, keepdims=True)
    return (cen * lax.rsqrt(var + 1e-5)).astype(BF)


def sigmoid(v):
    return 1.0 / (1.0 + jnp.exp(-v))


def split3(value):
    hi = float(np.asarray(value).astype(BF))
    mid = float(np.asarray(value - hi).astype(BF))
    return hi, mid, float(np.asarray(value - hi - mid).astype(BF))


def peer_barrier(me, n):
    sem = pltpu.get_barrier_semaphore()
    for d in range(1, n):
        pl.semaphore_signal(sem, inc=1, device_id={"dap": lax.rem(me + d, n)}, device_id_type=MESH)
    pl.semaphore_wait(sem, n - 1)


def rcopy(src, dst, ssem, rsem, dev):
    return pltpu.make_async_remote_copy(src_ref=src, dst_ref=dst, send_sem=ssem, recv_sem=rsem, device_id={"dap": dev}, device_id_type=MESH)


def ds8(start, size, unit=8):
    return pl.ds(pl.multiple_of(start, unit), size)


def msa_kernel(n, mask_ref, m_ref, z_ref, wb_ref, wqkvg_ref, wo_ref, wq2_ref, wkv_ref,
               m1_ref, x2_ref, o2_ref,
               ball, bias, brow, kv, lg, wot, qpart, ppart, tmp,
               ssem_b, rsem_b, ssem_q, rsem_q, ssem_p, rsem_p):
    me = lax.axis_index("dap")
    nseq, chan, nres = m_ref.shape
    rows = z_ref.shape[0]
    heads = wb_ref.shape[0]
    hd = chan // heads
    scale = hd ** -0.5
    base = me * nseq
    peer_barrier(me, n)

    pitch = rows + 8

    def bias_row(i, c):
        b = dot_nt(wb_ref[...], norm(z_ref[i].astype(F32), 1))
        brow[pl.ds(i, heads, stride=pitch), :] = b
        return c
    lax.fori_loop(0, rows, bias_row, 0, unroll=4)
    mine = ds8(me * rows, rows, 16)
    for h in range(heads):
        ball[h, mine, :] = brow[h * pitch:h * pitch + rows, :].astype(BF)
    sends = []
    for d in range(1, n):
        cp = rcopy(ball.at[:, mine, :], ball.at[:, mine, :], ssem_b.at[d], rsem_b.at[d], lax.rem(me + d, n))
        cp.start()
        sends.append(cp)
    wot[...] = wo_ref[...].astype(F32).T.astype(BF)
    qpart[me] = jnp.zeros((chan, nres), F32)
    for d in range(1, n):
        src = ds8(lax.rem(me + n - d, n) * rows, rows, 16)
        rcopy(ball.at[:, src, :], ball.at[:, src, :], ssem_b.at[d], rsem_b.at[d], me).wait_recv()
    for h in range(heads):
        bias[:, h * nres:(h + 1) * nres] = ball[h].astype(F32).T * LOG2E

    hi, mid, lo = split3(1e4 / scale)
    rid = lax.broadcasted_iota(jnp.int32, (16, 2 * nres), 0)
    lid = lax.broadcasted_iota(jnp.int32, (16, 2 * nres), 1)
    aug = jnp.where(rid == 0, hi, jnp.where(rid == 1, mid, jnp.where(rid == 2, lo, 0.0))).astype(BF)
    diag = (rid < 8) == (lid < nres)

    def row_pair(t, carry):
        s0 = t * 2
        mv = jnp.concatenate([m_ref[s0].astype(F32), m_ref[s0 + 1].astype(F32)], axis=1)
        xt = norm(mv, 0)
        proj = dot(wqkvg_ref[...], xt)
        outs = []
        for s in range(2):
            sl = slice(s * nres, (s + 1) * nres)
            mk = mask_ref[pl.ds(base + s0 + s, 1), :].astype(F32) - 1.0
            kaug = jnp.concatenate([proj[chan:2 * chan, sl], jnp.broadcast_to(mk, (16, nres))], axis=0)
            lhs = kaug.T.astype(BF)
            vt = proj[2 * chan:3 * chan, sl].astype(BF)
            for p in range(heads // 2):
                q16 = proj[16 * p:16 * p + 16, sl]
                blk = jnp.where(diag, jnp.concatenate([q16, q16], axis=1), 0.0).astype(BF)
                parts = []
                if p > 0:
                    parts.append(jnp.zeros((16 * p, 2 * nres), BF))
                parts.append(blk)
                if chan - 16 * p - 16 > 0:
                    parts.append(jnp.zeros((chan - 16 * p - 16, 2 * nres), BF))
                parts.append(aug)
                l = dot(lhs, jnp.concatenate(parts, axis=0)) * (scale * LOG2E) + bias[:, 256 * p:256 * p + 256]
                e = jnp.exp2(l - jnp.max(l, axis=0, keepdims=True))
                r = 1.0 / jnp.sum(e, axis=0, keepdims=True)
                o = dot(vt[16 * p:16 * p + 16, :], e.astype(BF))
                outs.append((o[0:8, 0:nres] * r[:, 0:nres], o[8:16, nres:] * r[:, nres:]))
        half = heads // 2
        ot = jnp.concatenate(
            [jnp.concatenate([v for pr in outs[s * half:(s + 1) * half] for v in pr], axis=0) for s in range(2)], axis=1)
        y = (sigmoid(rnd(proj[3 * chan:4 * chan, :])) * ot).astype(BF)
        m1 = (mv + dot(wot[...], y)).astype(BF)
        x2 = norm(m1.astype(F32), 0)
        kvp = rnd(dot(wkv_ref[...], x2))
        acc = qpart[me]
        for s in range(2):
            sl = slice(s * nres, (s + 1) * nres)
            m1_ref[s0 + s] = m1[:, sl]
            x2_ref[s0 + s] = x2[:, sl]
            kv[s0 + s] = kvp[:, sl]
            acc = acc + mask_ref[pl.ds(base + s0 + s, 1), :].astype(F32) * x2[:, sl].astype(F32)
        qpart[me] = acc
        return carry
    lax.fori_loop(0, nseq // 2, row_pair, 0)

    for d in range(1, n):
        cp = rcopy(qpart.at[me], qpart.at[me], ssem_q.at[d], rsem_q.at[d], lax.rem(me + d, n))
        cp.start()
        sends.append(cp)
    count = jnp.sum(mask_ref[...].astype(F32), axis=0, keepdims=True) + 1e-10
    for d in range(1, n):
        src = lax.rem(me + n - d, n)
        rcopy(qpart.at[src], qpart.at[src], ssem_q.at[d], rsem_q.at[d], me).wait_recv()
    tot = qpart[0]
    for d in range(1, n):
        tot = tot + qpart[d]
    tmp[...] = rnd(dot(wq2_ref[...], (tot / count).astype(BF)))
    qd = [tmp[pl.ds(d, heads, stride=hd), :] for d in range(hd)]
    unroll = 8

    def logit(t, mx):
        for u in range(unroll):
            s = t * unroll + u
            row = kv.at[s]
            l = qd[0] * row[0:1, :]
            for d in range(1, hd):
                l = l + qd[d] * row[d:d + 1, :]
            l = l * scale + (mask_ref[pl.ds(base + s, 1), :].astype(F32) - 1.0) * 1e4
            lg[s] = l
            mx = jnp.maximum(mx, l)
        return mx
    mx = lax.fori_loop(0, nseq // unroll, logit, jnp.full((heads, nres), -jnp.inf, F32))

    def weigh(t, carry):
        ssum, acc = carry
        acc = list(acc)
        for u in range(unroll):
            s = t * unroll + u
            row = kv.at[s]
            e = jnp.exp(lg[s] - mx)
            ssum = ssum + e
            eb = rnd(e)
            for d in range(hd):
                acc[d] = acc[d] + eb * row[hd + d:hd + d + 1, :]
        return ssum, tuple(acc)
    zero = jnp.zeros((heads, nres), F32)
    ssum, acc = lax.fori_loop(0, nseq // unroll, weigh, (zero, (zero,) * hd))
    ppart[me, 0:8, :] = mx
    ppart[me, 8:16, :] = ssum
    for d in range(hd):
        ppart[me, 16 + 8 * d:24 + 8 * d, :] = acc[d]
    for d in range(1, n):
        cp = rcopy(ppart.at[me], ppart.at[me], ssem_p.at[d], rsem_p.at[d], lax.rem(me + d, n))
        cp.start()
        sends.append(cp)
    for d in range(1, n):
        src = lax.rem(me + n - d, n)
        rcopy(ppart.at[src], ppart.at[src], ssem_p.at[d], rsem_p.at[d], me).wait_recv()
    top = ppart[0, 0:8, :]
    for d in range(1, n):
        top = jnp.maximum(top, ppart[d, 0:8, :])
    fac = [jnp.exp(ppart[d, 0:8, :] - top) for d in range(n)]
    den = fac[0] * ppart[0, 8:16, :]
    for d in range(1, n):
        den = den + fac[d] * ppart[d, 8:16, :]
    inv = 1.0 / den
    for c in range(hd):
        o = fac[0] * ppart[0, 16 + 8 * c:24 + 8 * c, :]
        for d in range(1, n):
            o = o + fac[d] * ppart[d, 16 + 8 * c:24 + 8 * c, :]
        o2_ref[pl.ds(c, heads, stride=hd), :] = o * inv
    for cp in sends:
        cp.wait_send()


def msa_call(n, mask, mt, z, wb, wqkvg, wo, wq2, wkv):
    nseq, chan, nres = mt.shape
    rows = z.shape[0]
    heads = wb.shape[0]
    dma = pltpu.SemaphoreType.DMA((n,))
    return pl.pallas_call(
        functools.partial(msa_kernel, n),
        name="msa",
        out_shape=[jax.ShapeDtypeStruct((nseq, chan, nres), BF), jax.ShapeDtypeStruct((nseq, chan, nres), BF),
                   jax.ShapeDtypeStruct((chan, nres), F32)],
        in_specs=[VM] * 8,
        out_specs=[VM] * 3,
        scratch_shapes=[
            pltpu.VMEM((heads, n * rows, nres), BF),
            pltpu.VMEM((nres, heads * nres), F32),
            pltpu.VMEM((heads * (rows + 8), nres), F32),
            pltpu.VMEM((nseq, wkv.shape[0], nres), F32),
            pltpu.VMEM((nseq, heads, nres), F32),
            pltpu.VMEM((chan, chan), BF),
            pltpu.VMEM((n, chan, nres), F32),
            pltpu.VMEM((n, chan + 16, nres), F32),
            pltpu.VMEM((chan, nres), F32),
            dma, dma, dma, dma, dma, dma,
        ],
        compiler_params=pltpu.CompilerParams(collective_id=0, has_side_effects=True),
    )(mask, mt, z, wb, wqkvg, wo, wq2, wkv)


def gate_kernel(mask_ref, m1_ref, x2_ref, o2_ref, wg_ref, wo_ref, wopm_ref, m2_ref, a_ref, c_ref, ac, at, wot):
    nseq, chan, nres = m1_ref.shape
    ne = chan // 2
    pitch = chan + 8
    wot[...] = wo_ref[...].astype(F32).T.astype(BF)
    o2 = jnp.concatenate([o2_ref[...]] * 2, axis=1)

    def pair(t, carry):
        s0 = t * 2
        xv = jnp.concatenate([x2_ref[s0], x2_ref[s0 + 1]], axis=1)
        y = (sigmoid(rnd(dot(wg_ref[...], xv))) * o2).astype(BF)
        m1 = jnp.concatenate([m1_ref[s0].astype(F32), m1_ref[s0 + 1].astype(F32)], axis=1)
        m2 = (m1 + dot(wot[...], y)).astype(BF)
        pr = rnd(dot(wopm_ref[...], norm(m2.astype(F32), 0)))
        for s in range(2):
            sl = slice(s * nres, (s + 1) * nres)
            m2_ref[s0 + s] = m2[:, sl]
            ac[ds8((s0 + s) * pitch, chan), :] = pr[:, sl] * mask_ref[pl.ds(s0 + s, 1), :].astype(F32)
        return carry
    lax.fori_loop(0, nseq // 2, pair, 0, unroll=2)

    pitch2 = ne + 8
    pad = jnp.zeros((nres - nseq, nres), F32)

    def plane(e, carry):
        a = jnp.concatenate([ac[pl.ds(e, nseq, stride=pitch), :], pad], axis=0)
        at[pl.ds(e, nres, stride=pitch2), :] = a.T
        c_ref[e] = ac[pl.ds(ne + e, nseq, stride=pitch), :].astype(BF)
        return carry
    lax.fori_loop(0, ne, plane, 0, unroll=2)

    def row(i, carry):
        a_ref[ds8(i * ne, ne, 32), :] = at[ds8(i * pitch2, ne), :].astype(BF)
        return carry
    lax.fori_loop(0, nres, row, 0, unroll=4)


def gate_call(mask, m1, x2, o2, wg, wo, wopm):
    nseq, chan, nres = m1.shape
    ne = chan // 2
    return pl.pallas_call(
        gate_kernel,
        name="gate",
        out_shape=[jax.ShapeDtypeStruct((nseq, chan, nres), BF), jax.ShapeDtypeStruct((nres * ne, nres), BF),
                   jax.ShapeDtypeStruct((ne, nseq, nres), BF)],
        in_specs=[VM] * 7,
        out_specs=[VM] * 3,
        scratch_shapes=[
            pltpu.VMEM((nseq * (chan + 8), nres), F32),
            pltpu.VMEM((nres * (ne + 8), nres), F32),
            pltpu.VMEM((chan, chan), BF),
        ],
    )(mask, m1, x2, o2, wg, wo, wopm)


def tri_attend(n, me, zin, wb_ref, wqkvg_ref, wo_ref, maskcol, zln, brow, ball, bias, proj, flat, wot, tsend, zrecv,
               ssem_b, rsem_b, ssem_t, rsem_t):
    rows, nres, chan = zin.shape
    heads = wb_ref.shape[0]
    hd = chan // heads
    scale = hd ** -0.5
    pitch = rows + 8
    mine = ds8(me * rows, rows, 16)
    sends = []

    def bias_row(i, c):
        zl = norm(zin[i].astype(F32), 1)
        zln[i] = zl
        brow[pl.ds(i, heads, stride=pitch), :] = dot_nt(wb_ref[...], zl)
        return c
    lax.fori_loop(0, rows, bias_row, 0, unroll=4)
    for h in range(heads):
        ball[h, mine, :] = brow[h * pitch:h * pitch + rows, :].astype(BF)
    for d in range(1, n):
        cp = rcopy(ball.at[:, mine, :], ball.at[:, mine, :], ssem_b.at[d], rsem_b.at[d], lax.rem(me + d, n))
        cp.start()
        sends.append(cp)
    wot[...] = wo_ref[...].astype(F32).T.astype(BF)

    def project(i, c):
        zl = zln[i]
        proj[i, 0:chan, :] = dot_nt(wqkvg_ref[0:chan, :], zl).astype(BF)
        proj[i, chan:2 * chan, :] = dot_nt(zl, wqkvg_ref[chan:2 * chan, :]).astype(BF)
        proj[i, 2 * chan:4 * chan, :] = dot_nt(wqkvg_ref[2 * chan:4 * chan, :], zl).astype(BF)
        return c
    lax.fori_loop(0, rows, project, 0, unroll=2)
    for d in range(1, n):
        src = ds8(lax.rem(me + n - d, n) * rows, rows, 16)
        rcopy(ball.at[:, src, :], ball.at[:, src, :], ssem_b.at[d], rsem_b.at[d], me).wait_recv()
    for h in range(heads):
        bias[:, h * nres:(h + 1) * nres] = (ball[h].astype(F32).T + maskcol[...]) * LOG2E
    zero = jnp.zeros((hd, nres), BF)

    def attend(i, c):
        kmat = proj[i, chan:2 * chan, :]
        outs = []
        for p in range(heads // 2):
            r0 = 2 * hd * p
            qa = proj[i, r0:r0 + hd, :]
            qb = proj[i, r0 + hd:r0 + 2 * hd, :]
            blk = jnp.concatenate([jnp.concatenate([qa, zero], axis=1), jnp.concatenate([zero, qb], axis=1)], axis=0)
            parts = []
            if p > 0:
                parts.append(jnp.zeros((r0, 2 * nres), BF))
            parts.append(blk)
            if chan - r0 - 2 * hd > 0:
                parts.append(jnp.zeros((chan - r0 - 2 * hd, 2 * nres), BF))
            l = dot(kmat, jnp.concatenate(parts, axis=0)) * (scale * LOG2E) + bias[:, 256 * p:256 * p + 256]
            e = jnp.exp2(l - jnp.max(l, axis=0, keepdims=True))
            r = 1.0 / jnp.sum(e, axis=0, keepdims=True)
            o = dot(proj[i, 2 * chan + r0:2 * chan + r0 + 2 * hd, :], e.astype(BF))
            outs.append(o[0:hd, 0:nres] * r[:, 0:nres])
            outs.append(o[hd:, nres:] * r[:, nres:])
        y = (sigmoid(proj[i, 3 * chan:4 * chan, :].astype(F32)) * jnp.concatenate(outs, axis=0)).astype(BF)
        upd = dot(wot[...], y).T
        flat[pl.ds(i, nres, stride=pitch), :] = zin[i].astype(F32) + upd
        return c
    lax.fori_loop(0, rows, attend, 0, unroll=2)

    def regroup(j, c):
        tsend[j] = flat[ds8(j * pitch, rows), :].astype(BF)
        return c
    lax.fori_loop(0, nres, regroup, 0, unroll=4)
    for d in range(1, n):
        dst = lax.rem(me + d, n)
        cp = rcopy(tsend.at[pl.ds(dst * rows, rows)], zrecv.at[:, mine, :], ssem_t.at[d], rsem_t.at[d], dst)
        cp.start()
        sends.append(cp)
    zrecv[:, mine, :] = tsend[pl.ds(me * rows, rows)]
    for d in range(1, n):
        src = ds8(lax.rem(me + n - d, n) * rows, rows, 16)
        rcopy(zrecv.at[:, src, :], zrecv.at[:, src, :], ssem_t.at[d], rsem_t.at[d], me).wait_recv()
    return sends


def pair_kernel(n, nchunk, a_ref, c_ref, z_ref, cnt_ref, rm_ref, wopm_ref, wb1_ref, wqkvg1_ref, wo1_ref, wb2_ref, wqkvg2_ref, wo2_ref,
                zo_ref,
                call, aall, upd, osc, z1, zln, brow, ball1, ball2, bias, proj, flat, wot, maskcol, tsend1, tsend2, zmid, zfin,
                ssem_a, rsem_a, ssem_c, rsem_c, ssem_b1, rsem_b1, ssem_t1, rsem_t1, ssem_b2, rsem_b2, ssem_t2, rsem_t2):
    me = lax.axis_index("dap")
    nf, nseq, nres = c_ref.shape
    rows, _, chan = z_ref.shape
    ne = a_ref.shape[0] // nres
    fq = nf // nchunk
    nx = n // 2
    x, k = lax.div(me, 2), lax.rem(me, 2)
    partner = x * 2 + 1 - k
    right = lax.rem(x + 1, nx) * 2 + k
    left = lax.rem(x + nx - 1, nx) * 2 + k
    far = lax.rem(x + 2, nx) * 2 + k
    mine = me
    peer_barrier(me, n)
    arows = rows * ne
    sends = []

    def go(src, dst, ssem, rsem, dev):
        cp = rcopy(src, dst, ssem, rsem, dev)
        cp.start()
        sends.append(cp)

    def other(dev):
        return dev + 1 - 2 * k

    def blk(q, dev, lo=0, size=None):
        size = fq if size is None else size
        return call.at[pl.ds(q * fq + lo, size), dev, 0:nseq, :]

    def own(q):
        src = c_ref.at[pl.ds(q * fq, fq)]
        go(src, blk(q, me), ssem_c.at[q, 0], rsem_c.at[q, 0], right)
        go(src, blk(q, me), ssem_c.at[q, 1], rsem_c.at[q, 1], left)
        go(src, blk(q, me), ssem_c.at[q, 2], rsem_c.at[q, 2], partner)

    def got(q, kind, dev, lo=0, size=None):
        b = blk(q, dev, lo, size)
        rcopy(b, b, ssem_c.at[q, kind], rsem_c.at[q, kind], me).wait_recv()

    def relay(q, kind, dev, to, lo=0, size=None):
        b = blk(q, dev, lo, size)
        go(b, b, ssem_c.at[q, kind], rsem_c.at[q, kind], to)

    for d in range(1, n):
        dst = lax.rem(me + d, n)
        go(a_ref.at[pl.ds(dst * arows, arows), :], aall.at[me], ssem_a.at[d], rsem_a.at[d], dst)
    own(0)
    own(1)
    aall[me] = a_ref[ds8(me * arows, arows, 32), :]
    padz = jnp.zeros((call.shape[1], call.shape[2] - nseq, nres), BF)

    def fill(f, c):
        call[f, :, nseq:, :] = padz
        call[f, me, 0:nseq, :] = c_ref[f]
        return c
    lax.fori_loop(0, nf, fill, 0)
    maskcol[...] = jnp.broadcast_to((rm_ref[...].astype(F32) - 1.0) * 1e4, (nres, nres)).T
    hq = fq // 2

    for q in range(nchunk):
        if q + 2 < nchunk:
            own(q + 2)
        got(q, 0, left)
        relay(q, 3, left, right, 0, hq)
        relay(q, 5, left, partner)
        got(q, 1, right)
        relay(q, 4, right, left, hq, hq)
        relay(q, 6, right, partner)
        got(q, 3, far, 0, hq)
        relay(q, 7, far, partner, 0, hq)
        got(q, 4, far, hq, hq)
        relay(q, 8, far, partner, hq, hq)
        if q == 0:
            for d in range(1, n):
                src = lax.rem(me + n - d, n)
                rcopy(aall.at[src], aall.at[src], ssem_a.at[d], rsem_a.at[d], me).wait_recv()
        got(q, 2, partner)
        got(q, 5, other(left))
        got(q, 6, other(right))
        got(q, 7, other(far), 0, hq)
        got(q, 8, other(far), hq, hq)

        def outer(g, c):
            acc = None
            for kk in range(n // 2):
                rhs = jnp.concatenate(
                    [jnp.concatenate([call[q * fq + 2 * g + u, 2 * kk], call[q * fq + 2 * g + u, 2 * kk + 1]], axis=0) for u in range(2)],
                    axis=1)
                lhs = jnp.concatenate([aall[2 * kk], aall[2 * kk + 1]], axis=1)
                part = dot(lhs, rhs)
                acc = part if acc is None else acc + part
            ob = acc.astype(BF)
            for u in range(2):
                for i in range(rows):
                    osc[i, ds8((2 * g + u) * ne, ne, 32), :] = ob[i * ne:(i + 1) * ne, u * nres:(u + 1) * nres]
            return c
        lax.fori_loop(0, fq // 2, outer, 0)

        def contract(g, c):
            rhs = jnp.concatenate([osc[2 * g], osc[2 * g + 1]], axis=1)
            part = dot(wopm_ref[:, q * fq * ne:(q + 1) * fq * ne], rhs)
            for u in range(2):
                v = part[:, u * nres:(u + 1) * nres]
                upd[2 * g + u] = v if q == 0 else upd[2 * g + u] + v
            return c
        lax.fori_loop(0, rows // 2, contract, 0, unroll=2)

    def residual(i, c):
        u = upd[i] / (1e-3 + cnt_ref[pl.ds(i, 1), :])
        z1[i] = (z_ref[i].astype(F32) + u.T).astype(BF)
        return c
    lax.fori_loop(0, rows, residual, 0, unroll=2)

    sends += tri_attend(n, me, z1, wb1_ref, wqkvg1_ref, wo1_ref, maskcol, zln, brow, ball1, bias, proj, flat, wot, tsend1, zmid,
                        ssem_b1, rsem_b1, ssem_t1, rsem_t1)
    sends += tri_attend(n, me, zmid, wb2_ref, wqkvg2_ref, wo2_ref, maskcol, zln, brow, ball2, bias, proj, flat, wot, tsend2, zfin,
                        ssem_b2, rsem_b2, ssem_t2, rsem_t2)
    zo_ref[...] = zfin[...]
    for cp in sends:
        cp.wait_send()


def pair_call(n, a, c, z, cnt, rm, wopm, wb1, wqkvg1, wo1, wb2, wqkvg2, wo2):
    nf, nseq, nres = c.shape
    rows, _, chan = z.shape
    ne = a.shape[0] // nres
    heads = wb1.shape[0]
    nchunk = 4
    fq = nf // nchunk
    dma = pltpu.SemaphoreType.DMA((n,))
    dmac = pltpu.SemaphoreType.DMA((nchunk, 9))
    pitch = rows + 8
    vz = pltpu.VMEM((rows, nres, chan), BF)
    return pl.pallas_call(
        functools.partial(pair_kernel, n, nchunk),
        name="pair",
        out_shape=jax.ShapeDtypeStruct(z.shape, BF),
        in_specs=[VM] * 12,
        out_specs=VM,
        scratch_shapes=[
            pltpu.VMEM((nf, n, 128, nres), BF),
            pltpu.VMEM((n, rows * ne, nres), BF),
            pltpu.VMEM((rows, chan, nres), F32),
            pltpu.VMEM((rows, fq * ne, nres), BF),
            vz, vz,
            pltpu.VMEM((heads * pitch, nres), F32),
            pltpu.VMEM((heads, n * rows, nres), BF),
            pltpu.VMEM((heads, n * rows, nres), BF),
            pltpu.VMEM((nres, heads * nres), F32),
            pltpu.VMEM((rows, 4 * chan, nres), BF),
            pltpu.VMEM((nres * pitch, chan), F32),
            pltpu.VMEM((chan, chan), BF),
            pltpu.VMEM((nres, nres), F32),
            pltpu.VMEM((nres, rows, chan), BF),
            pltpu.VMEM((nres, rows, chan), BF),
            vz, vz,
            dma, dma, dmac, dmac, dma, dma, dma, dma, dma, dma, dma, dma,
        ],
        compiler_params=pltpu.CompilerParams(collective_id=1, has_side_effects=True),
    )(a, c, z, cnt, rm, wopm, wb1, wqkvg1, wo1, wb2, wqkvg2, wo2)


def flat_t(w):
    return jnp.moveaxis(w, 0, -1).reshape(-1, w.shape[0])


def solution(mesh):
    n = mesh.shape["dap"]

    def block(msa, pair, msa_mask, res_mask, row_bias_w, row_qkvg_w, row_out_w, col_query_w, col_kv_w, col_gate_w, col_out_w,
              opm_proj_w, opm_out_w, start_bias_w, start_qkvg_w, start_out_w, end_bias_w, end_qkvg_w, end_out_w):
        nseq, nres, chan = msa.shape
        rows = pair.shape[0]
        pdim = pair.shape[2]
        me = lax.axis_index("dap")
        mt = jnp.transpose(msa, (0, 2, 1))
        m1, x2, o2 = msa_call(n, msa_mask, mt, pair, row_bias_w.T, flat_t(row_qkvg_w), row_out_w.reshape(chan, chan),
                              flat_t(col_query_w), flat_t(col_kv_w))
        seq_mask = lax.dynamic_slice_in_dim(msa_mask, me * nseq, nseq, axis=0)
        m2, a, c = gate_call(seq_mask, m1, x2, o2, flat_t(col_gate_w), col_out_w.reshape(chan, chan), flat_t(opm_proj_w))
        own_mask = lax.dynamic_slice_in_dim(msa_mask, me * rows, rows, axis=1)
        cnt = jnp.einsum('si,sj->ij', own_mask.astype(BF), msa_mask.astype(BF), preferred_element_type=F32)
        wopm = jnp.transpose(opm_out_w, (2, 1, 0)).reshape(pdim, -1)
        zo = pair_call(n, a, c, pair, cnt, res_mask.reshape(1, nres), wopm,
                       start_bias_w.T, flat_t(start_qkvg_w), start_out_w.reshape(pdim, pdim),
                       end_bias_w.T, flat_t(end_qkvg_w), end_out_w.reshape(pdim, pdim))
        return jnp.transpose(m2, (0, 2, 1)), zo

    row_spec = P(('data', 'dap'), None, None)
    in_specs = (row_spec, row_spec, P('data', None), P('data')) + (P(),) * 15
    return jax.shard_map(block, mesh=mesh, in_specs=in_specs, out_specs=(row_spec, row_spec), check_vma=False)
```

```python
import functools
import math

import jax
import jax.numpy as jnp
import numpy as np
from jax import lax
from jax.experimental import pallas as pl
from jax.experimental.pallas import tpu as pltpu
from jax.sharding import PartitionSpec as P

BF = jnp.bfloat16
F32 = jnp.float32
MESH = pl.DeviceIdType.MESH
LOG2E = math.log2(math.e)
VM = pl.BlockSpec(memory_space=pltpu.VMEM)


def dot(a, b):
    return lax.dot_general(a, b, (((1,), (0,)), ((), ())), preferred_element_type=F32)


def dot_nt(a, b):
    return lax.dot_general(a, b, (((1,), (1,)), ((), ())), preferred_element_type=F32)


def rnd(v):
    return v.astype(BF).astype(F32)


def norm(v, axis):
    mean = jnp.mean(v, axis=axis, keepdims=True)
    cen = v - mean
    var = jnp.mean(cen * cen, axis=axis, keepdims=True)
    return (cen * lax.rsqrt(var + 1e-5)).astype(BF)


def sigmoid(v):
    return 1.0 / (1.0 + jnp.exp(-v))


def split3(value):
    hi = float(np.asarray(value).astype(BF))
    mid = float(np.asarray(value - hi).astype(BF))
    return hi, mid, float(np.asarray(value - hi - mid).astype(BF))


def peer_barrier(me, n):
    sem = pltpu.get_barrier_semaphore()
    for d in range(1, n):
        pl.semaphore_signal(sem, inc=1, device_id={"dap": lax.rem(me + d, n)}, device_id_type=MESH)
    pl.semaphore_wait(sem, n - 1)


def rcopy(src, dst, ssem, rsem, dev):
    return pltpu.make_async_remote_copy(src_ref=src, dst_ref=dst, send_sem=ssem, recv_sem=rsem, device_id={"dap": dev}, device_id_type=MESH)


def ds8(start, size, unit=8):
    return pl.ds(pl.multiple_of(start, unit), size)


def msa_kernel(n, mask_ref, m_ref, z_ref, wb_ref, wqkvg_ref, wo_ref, wq2_ref, wkv_ref, wg2_ref,
               m1_ref, g2_ref, o2_ref,
               ball, bias, brow, kv, lg, wot, qpart, ppart, tmp, x2_ref, xbuf, klhs, qblk, vbuf, gbuf, lbuf, mbuf, pbuf, rbuf, obuf,
               ssem_b, rsem_b, ssem_q, rsem_q, ssem_p, rsem_p):
    me = lax.axis_index("dap")
    nseq, chan, nres = m_ref.shape
    rows = z_ref.shape[0]
    heads = wb_ref.shape[0]
    hd = chan // heads
    scale = hd ** -0.5
    base = me * nseq
    peer_barrier(me, n)

    pitch = rows + 8

    def bias_row(i, c):
        b = dot_nt(wb_ref[...], norm(z_ref[i].astype(F32), 1))
        brow[pl.ds(i, heads, stride=pitch), :] = b
        return c
    lax.fori_loop(0, rows, bias_row, 0, unroll=4)
    mine = ds8(me * rows, rows, 16)
    for h in range(heads):
        ball[h, mine, :] = brow[h * pitch:h * pitch + rows, :].astype(BF)
    sends = []
    for d in range(1, n):
        cp = rcopy(ball.at[:, mine, :], ball.at[:, mine, :], ssem_b.at[d], rsem_b.at[d], lax.rem(me + d, n))
        cp.start()
        sends.append(cp)
    wot[...] = wo_ref[...].astype(F32).T.astype(BF)
    rid = lax.broadcasted_iota(jnp.int32, (16, 2 * nres), 0)
    lid = lax.broadcasted_iota(jnp.int32, (16, 2 * nres), 1)
    diag = (rid < 8) == (lid < nres)

    def lnorm(t, carry):
        xbuf[t] = norm(jnp.concatenate([m_ref[2 * t].astype(F32), m_ref[2 * t + 1].astype(F32)], axis=1), 0)
        return carry
    lax.fori_loop(0, nseq // 2, lnorm, 0, unroll=2)

    def project(t, carry):
        s0 = t * 2
        proj = dot(wqkvg_ref[...], xbuf[t])
        gbuf[t] = proj[3 * chan:4 * chan, :].astype(BF)
        for s in range(2):
            sl = slice(s * nres, (s + 1) * nres)
            mk = mask_ref[pl.ds(base + s0 + s, 1), :].astype(F32) - 1.0
            kaug = jnp.concatenate([proj[chan:2 * chan, sl], jnp.broadcast_to(mk, (nres - chan, nres))], axis=0)
            klhs[s0 + s] = kaug.T.astype(BF)
            vbuf[s0 + s] = proj[2 * chan:3 * chan, sl].astype(BF)
            for p in range(heads // 2):
                q16 = proj[16 * p:16 * p + 16, sl]
                qblk[s0 + s, 16 * p:16 * p + 16, :] = jnp.where(diag, jnp.concatenate([q16, q16], axis=1), 0.0).astype(BF)
        return carry
    lax.fori_loop(0, nseq // 2, project, 0, unroll=2)
    for d in range(1, n):
        src = ds8(lax.rem(me + n - d, n) * rows, rows, 16)
        rcopy(ball.at[:, src, :], ball.at[:, src, :], ssem_b.at[d], rsem_b.at[d], me).wait_recv()
    for h in range(heads):
        bias[:, h * nres:(h + 1) * nres] = ball[h].astype(F32).T * LOG2E

    hi, mid, lo = split3(1e4 / scale)
    rid = lax.broadcasted_iota(jnp.int32, (16, 2 * nres), 0)
    lid = lax.broadcasted_iota(jnp.int32, (16, 2 * nres), 1)
    aug = jnp.where(rid == 0, hi, jnp.where(rid == 1, mid, jnp.where(rid == 2, lo, 0.0))).astype(BF)

    npair = nseq // 2
    half = heads // 2
    wide = 2 * nres

    def qk(t, u):
        s, p = u // half, u % half
        parts = []
        if p > 0:
            parts.append(jnp.zeros((16 * p, wide), BF))
        parts.append(qblk[t * 2 + s, 16 * p:16 * p + 16, :])
        if chan - 16 * p - 16 > 0:
            parts.append(jnp.zeros((chan - 16 * p - 16, wide), BF))
        parts.append(aug)
        l = dot(klhs[t * 2 + s, :, 0:chan + 16], jnp.concatenate(parts, axis=0)) * (scale * LOG2E) + bias[:, wide * p:wide * p + wide]
        lbuf[u] = l
        mbuf[u, 0:1, :] = jnp.max(l, axis=0, keepdims=True)

    def ex(u):
        e = jnp.exp2(lbuf[u] - mbuf[u, 0:1, :])
        pbuf[u] = e.astype(BF)
        rbuf[u, 0:1, :] = 1.0 / jnp.sum(e, axis=0, keepdims=True)

    def pv(t, u):
        s, p = u // half, u % half
        o = dot(vbuf[t * 2 + s, 16 * p:16 * p + 16, :], pbuf[u])
        sl = slice(s * nres, (s + 1) * nres)
        obuf[t, 16 * p:16 * p + 8, sl] = o[0:8, 0:nres] * rbuf[u, 0:1, 0:nres]
        obuf[t, 16 * p + 8:16 * p + 16, sl] = o[8:16, nres:] * rbuf[u, 0:1, nres:]

    units = 2 * half
    for u in range(units):
        qk(0, u)

    def row_pair(t, carry):
        tn = jnp.minimum(t + 1, npair - 1)
        for u in range(units):
            ex(u)
            qk(tn, u)
            if u > 0:
                pv(t, u - 1)
        pv(t, units - 1)
        return carry
    lax.fori_loop(0, npair, row_pair, 0)

    def finish(t, carry):
        s0 = t * 2
        mv = jnp.concatenate([m_ref[s0].astype(F32), m_ref[s0 + 1].astype(F32)], axis=1)
        y = (sigmoid(gbuf[t].astype(F32)) * obuf[t]).astype(BF)
        m1 = (mv + dot(wot[...], y)).astype(BF)
        for s in range(2):
            m1_ref[s0 + s] = m1[:, s * nres:(s + 1) * nres]
        return carry
    lax.fori_loop(0, npair, finish, 0, unroll=4)

    def renorm(t, acc):
        s0 = t * 2
        m1 = jnp.concatenate([m1_ref[s0].astype(F32), m1_ref[s0 + 1].astype(F32)], axis=1)
        x2 = norm(m1, 0)
        for s in range(2):
            sl = slice(s * nres, (s + 1) * nres)
            x2_ref[s0 + s] = x2[:, sl]
            acc = acc + mask_ref[pl.ds(base + s0 + s, 1), :].astype(F32) * x2[:, sl].astype(F32)
        return acc
    qpart[me] = lax.fori_loop(0, npair, renorm, jnp.zeros((chan, nres), F32), unroll=2)

    for d in range(1, n):
        cp = rcopy(qpart.at[me], qpart.at[me], ssem_q.at[d], rsem_q.at[d], lax.rem(me + d, n))
        cp.start()
        sends.append(cp)

    def keyval(t, carry):
        s0 = t * 2
        xv = jnp.concatenate([x2_ref[s0], x2_ref[s0 + 1]], axis=1)
        kvp = rnd(dot(wkv_ref[...], xv))
        g2_ref[t] = dot(wg2_ref[...], xv).astype(BF)
        for s in range(2):
            kv[s0 + s] = kvp[:, s * nres:(s + 1) * nres]
        return carry
    lax.fori_loop(0, npair, keyval, 0, unroll=4)
    count = jnp.sum(mask_ref[...].astype(F32), axis=0, keepdims=True) + 1e-10
    for d in range(1, n):
        src = lax.rem(me + n - d, n)
        rcopy(qpart.at[src], qpart.at[src], ssem_q.at[d], rsem_q.at[d], me).wait_recv()
    tot = qpart[0]
    for d in range(1, n):
        tot = tot + qpart[d]
    tmp[...] = rnd(dot(wq2_ref[...], (tot / count).astype(BF)))
    qd = [tmp[pl.ds(d, heads, stride=hd), :] for d in range(hd)]
    unroll = 8

    def logit(t, mx):
        for u in range(unroll):
            s = t * unroll + u
            row = kv.at[s]
            l = qd[0] * row[0:1, :]
            for d in range(1, hd):
                l = l + qd[d] * row[d:d + 1, :]
            l = l * scale + (mask_ref[pl.ds(base + s, 1), :].astype(F32) - 1.0) * 1e4
            lg[s] = l
            mx = jnp.maximum(mx, l)
        return mx
    mx = lax.fori_loop(0, nseq // unroll, logit, jnp.full((heads, nres), -jnp.inf, F32))

    def weigh(t, carry):
        ssum, acc = carry
        acc = list(acc)
        for u in range(unroll):
            s = t * unroll + u
            row = kv.at[s]
            e = jnp.exp(lg[s] - mx)
            ssum = ssum + e
            eb = rnd(e)
            for d in range(hd):
                acc[d] = acc[d] + eb * row[hd + d:hd + d + 1, :]
        return ssum, tuple(acc)
    zero = jnp.zeros((heads, nres), F32)
    ssum, acc = lax.fori_loop(0, nseq // unroll, weigh, (zero, (zero,) * hd))
    ppart[me, 0:8, :] = mx
    ppart[me, 8:16, :] = ssum
    for d in range(hd):
        ppart[me, 16 + 8 * d:24 + 8 * d, :] = acc[d]
    for d in range(1, n):
        cp = rcopy(ppart.at[me], ppart.at[me], ssem_p.at[d], rsem_p.at[d], lax.rem(me + d, n))
        cp.start()
        sends.append(cp)
    for d in range(1, n):
        src = lax.rem(me + n - d, n)
        rcopy(ppart.at[src], ppart.at[src], ssem_p.at[d], rsem_p.at[d], me).wait_recv()
    top = ppart[0, 0:8, :]
    for d in range(1, n):
        top = jnp.maximum(top, ppart[d, 0:8, :])
    fac = [jnp.exp(ppart[d, 0:8, :] - top) for d in range(n)]
    den = fac[0] * ppart[0, 8:16, :]
    for d in range(1, n):
        den = den + fac[d] * ppart[d, 8:16, :]
    inv = 1.0 / den
    for c in range(hd):
        o = fac[0] * ppart[0, 16 + 8 * c:24 + 8 * c, :]
        for d in range(1, n):
            o = o + fac[d] * ppart[d, 16 + 8 * c:24 + 8 * c, :]
        o2_ref[pl.ds(c, heads, stride=hd), :] = o * inv
    for cp in sends:
        cp.wait_send()


def msa_call(n, mask, mt, z, wb, wqkvg, wo, wq2, wkv, wg2):
    nseq, chan, nres = mt.shape
    rows = z.shape[0]
    heads = wb.shape[0]
    dma = pltpu.SemaphoreType.DMA((n,))
    return pl.pallas_call(
        functools.partial(msa_kernel, n),
        name="msa",
        out_shape=[jax.ShapeDtypeStruct((nseq, chan, nres), BF), jax.ShapeDtypeStruct((nseq // 2, chan, 2 * nres), BF),
                   jax.ShapeDtypeStruct((chan, nres), F32)],
        in_specs=[VM] * 9,
        out_specs=[VM] * 3,
        scratch_shapes=[
            pltpu.VMEM((heads, n * rows, nres), BF),
            pltpu.VMEM((nres, heads * nres), F32),
            pltpu.VMEM((heads * (rows + 8), nres), F32),
            pltpu.VMEM((nseq, wkv.shape[0], nres), F32),
            pltpu.VMEM((nseq, heads, nres), F32),
            pltpu.VMEM((chan, chan), BF),
            pltpu.VMEM((n, chan, nres), F32),
            pltpu.VMEM((n, chan + 16, nres), F32),
            pltpu.VMEM((chan, nres), F32),
            pltpu.VMEM((nseq, chan, nres), BF),
            pltpu.VMEM((nseq // 2, chan, 2 * nres), BF),
            pltpu.VMEM((nseq, nres, nres), BF),
            pltpu.VMEM((nseq, chan, 2 * nres), BF),
            pltpu.VMEM((nseq, chan, nres), BF),
            pltpu.VMEM((nseq // 2, chan, 2 * nres), BF),
            pltpu.VMEM((heads, nres, 2 * nres), F32),
            pltpu.VMEM((heads, 8, 2 * nres), F32),
            pltpu.VMEM((heads, nres, 2 * nres), BF),
            pltpu.VMEM((heads, 8, 2 * nres), F32),
            pltpu.VMEM((nseq // 2, chan, 2 * nres), F32),
            dma, dma, dma, dma, dma, dma,
        ],
        compiler_params=pltpu.CompilerParams(collective_id=0, has_side_effects=True),
    )(mask, mt, z, wb, wqkvg, wo, wq2, wkv, wg2)


def gate_kernel(mask_ref, m1_ref, g2_ref, o2_ref, wo_ref, wopm_ref, m2_ref, a_ref, c_ref, ac, at, wot, xbuf):
    nseq, chan, nres = m1_ref.shape
    ne = chan // 2
    pitch = chan + 8
    wot[...] = wo_ref[...].astype(F32).T.astype(BF)

    def gate(t, carry):
        s0 = t * 2
        y = (sigmoid(g2_ref[t].astype(F32)) * jnp.concatenate([o2_ref[...]] * 2, axis=1)).astype(BF)
        m1 = jnp.concatenate([m1_ref[s0].astype(F32), m1_ref[s0 + 1].astype(F32)], axis=1)
        m2 = (m1 + dot(wot[...], y)).astype(BF)
        for s in range(2):
            m2_ref[s0 + s] = m2[:, s * nres:(s + 1) * nres]
        return carry
    lax.fori_loop(0, nseq // 2, gate, 0, unroll=4)

    def renorm(t, carry):
        xbuf[t] = norm(jnp.concatenate([m2_ref[2 * t].astype(F32), m2_ref[2 * t + 1].astype(F32)], axis=1), 0)
        return carry
    lax.fori_loop(0, nseq // 2, renorm, 0, unroll=2)

    def project(t, carry):
        pr = rnd(dot(wopm_ref[...], xbuf[t]))
        for s in range(2):
            ac[ds8((2 * t + s) * pitch, chan), :] = pr[:, s * nres:(s + 1) * nres] * mask_ref[pl.ds(2 * t + s, 1), :].astype(F32)
        return carry
    lax.fori_loop(0, nseq // 2, project, 0, unroll=4)

    pitch2 = ne + 8
    pad = jnp.zeros((nres - nseq, nres), F32)

    def plane(e, carry):
        a = jnp.concatenate([ac[pl.ds(e, nseq, stride=pitch), :], pad], axis=0)
        at[pl.ds(e, nres, stride=pitch2), :] = a.T
        c_ref[e] = ac[pl.ds(ne + e, nseq, stride=pitch), :].astype(BF)
        return carry
    lax.fori_loop(0, ne, plane, 0, unroll=4)

    def row(i, carry):
        a_ref[ds8(i * ne, ne, 32), :] = at[ds8(i * pitch2, ne), :].astype(BF)
        return carry
    lax.fori_loop(0, nres, row, 0, unroll=4)


def gate_call(mask, m1, g2, o2, wo, wopm):
    nseq, chan, nres = m1.shape
    ne = chan // 2
    return pl.pallas_call(
        gate_kernel,
        name="gate",
        out_shape=[jax.ShapeDtypeStruct((nseq, chan, nres), BF), jax.ShapeDtypeStruct((nres * ne, nres), BF),
                   jax.ShapeDtypeStruct((ne, nseq, nres), BF)],
        in_specs=[VM] * 6,
        out_specs=[VM] * 3,
        scratch_shapes=[
            pltpu.VMEM((nseq * (chan + 8), nres), F32),
            pltpu.VMEM((nres * (ne + 8), nres), F32),
            pltpu.VMEM((chan, chan), BF),
            pltpu.VMEM((nseq // 2, chan, 2 * nres), BF),
        ],
    )(mask, m1, g2, o2, wo, wopm)


def tri_attend(n, me, zin, wb_ref, wqkvg_ref, wo_ref, maskcol, zln, brow, ball, bias, proj, flat, wot, lbuf, mbuf, pbuf, rbuf, obuf, tsend, zrecv,
               ssem_b, rsem_b, ssem_t, rsem_t):
    rows, nres, chan = zin.shape
    heads = wb_ref.shape[0]
    hd = chan // heads
    scale = hd ** -0.5
    pitch = rows + 8
    mine = ds8(me * rows, rows, 16)
    sends = []

    def bias_row(i, c):
        zl = norm(zin[i].astype(F32), 1)
        zln[i] = zl
        brow[pl.ds(i, heads, stride=pitch), :] = dot_nt(wb_ref[...], zl)
        return c
    lax.fori_loop(0, rows, bias_row, 0, unroll=4)
    for h in range(heads):
        ball[h, mine, :] = brow[h * pitch:h * pitch + rows, :].astype(BF)
    for d in range(1, n):
        cp = rcopy(ball.at[:, mine, :], ball.at[:, mine, :], ssem_b.at[d], rsem_b.at[d], lax.rem(me + d, n))
        cp.start()
        sends.append(cp)
    wot[...] = wo_ref[...].astype(F32).T.astype(BF)

    def project(i, c):
        zl = zln[i]
        proj[i, 0:chan, :] = dot_nt(wqkvg_ref[0:chan, :], zl).astype(BF)
        proj[i, chan:2 * chan, :] = dot_nt(zl, wqkvg_ref[chan:2 * chan, :]).astype(BF)
        proj[i, 2 * chan:4 * chan, :] = dot_nt(wqkvg_ref[2 * chan:4 * chan, :], zl).astype(BF)
        return c
    lax.fori_loop(0, rows, project, 0, unroll=2)
    for d in range(1, n):
        src = ds8(lax.rem(me + n - d, n) * rows, rows, 16)
        rcopy(ball.at[:, src, :], ball.at[:, src, :], ssem_b.at[d], rsem_b.at[d], me).wait_recv()
    for h in range(heads):
        bias[:, h * nres:(h + 1) * nres] = (ball[h].astype(F32).T + maskcol[...]) * LOG2E
    zero = jnp.zeros((hd, nres), BF)

    half = heads // 2
    wide = 2 * nres

    def qk(i, p, u):
        r0 = 2 * hd * p
        qa = proj[i, r0:r0 + hd, :]
        qb = proj[i, r0 + hd:r0 + 2 * hd, :]
        parts = [jnp.zeros((r0, wide), BF)] if p > 0 else []
        parts.append(jnp.concatenate([qa, zero], axis=1))
        parts.append(jnp.concatenate([zero, qb], axis=1))
        if chan - r0 - 2 * hd > 0:
            parts.append(jnp.zeros((chan - r0 - 2 * hd, wide), BF))
        l = dot(proj[i, chan:2 * chan, :], jnp.concatenate(parts, axis=0)) * (scale * LOG2E) + bias[:, wide * p:wide * p + wide]
        lbuf[u] = l
        mbuf[u, 0:1, :] = jnp.max(l, axis=0, keepdims=True)

    def ex(u):
        e = jnp.exp2(lbuf[u] - mbuf[u, 0:1, :])
        pbuf[u] = e.astype(BF)
        rbuf[u, 0:1, :] = 1.0 / jnp.sum(e, axis=0, keepdims=True)

    def pv(i, p, u):
        r0 = 2 * hd * p
        o = dot(proj[i, 2 * chan + r0:2 * chan + r0 + 2 * hd, :], pbuf[u])
        obuf[i, r0:r0 + hd, :] = o[0:hd, 0:nres] * rbuf[u, 0:1, 0:nres]
        obuf[i, r0 + hd:r0 + 2 * hd, :] = o[hd:, nres:] * rbuf[u, 0:1, nres:]

    units = [(i, p) for i in range(2) for p in range(half)]
    for u, (i, p) in enumerate(units):
        qk(i, p, u)

    def attend(t, c):
        nxt = jnp.minimum(2 * t + 2, rows - 2)
        for u, (i, p) in enumerate(units):
            ex(u)
            qk(nxt + i, p, u)
            if u > 0:
                pv(2 * t + units[u - 1][0], units[u - 1][1], u - 1)
        pv(2 * t + units[-1][0], units[-1][1], len(units) - 1)
        return c
    lax.fori_loop(0, rows // 2, attend, 0)

    def finish(i, c):
        y = (sigmoid(proj[i, 3 * chan:4 * chan, :].astype(F32)) * obuf[i]).astype(BF)
        upd = dot(wot[...], y).T
        flat[pl.ds(i, nres, stride=pitch), :] = zin[i].astype(F32) + upd
        return c
    lax.fori_loop(0, rows, finish, 0, unroll=4)

    def regroup(j, c):
        tsend[j] = flat[ds8(j * pitch, rows), :].astype(BF)
        return c
    lax.fori_loop(0, nres, regroup, 0, unroll=4)
    for d in range(1, n):
        dst = lax.rem(me + d, n)
        cp = rcopy(tsend.at[pl.ds(dst * rows, rows)], zrecv.at[:, mine, :], ssem_t.at[d], rsem_t.at[d], dst)
        cp.start()
        sends.append(cp)
    zrecv[:, mine, :] = tsend[pl.ds(me * rows, rows)]
    for d in range(1, n):
        src = ds8(lax.rem(me + n - d, n) * rows, rows, 16)
        rcopy(zrecv.at[:, src, :], zrecv.at[:, src, :], ssem_t.at[d], rsem_t.at[d], me).wait_recv()
    return sends


def pair_kernel(n, nchunk, a_ref, c_ref, z_ref, cnt_ref, rm_ref, wopm_ref, wb1_ref, wqkvg1_ref, wo1_ref, wb2_ref, wqkvg2_ref, wo2_ref,
                zo_ref,
                call, aall, upd, osc, z1, zln, brow, ball1, ball2, bias, proj, flat, wot, lbuf, mbuf, pbuf, rbuf, obuf, arel, maskcol, tsend1, tsend2, zmid, zfin,
                ssem_a, rsem_a, ssem_r, rsem_r, ssem_c, rsem_c, ssem_b1, rsem_b1, ssem_t1, rsem_t1, ssem_b2, rsem_b2, ssem_t2, rsem_t2):
    me = lax.axis_index("dap")
    nf, nseq, nres = c_ref.shape
    rows, _, chan = z_ref.shape
    ne = a_ref.shape[0] // nres
    fq = nf // nchunk
    nx = n // 2
    x, k = lax.div(me, 2), lax.rem(me, 2)
    partner = x * 2 + 1 - k
    right = lax.rem(x + 1, nx) * 2 + k
    left = lax.rem(x + nx - 1, nx) * 2 + k
    far = lax.rem(x + 2, nx) * 2 + k
    mine = me
    peer_barrier(me, n)
    arows = rows * ne
    sends = []

    def go(src, dst, ssem, rsem, dev):
        cp = rcopy(src, dst, ssem, rsem, dev)
        cp.start()
        sends.append(cp)

    def other(dev):
        return dev + 1 - 2 * k

    def blk(q, dev, lo=0, size=None):
        size = fq if size is None else size
        return call.at[pl.ds(q * fq + lo, size), dev, 0:nseq, :]

    def own(q):
        src = c_ref.at[pl.ds(q * fq, fq)]
        go(src, blk(q, me), ssem_c.at[q, 0], rsem_c.at[q, 0], right)
        go(src, blk(q, me), ssem_c.at[q, 1], rsem_c.at[q, 1], left)
        go(src, blk(q, me), ssem_c.at[q, 2], rsem_c.at[q, 2], partner)

    def got(q, kind, dev, lo=0, size=None):
        b = blk(q, dev, lo, size)
        rcopy(b, b, ssem_c.at[q, kind], rsem_c.at[q, kind], me).wait_recv()

    def relay(q, kind, dev, to, lo=0, size=None):
        b = blk(q, dev, lo, size)
        go(b, b, ssem_c.at[q, kind], rsem_c.at[q, kind], to)

    rightc, leftc, farc = lax.rem(x + 1, nx) * 2, lax.rem(x + nx - 1, nx) * 2, lax.rem(x + 2, nx) * 2

    def ablk(dst):
        return a_ref.at[pl.ds(dst * arows, arows), :]

    go(ablk(farc), arel.at[0], ssem_a.at[0], rsem_a.at[0], right)
    go(ablk(farc + 1), arel.at[1], ssem_a.at[1], rsem_a.at[1], left)
    for j in range(2):
        go(ablk(rightc + j), aall.at[me], ssem_a.at[2 + j], rsem_a.at[2 + k], rightc + j)
        go(ablk(leftc + j), aall.at[me], ssem_a.at[4 + j], rsem_a.at[4 + k], leftc + j)
    go(ablk(partner), aall.at[me], ssem_a.at[6], rsem_a.at[6], partner)
    own(0)
    own(1)
    aall[me] = a_ref[ds8(me * arows, arows, 32), :]
    padz = jnp.zeros((call.shape[1], call.shape[2] - nseq, nres), BF)

    def fill(f, c):
        call[f, :, nseq:, :] = padz
        call[f, me, 0:nseq, :] = c_ref[f]
        return c
    lax.fori_loop(0, nf, fill, 0)
    maskcol[...] = jnp.broadcast_to((rm_ref[...].astype(F32) - 1.0) * 1e4, (nres, nres)).T
    hq = fq // 2

    def neighbours(q):
        got(q, 0, left)
        relay(q, 3, left, right, 0, hq)
        relay(q, 5, left, partner)
        got(q, 1, right)
        relay(q, 4, right, left, hq, hq)
        relay(q, 6, right, partner)
        if q + 2 < nchunk:
            own(q + 2)

    def gota(slot, sem):
        rcopy(aall.at[slot], aall.at[slot], ssem_a.at[0], sem, me).wait_recv()

    rcopy(arel.at[0], arel.at[0], ssem_a.at[0], rsem_a.at[0], me).wait_recv()
    go(arel.at[0], aall.at[left], ssem_r.at[0], rsem_r.at[k], rightc)
    rcopy(arel.at[1], arel.at[1], ssem_a.at[1], rsem_a.at[1], me).wait_recv()
    go(arel.at[1], aall.at[right], ssem_r.at[1], rsem_r.at[k], leftc + 1)
    neighbours(0)
    neighbours(1)
    for j in range(2):
        gota(leftc + j, rsem_a.at[2 + j])
        gota(rightc + j, rsem_a.at[4 + j])
        gota(farc + j, rsem_r.at[j])
    gota(partner, rsem_a.at[6])

    for q in range(nchunk):
        got(q, 3, far, 0, hq)
        relay(q, 7, far, partner, 0, hq)
        got(q, 4, far, hq, hq)
        relay(q, 8, far, partner, hq, hq)
        got(q, 2, partner)
        got(q, 5, other(left))
        got(q, 6, other(right))
        got(q, 7, other(far), 0, hq)
        got(q, 8, other(far), hq, hq)

        def outer(g, c):
            acc = None
            for kk in range(n // 2):
                rhs = jnp.concatenate(
                    [jnp.concatenate([call[q * fq + 2 * g + u, 2 * kk], call[q * fq + 2 * g + u, 2 * kk + 1]], axis=0) for u in range(2)],
                    axis=1)
                lhs = jnp.concatenate([aall[2 * kk], aall[2 * kk + 1]], axis=1)
                part = dot(lhs, rhs)
                acc = part if acc is None else acc + part
            ob = acc.astype(BF)
            for u in range(2):
                for i in range(rows):
                    osc[i, ds8((2 * g + u) * ne, ne, 32), :] = ob[i * ne:(i + 1) * ne, u * nres:(u + 1) * nres]
            return c
        lax.fori_loop(0, fq // 2, outer, 0)

        def contract(g, c):
            rhs = jnp.concatenate([osc[2 * g], osc[2 * g + 1]], axis=1)
            part = dot(wopm_ref[:, q * fq * ne:(q + 1) * fq * ne], rhs)
            for u in range(2):
                v = part[:, u * nres:(u + 1) * nres]
                upd[2 * g + u] = v if q == 0 else upd[2 * g + u] + v
            return c
        lax.fori_loop(0, rows // 2, contract, 0, unroll=2)
        if q + 2 < nchunk:
            neighbours(q + 2)

    def residual(i, c):
        u = upd[i] / (1e-3 + cnt_ref[pl.ds(i, 1), :])
        z1[i] = (z_ref[i].astype(F32) + u.T).astype(BF)
        return c
    lax.fori_loop(0, rows, residual, 0, unroll=2)

    sends += tri_attend(n, me, z1, wb1_ref, wqkvg1_ref, wo1_ref, maskcol, zln, brow, ball1, bias, proj, flat, wot, lbuf, mbuf, pbuf, rbuf, obuf, tsend1, zmid,
                        ssem_b1, rsem_b1, ssem_t1, rsem_t1)
    sends += tri_attend(n, me, zmid, wb2_ref, wqkvg2_ref, wo2_ref, maskcol, zln, brow, ball2, bias, proj, flat, wot, lbuf, mbuf, pbuf, rbuf, obuf, tsend2, zfin,
                        ssem_b2, rsem_b2, ssem_t2, rsem_t2)
    zo_ref[...] = zfin[...]
    for cp in sends:
        cp.wait_send()


def pair_call(n, a, c, z, cnt, rm, wopm, wb1, wqkvg1, wo1, wb2, wqkvg2, wo2):
    nf, nseq, nres = c.shape
    rows, _, chan = z.shape
    ne = a.shape[0] // nres
    heads = wb1.shape[0]
    nchunk = 4
    fq = nf // nchunk
    dma = pltpu.SemaphoreType.DMA((n,))
    dmac = pltpu.SemaphoreType.DMA((nchunk, 9))
    pitch = rows + 8
    vz = pltpu.VMEM((rows, nres, chan), BF)
    return pl.pallas_call(
        functools.partial(pair_kernel, n, nchunk),
        name="pair",
        out_shape=jax.ShapeDtypeStruct(z.shape, BF),
        in_specs=[VM] * 12,
        out_specs=VM,
        scratch_shapes=[
            pltpu.VMEM((nf, n, 128, nres), BF),
            pltpu.VMEM((n, rows * ne, nres), BF),
            pltpu.VMEM((rows, chan, nres), F32),
            pltpu.VMEM((rows, fq * ne, nres), BF),
            vz, vz,
            pltpu.VMEM((heads * pitch, nres), F32),
            pltpu.VMEM((heads, n * rows, nres), BF),
            pltpu.VMEM((heads, n * rows, nres), BF),
            pltpu.VMEM((nres, heads * nres), F32),
            pltpu.VMEM((rows, 4 * chan, nres), BF),
            pltpu.VMEM((nres * pitch, chan), F32),
            pltpu.VMEM((chan, chan), BF),
            pltpu.VMEM((heads, nres, 2 * nres), F32),
            pltpu.VMEM((heads, 8, 2 * nres), F32),
            pltpu.VMEM((heads, nres, 2 * nres), BF),
            pltpu.VMEM((heads, 8, 2 * nres), F32),
            pltpu.VMEM((rows, chan, nres), F32),
            pltpu.VMEM((2, rows * ne, nres), BF),
            pltpu.VMEM((nres, nres), F32),
            pltpu.VMEM((nres, rows, chan), BF),
            pltpu.VMEM((nres, rows, chan), BF),
            vz, vz,
            dma, dma, dma, dma, dmac, dmac, dma, dma, dma, dma, dma, dma, dma, dma,
        ],
        compiler_params=pltpu.CompilerParams(collective_id=1, has_side_effects=True),
    )(a, c, z, cnt, rm, wopm, wb1, wqkvg1, wo1, wb2, wqkvg2, wo2)


def flat_t(w):
    return jnp.moveaxis(w, 0, -1).reshape(-1, w.shape[0])


def solution(mesh):
    n = mesh.shape["dap"]

    def block(msa, pair, msa_mask, res_mask, row_bias_w, row_qkvg_w, row_out_w, col_query_w, col_kv_w, col_gate_w, col_out_w,
              opm_proj_w, opm_out_w, start_bias_w, start_qkvg_w, start_out_w, end_bias_w, end_qkvg_w, end_out_w):
        nseq, nres, chan = msa.shape
        rows = pair.shape[0]
        pdim = pair.shape[2]
        me = lax.axis_index("dap")
        mt = jnp.transpose(msa, (0, 2, 1))
        m1, g2, o2 = msa_call(n, msa_mask, mt, pair, row_bias_w.T, flat_t(row_qkvg_w), row_out_w.reshape(chan, chan),
                              flat_t(col_query_w), flat_t(col_kv_w), flat_t(col_gate_w))
        seq_mask = lax.dynamic_slice_in_dim(msa_mask, me * nseq, nseq, axis=0)
        m2, a, c = gate_call(seq_mask, m1, g2, o2, col_out_w.reshape(chan, chan), flat_t(opm_proj_w))
        own_mask = lax.dynamic_slice_in_dim(msa_mask, me * rows, rows, axis=1)
        cnt = jnp.einsum('si,sj->ij', own_mask.astype(BF), msa_mask.astype(BF), preferred_element_type=F32)
        wopm = jnp.transpose(opm_out_w, (2, 1, 0)).reshape(pdim, -1)
        zo = pair_call(n, a, c, pair, cnt, res_mask.reshape(1, nres), wopm,
                       start_bias_w.T, flat_t(start_qkvg_w), start_out_w.reshape(pdim, pdim),
                       end_bias_w.T, flat_t(end_qkvg_w), end_out_w.reshape(pdim, pdim))
        return jnp.transpose(m2, (0, 2, 1)), zo

    row_spec = P(('data', 'dap'), None, None)
    in_specs = (row_spec, row_spec, P('data', None), P('data')) + (P(),) * 15
    return jax.shard_map(block, mesh=mesh, in_specs=in_specs, out_specs=(row_spec, row_spec), check_vma=False)
```

```python
import functools
import math

import jax
import jax.numpy as jnp
import numpy as np
from jax import lax
from jax.experimental import pallas as pl
from jax.experimental.pallas import tpu as pltpu
from jax.sharding import PartitionSpec as P

BF = jnp.bfloat16
F32 = jnp.float32
MESH = pl.DeviceIdType.MESH
LOG2E = math.log2(math.e)
VM = pl.BlockSpec(memory_space=pltpu.VMEM)


def dot(a, b):
    return lax.dot_general(a, b, (((1,), (0,)), ((), ())), preferred_element_type=F32)


def dot_nt(a, b):
    return lax.dot_general(a, b, (((1,), (1,)), ((), ())), preferred_element_type=F32)


def rnd(v):
    return v.astype(BF).astype(F32)


def norm(v, axis):
    mean = jnp.mean(v, axis=axis, keepdims=True)
    cen = v - mean
    var = jnp.mean(cen * cen, axis=axis, keepdims=True)
    return (cen * lax.rsqrt(var + 1e-5)).astype(BF)


def sigmoid(v):
    return 1.0 / (1.0 + jnp.exp(-v))


def split3(value):
    hi = float(np.asarray(value).astype(BF))
    mid = float(np.asarray(value - hi).astype(BF))
    return hi, mid, float(np.asarray(value - hi - mid).astype(BF))


def rcopy(src, dst, ssem, rsem, dev):
    return pltpu.make_async_remote_copy(src_ref=src, dst_ref=dst, send_sem=ssem, recv_sem=rsem, device_id={"dap": dev}, device_id_type=MESH)


def loop(count, body, unroll=1):
    lax.fori_loop(0, count, lambda t, c: (body(t), c)[-1], 0, unroll=unroll)


def cat(*v):
    return jnp.concatenate(v, axis=-1)


def stack(*v):
    return jnp.concatenate(v, axis=0)


def part(s, width):
    return slice(s * width, s * width + width)


class Place:
    def __init__(self, n):
        nx = n // 2
        self.n, self.me = n, lax.axis_index("dap")
        x, self.k = lax.div(self.me, 2), lax.rem(self.me, 2)
        self.rightc, self.leftc, self.farc = (lax.rem(x + d, nx) * 2 for d in (1, nx - 1, 2))
        self.right, self.left, self.far = (c + self.k for c in (self.rightc, self.leftc, self.farc))
        self.partner = self.other(self.me)
        self.sends = []

    def other(self, dev):
        return dev + 1 - 2 * self.k

    def signal(self):
        sem = pltpu.get_barrier_semaphore()
        for d in range(1, self.n):
            pl.semaphore_signal(sem, inc=1, device_id={"dap": lax.rem(self.me + d, self.n)}, device_id_type=MESH)

    def meet(self):
        pl.semaphore_wait(pltpu.get_barrier_semaphore(), self.n - 1)

    def go(self, src, dst, ssem, rsem, dev):
        cp = rcopy(src, dst, ssem, rsem, dev)
        cp.start()
        self.sends.append(cp)

    def got(self, dst, rsem):
        rcopy(dst, dst, rsem, rsem, self.me).wait_recv()

    def drain(self):
        for cp in self.sends:
            cp.wait_send()

    def to_all(self, src, slot, ssem, rsem):
        for d in range(1, self.n):
            self.go(src, slot(self.me), ssem.at[d], rsem.at[d], lax.rem(self.me + d, self.n))

    def from_all(self, slot, rsem):
        for d in range(1, self.n):
            self.got(slot(lax.rem(self.me + self.n - d, self.n)), rsem.at[d])

    def scatter(self, blk, slot, rel, ssem, rsem):
        k, me = self.k, self.me
        self.go(blk(self.farc), rel.at[0], ssem.at[0], rsem.at[0], self.right)
        self.go(blk(self.farc + 1), rel.at[1], ssem.at[1], rsem.at[1], self.left)
        for j in range(2):
            self.go(blk(self.rightc + j), slot(me), ssem.at[2 + j], rsem.at[2 + k], self.rightc + j)
            self.go(blk(self.leftc + j), slot(me), ssem.at[4 + j], rsem.at[4 + k], self.leftc + j)
        self.go(blk(self.partner), slot(me), ssem.at[6], rsem.at[6], self.partner)

    def scatter_relay(self, slot, rel, ssem, rsem):
        self.got(rel.at[0], rsem.at[0])
        self.go(rel.at[0], slot(self.left), ssem.at[7], rsem.at[7 + self.k], self.rightc)
        self.got(rel.at[1], rsem.at[1])
        self.go(rel.at[1], slot(self.right), ssem.at[8], rsem.at[7 + self.k], self.leftc + 1)

    def scatter_wait(self, slot, rsem):
        for j in range(2):
            self.got(slot(self.leftc + j), rsem.at[2 + j])
            self.got(slot(self.rightc + j), rsem.at[4 + j])
            self.got(slot(self.farc + j), rsem.at[7 + j])
        self.got(slot(self.partner), rsem.at[6])

    def spread(self, src, slot, ssem, rsem):
        for i, dev in enumerate((self.right, self.left, self.partner)):
            self.go(src, slot(self.me), ssem.at[i], rsem.at[i], dev)

    def spread_relay(self, slot, lower, upper, ssem, rsem):
        left, right = self.left, self.right
        self.got(slot(left), rsem.at[0])
        self.go(lower(left), lower(left), ssem.at[3], rsem.at[3], right)
        self.go(slot(left), slot(left), ssem.at[5], rsem.at[5], self.partner)
        self.got(slot(right), rsem.at[1])
        self.go(upper(right), upper(right), ssem.at[4], rsem.at[4], left)
        self.go(slot(right), slot(right), ssem.at[6], rsem.at[6], self.partner)

    def spread_wait(self, slot, lower, upper, ssem, rsem):
        for i, half in enumerate((lower, upper)):
            self.got(half(self.far), rsem.at[3 + i])
            self.go(half(self.far), half(self.far), ssem.at[7 + i], rsem.at[7 + i], self.partner)
        self.got(slot(self.partner), rsem.at[2])
        self.got(slot(self.other(self.left)), rsem.at[5])
        self.got(slot(self.other(self.right)), rsem.at[6])
        for i, half in enumerate((lower, upper)):
            self.got(half(self.other(self.far)), rsem.at[7 + i])


def ds8(start, size, unit=8):
    return pl.ds(pl.multiple_of(start, unit), size)


def msa_kernel(n, nin, *refs):
    inputs, outputs, held = refs[:nin], refs[nin:nin + 3], refs[nin + 3:2 * nin + 3]
    msa_body(n, inputs, held, *outputs, *refs[2 * nin + 3:])


def msa_body(n, inputs, held,
               m1_ref, g2_ref, o2_ref, isem,
               ball, bias, brow, kv, lg, wot, qpart, ppart, tmp, x2_ref, xbuf, klhs, qblk, vbuf, gbuf, lbuf, mbuf, pbuf, rbuf, obuf,
               ssem_b, rsem_b, ssem_q, rsem_q, ssem_p, rsem_p):
    pc = Place(n)
    me = pc.me
    pc.signal()
    loads = [pltpu.make_async_copy(a, b, isem.at[i]) for i, (a, b) in enumerate(zip(inputs, held))]
    for cp in loads:
        cp.start()
    z_ref, wb_ref, mask_ref, m_ref, wqkvg_ref, wo_ref, wq2_ref, wkv_ref, wg2_ref = held
    loads[0].wait()
    loads[1].wait()
    nseq, chan, nres = m_ref.shape
    rows = z_ref.shape[0]
    heads = wb_ref.shape[0]
    hd = chan // heads
    scale = hd ** -0.5
    base = me * nseq

    pitch = rows + 8

    def bias_row(i):
        b = dot_nt(wb_ref[:], norm(z_ref[i].astype(F32), 1))
        brow[pl.ds(i, heads, stride=pitch), :] = b
    loop(rows, bias_row, 4)
    mine = ds8(me * rows, rows, 16)
    for h in range(heads):
        ball[h, mine, :] = brow[h * pitch:h * pitch + rows, :].astype(BF)
    def bslot(dev):
        return ball.at[:, ds8(dev * rows, rows, 16), :]

    pc.meet()
    pc.to_all(bslot(me), bslot, ssem_b, rsem_b)
    for cp in loads[2:]:
        cp.wait()
    wot[:] = wo_ref[:].astype(F32).T.astype(BF)
    rid = lax.broadcasted_iota(jnp.int32, (16, 2 * nres), 0)
    lid = lax.broadcasted_iota(jnp.int32, (16, 2 * nres), 1)
    diag = (rid < 8) == (lid < nres)

    def lnorm(t):
        xbuf[t] = norm(jnp.concatenate([m_ref[2 * t].astype(F32), m_ref[2 * t + 1].astype(F32)], axis=1), 0)
    loop(nseq // 2, lnorm, 2)

    def project(t):
        s0 = t * 2
        proj = dot(wqkvg_ref[:], xbuf[t])
        gbuf[t] = proj[3 * chan:4 * chan, :].astype(BF)
        for s in range(2):
            sl = slice(s * nres, (s + 1) * nres)
            mk = mask_ref[pl.ds(base + s0 + s, 1), :].astype(F32) - 1.0
            kaug = jnp.concatenate([proj[chan:2 * chan, sl], jnp.broadcast_to(mk, (nres - chan, nres))], axis=0)
            klhs[s0 + s] = kaug.T.astype(BF)
            vbuf[s0 + s] = proj[2 * chan:3 * chan, sl].astype(BF)
            for p in range(heads // 2):
                q16 = proj[16 * p:16 * p + 16, sl]
                qblk[s0 + s, 16 * p:16 * p + 16, :] = jnp.where(diag, jnp.concatenate([q16, q16], axis=1), 0.0).astype(BF)
    loop(nseq // 2, project, 2)
    pc.from_all(bslot, rsem_b)
    for h in range(heads):
        bias[:, h * nres:(h + 1) * nres] = ball[h].astype(F32).T * LOG2E

    hi, mid, lo = split3(1e4 / scale)
    rid = lax.broadcasted_iota(jnp.int32, (16, 2 * nres), 0)
    lid = lax.broadcasted_iota(jnp.int32, (16, 2 * nres), 1)
    aug = jnp.where(rid == 0, hi, jnp.where(rid == 1, mid, jnp.where(rid == 2, lo, 0.0))).astype(BF)

    npair = nseq // 2
    half = heads // 2
    wide = 2 * nres

    def qk(t, u):
        s, p = u // half, u % half
        parts = []
        if p > 0:
            parts.append(jnp.zeros((16 * p, wide), BF))
        parts.append(qblk[t * 2 + s, 16 * p:16 * p + 16, :])
        if chan - 16 * p - 16 > 0:
            parts.append(jnp.zeros((chan - 16 * p - 16, wide), BF))
        parts.append(aug)
        l = dot(klhs[t * 2 + s, :, :chan + 16], jnp.concatenate(parts, axis=0)) * (scale * LOG2E) + bias[:, wide * p:wide * p + wide]
        lbuf[u] = l
        mbuf[u, 0:1, :] = jnp.max(l, axis=0, keepdims=True)

    def ex(u):
        e = jnp.exp2(lbuf[u] - mbuf[u, 0:1, :])
        pbuf[u] = e.astype(BF)
        rbuf[u, 0:1, :] = 1.0 / jnp.sum(e, axis=0, keepdims=True)

    def pv(t, u):
        s, p = u // half, u % half
        o = dot(vbuf[t * 2 + s, 16 * p:16 * p + 16, :], pbuf[u])
        sl = slice(s * nres, (s + 1) * nres)
        obuf[t, 16 * p:16 * p + 8, sl] = o[:8, :nres] * rbuf[u, 0:1, :nres]
        obuf[t, 16 * p + 8:16 * p + 16, sl] = o[8:16, nres:] * rbuf[u, 0:1, nres:]

    units = 2 * half
    for u in range(units):
        qk(0, u)

    def row_pair(t):
        tn = jnp.minimum(t + 1, npair - 1)
        for u in range(units):
            ex(u)
            qk(tn, u)
            if u > 0:
                pv(t, u - 1)
        pv(t, units - 1)
    loop(npair, row_pair)

    def finish(t):
        s0 = t * 2
        mv = jnp.concatenate([m_ref[s0].astype(F32), m_ref[s0 + 1].astype(F32)], axis=1)
        y = (sigmoid(gbuf[t].astype(F32)) * obuf[t]).astype(BF)
        m1 = (mv + dot(wot[:], y)).astype(BF)
        for s in range(2):
            m1_ref[s0 + s] = m1[:, s * nres:(s + 1) * nres]
    loop(npair, finish, 4)

    def renorm(t, acc):
        s0 = t * 2
        m1 = jnp.concatenate([m1_ref[s0].astype(F32), m1_ref[s0 + 1].astype(F32)], axis=1)
        x2 = norm(m1, 0)
        for s in range(2):
            sl = slice(s * nres, (s + 1) * nres)
            x2_ref[s0 + s] = x2[:, sl]
            acc = acc + mask_ref[pl.ds(base + s0 + s, 1), :].astype(F32) * x2[:, sl].astype(F32)
        return acc
    qpart[me] = lax.fori_loop(0, npair, renorm, jnp.zeros((chan, nres), F32), unroll=2)

    halfq = chan // 2
    qslots = (lambda dev: qpart.at[dev]), (lambda dev: qpart.at[dev, :halfq]), (lambda dev: qpart.at[dev, halfq:])
    pc.spread(qpart.at[me], qslots[0], ssem_q, rsem_q)

    def keyval(t):
        s0 = t * 2
        xv = jnp.concatenate([x2_ref[s0], x2_ref[s0 + 1]], axis=1)
        kvp = rnd(dot(wkv_ref[:], xv))
        g2_ref[t] = dot(wg2_ref[:], xv).astype(BF)
        for s in range(2):
            kv[s0 + s] = kvp[:, s * nres:(s + 1) * nres]
    loop(npair, keyval, 4)
    count = jnp.sum(mask_ref[:].astype(F32), axis=0, keepdims=True) + 1e-10
    pc.spread_relay(*qslots, ssem_q, rsem_q)
    pc.spread_wait(*qslots, ssem_q, rsem_q)
    tot = qpart[0]
    for d in range(1, n):
        tot = tot + qpart[d]
    tmp[:] = rnd(dot(wq2_ref[:], (tot / count).astype(BF)))
    qd = [tmp[pl.ds(d, heads, stride=hd), :] for d in range(hd)]
    unroll = 8

    def logit(t, mx):
        for u in range(unroll):
            s = t * unroll + u
            row = kv.at[s]
            l = qd[0] * row[0:1, :]
            for d in range(1, hd):
                l = l + qd[d] * row[d:d + 1, :]
            l = l * scale + (mask_ref[pl.ds(base + s, 1), :].astype(F32) - 1.0) * 1e4
            lg[s] = l
            mx = jnp.maximum(mx, l)
        return mx
    mx = lax.fori_loop(0, nseq // unroll, logit, jnp.full((heads, nres), -jnp.inf, F32))

    def weigh(t, carry):
        ssum, acc = carry
        acc = list(acc)
        for u in range(unroll):
            s = t * unroll + u
            row = kv.at[s]
            e = jnp.exp(lg[s] - mx)
            ssum = ssum + e
            eb = rnd(e)
            for d in range(hd):
                acc[d] = acc[d] + eb * row[hd + d:hd + d + 1, :]
        return ssum, tuple(acc)
    zero = jnp.zeros((heads, nres), F32)
    ssum, acc = lax.fori_loop(0, nseq // unroll, weigh, (zero, (zero,) * hd))
    ppart[me, :8, :] = mx
    ppart[me, 8:16, :] = ssum
    for d in range(hd):
        ppart[me, 16 + 8 * d:24 + 8 * d, :] = acc[d]
    halfp = 8 + chan // 2
    pslots = (lambda dev: ppart.at[dev]), (lambda dev: ppart.at[dev, :halfp]), (lambda dev: ppart.at[dev, halfp:])
    pc.spread(ppart.at[me], pslots[0], ssem_p, rsem_p)
    pc.spread_relay(*pslots, ssem_p, rsem_p)
    pc.spread_wait(*pslots, ssem_p, rsem_p)
    top = ppart[0, :8, :]
    for d in range(1, n):
        top = jnp.maximum(top, ppart[d, :8, :])
    fac = [jnp.exp(ppart[d, :8, :] - top) for d in range(n)]
    den = fac[0] * ppart[0, 8:16, :]
    for d in range(1, n):
        den = den + fac[d] * ppart[d, 8:16, :]
    inv = 1.0 / den
    for c in range(hd):
        o = fac[0] * ppart[0, 16 + 8 * c:24 + 8 * c, :]
        for d in range(1, n):
            o = o + fac[d] * ppart[d, 16 + 8 * c:24 + 8 * c, :]
        o2_ref[pl.ds(c, heads, stride=hd), :] = o * inv
    pc.drain()


def msa_call(n, mask, mt, z, wb, wqkvg, wo, wq2, wkv, wg2):
    nseq, chan, nres = mt.shape
    rows = z.shape[0]
    heads = wb.shape[0]
    dma = pltpu.SemaphoreType.DMA((n,))
    dma9 = pltpu.SemaphoreType.DMA((9,))
    args = [pltpu.with_memory_space_constraint(v, pltpu.HBM) for v in (z, wb, mask, mt, wqkvg, wo, wq2, wkv, wg2)]
    return pl.pallas_call(
        functools.partial(msa_kernel, n, len(args)),
        name="msa",
        out_shape=[jax.ShapeDtypeStruct((nseq, chan, nres), BF), jax.ShapeDtypeStruct((nseq // 2, chan, 2 * nres), BF),
                   jax.ShapeDtypeStruct((chan, nres), F32)],
        in_specs=[pl.BlockSpec(memory_space=pltpu.HBM)] * len(args),
        out_specs=[VM] * 3,
        scratch_shapes=[pltpu.VMEM(v.shape, v.dtype) for v in args] + [
            dma9,
            pltpu.VMEM((heads, n * rows, nres), BF),
            pltpu.VMEM((nres, heads * nres), F32),
            pltpu.VMEM((heads * (rows + 8), nres), F32),
            pltpu.VMEM((nseq, wkv.shape[0], nres), F32),
            pltpu.VMEM((nseq, heads, nres), F32),
            pltpu.VMEM((chan, chan), BF),
            pltpu.VMEM((n, chan, nres), F32),
            pltpu.VMEM((n, chan + 16, nres), F32),
            pltpu.VMEM((chan, nres), F32),
            pltpu.VMEM((nseq, chan, nres), BF),
            pltpu.VMEM((nseq // 2, chan, 2 * nres), BF),
            pltpu.VMEM((nseq, nres, nres), BF),
            pltpu.VMEM((nseq, chan, 2 * nres), BF),
            pltpu.VMEM((nseq, chan, nres), BF),
            pltpu.VMEM((nseq // 2, chan, 2 * nres), BF),
            pltpu.VMEM((heads, nres, 2 * nres), F32),
            pltpu.VMEM((heads, 8, 2 * nres), F32),
            pltpu.VMEM((heads, nres, 2 * nres), BF),
            pltpu.VMEM((heads, 8, 2 * nres), F32),
            pltpu.VMEM((nseq // 2, chan, 2 * nres), F32),
            dma, dma, dma9, dma9, dma9, dma9,
        ],
        compiler_params=pltpu.CompilerParams(vmem_limit_bytes=36 * 2 ** 20, collective_id=0, has_side_effects=True),
    )(*args)


def gate_kernel(m1_ref, g2_ref, o2_ref, wo_ref, m2_ref, x_ref, wot):
    nseq, chan, nres = m1_ref.shape
    wot[:] = wo_ref[:].astype(F32).T.astype(BF)

    def gate(t):
        y = (sigmoid(g2_ref[t].astype(F32)) * cat(o2_ref[:], o2_ref[:])).astype(BF)
        m2 = (cat(m1_ref[2 * t].astype(F32), m1_ref[2 * t + 1].astype(F32)) + dot(wot[:], y)).astype(BF)
        for s in range(2):
            m2_ref[2 * t + s] = m2[:, part(s, nres)]
    loop(nseq // 2, gate, 4)

    def renorm(t):
        x_ref[t] = norm(cat(m2_ref[2 * t].astype(F32), m2_ref[2 * t + 1].astype(F32)), 0)
    loop(nseq // 2, renorm, 2)


def gate_call(m1, g2, o2, wo):
    nseq, chan, nres = m1.shape
    return pl.pallas_call(
        gate_kernel,
        name="gate",
        out_shape=[jax.ShapeDtypeStruct(m1.shape, BF), jax.ShapeDtypeStruct(g2.shape, BF)],
        in_specs=[VM] * 4,
        out_specs=[VM] * 2,
        scratch_shapes=[pltpu.VMEM((chan, chan), BF)],
        compiler_params=pltpu.CompilerParams(vmem_limit_bytes=16 * 2 ** 20),
    )(m1, g2, o2, wo)


def tri_attend(pc, zin, wb_ref, wqkvg_ref, wo_ref, maskcol, zln, brow, ball, bias, proj, flat, wot, lbuf, mbuf, pbuf, rbuf, obuf, zrel, tsend, zrecv,
               ssem_b, rsem_b, ssem_t, rsem_t):
    me = pc.me
    rows, nres, chan = zin.shape
    heads = wb_ref.shape[0]
    hd = chan // heads
    scale = hd ** -0.5
    pitch = rows + 8
    mine = ds8(me * rows, rows, 16)

    def bias_row(i):
        zl = norm(zin[i].astype(F32), 1)
        zln[i] = zl
        brow[pl.ds(i, heads, stride=pitch), :] = dot_nt(wb_ref[:], zl)
    loop(rows, bias_row, 4)
    for h in range(heads):
        ball[h, mine, :] = brow[h * pitch:h * pitch + rows, :].astype(BF)

    def bslot(dev):
        return ball.at[:, ds8(dev * rows, rows, 16), :]

    pc.to_all(bslot(me), bslot, ssem_b, rsem_b)
    wot[:] = wo_ref[:].astype(F32).T.astype(BF)

    def project(i):
        zl = zln[i]
        proj[i, :chan, :] = dot_nt(wqkvg_ref[:chan, :], zl).astype(BF)
        proj[i, chan:2 * chan, :] = dot_nt(zl, wqkvg_ref[chan:2 * chan, :]).astype(BF)
        proj[i, 2 * chan:4 * chan, :] = dot_nt(wqkvg_ref[2 * chan:4 * chan, :], zl).astype(BF)
    loop(rows, project, 2)
    pc.from_all(bslot, rsem_b)
    for h in range(heads):
        bias[:, h * nres:(h + 1) * nres] = (ball[h].astype(F32).T + maskcol[:]) * LOG2E
    zero = jnp.zeros((hd, nres), BF)

    half = heads // 2
    wide = 2 * nres

    def qk(i, p, u):
        r0 = 2 * hd * p
        qa = proj[i, r0:r0 + hd, :]
        qb = proj[i, r0 + hd:r0 + 2 * hd, :]
        parts = [jnp.zeros((r0, wide), BF)] if p > 0 else []
        parts.append(jnp.concatenate([qa, zero], axis=1))
        parts.append(jnp.concatenate([zero, qb], axis=1))
        if chan - r0 - 2 * hd > 0:
            parts.append(jnp.zeros((chan - r0 - 2 * hd, wide), BF))
        l = dot(proj[i, chan:2 * chan, :], jnp.concatenate(parts, axis=0)) * (scale * LOG2E) + bias[:, wide * p:wide * p + wide]
        lbuf[u] = l
        mbuf[u, 0:1, :] = jnp.max(l, axis=0, keepdims=True)

    def ex(u):
        e = jnp.exp2(lbuf[u] - mbuf[u, 0:1, :])
        pbuf[u] = e.astype(BF)
        rbuf[u, 0:1, :] = 1.0 / jnp.sum(e, axis=0, keepdims=True)

    def pv(i, p, u):
        r0 = 2 * hd * p
        o = dot(proj[i, 2 * chan + r0:2 * chan + r0 + 2 * hd, :], pbuf[u])
        obuf[i, r0:r0 + hd, :] = o[:hd, :nres] * rbuf[u, 0:1, :nres]
        obuf[i, r0 + hd:r0 + 2 * hd, :] = o[hd:, nres:] * rbuf[u, 0:1, nres:]

    units = [(i, p) for i in range(2) for p in range(half)]
    for u, (i, p) in enumerate(units):
        qk(i, p, u)

    def attend(t):
        nxt = jnp.minimum(2 * t + 2, rows - 2)
        for u, (i, p) in enumerate(units):
            ex(u)
            qk(nxt + i, p, u)
            if u > 0:
                pv(2 * t + units[u - 1][0], units[u - 1][1], u - 1)
        pv(2 * t + units[-1][0], units[-1][1], len(units) - 1)
    loop(rows // 2, attend)

    def finish(i):
        y = (sigmoid(proj[i, 3 * chan:4 * chan, :].astype(F32)) * obuf[i]).astype(BF)
        upd = dot(wot[:], y).T
        flat[pl.ds(i, nres, stride=pitch), :] = zin[i].astype(F32) + upd
    loop(rows, finish, 4)

    def regroup(j):
        tsend[j] = flat[ds8(j * pitch, rows), :].astype(BF)
    loop(nres, regroup, 4)

    def tblk(dev):
        return tsend.at[pl.ds(dev * rows, rows)]

    def tslot(dev):
        return zrecv.at[:, ds8(dev * rows, rows, 16), :]

    pc.scatter(tblk, tslot, zrel, ssem_t, rsem_t)
    zrecv[:, mine, :] = tsend[pl.ds(me * rows, rows)]
    pc.scatter_relay(tslot, zrel, ssem_t, rsem_t)
    pc.scatter_wait(tslot, rsem_t)


def pair_kernel(n, nchunk, mask_ref, x_ref, z_ref, rm_ref, wproj_ref, wopm_ref, wb1_ref, wqkvg1_ref, wo1_ref, wb2_ref, wqkvg2_ref, wo2_ref,
                zo_ref,
                ac, at, w32, wt, cbuf, asend, csend, call, apack, arel, aall, upd, osc, z1, zln, brow, ball1, ball2, bias, proj, flat, wot,
                lbuf, mbuf, pbuf, rbuf, obuf, maskcol, tsend1, tsend2, zrel1, zrel2, zmid, zfin,
                ssem_a, rsem_a, ssem_c, rsem_c, ssem_b1, rsem_b1, ssem_t1, rsem_t1, ssem_b2, rsem_b2, ssem_t2, rsem_t2):
    pc = Place(n)
    me = pc.me
    pc.signal()
    rows, nres, chan = z_ref.shape
    nf, nseq = csend.shape[0:2]
    ne = nf
    fq = nf // nchunk
    hq = fq // 2
    lane = lax.broadcasted_iota(jnp.int32, (nres, nres), 1)
    pitch = ac.shape[0] // nseq
    pitch2 = at.shape[0] // nres

    def project(t):
        pr = rnd(dot(wproj_ref[:], x_ref[t]))
        for s in range(2):
            mk = mask_ref[pl.ds(me * nseq + 2 * t + s, 1), :].astype(F32)
            ac[ds8((2 * t + s) * pitch, 2 * ne), :] = pr[:, part(s, nres)] * mk
    loop(nseq // 2, project, 4)
    pad = jnp.zeros((nres - nseq, nres), F32)

    def plane(e):
        at[pl.ds(e, nres, stride=pitch2), :] = stack(ac[pl.ds(e, nseq, stride=pitch), :], pad).T
    loop(ne, plane, 4)
    blocks = rows * ne // nres
    per = nres // ne

    def pack(d):
        v = [stack(*[at[ds8((d * rows + b * per + u) * pitch2, ne), :] for u in range(per)]) for b in range(blocks)]
        for r in range(blocks - 1):
            asend[d, part(r, nres), :] = jnp.where(lane >= nseq, pltpu.roll(v[-1], nseq - r * (nres - nseq), 1), v[r]).astype(BF)
    loop(n, pack)
    pc.meet()

    def aslot(dev):
        return apack.at[dev]

    pc.scatter(lambda dev: asend.at[dev], aslot, arel, ssem_a, rsem_a)

    def cslots(q):
        def slot(lo, size):
            return lambda dev: call.at[pl.ds(q * fq + lo, size), dev, :nseq, :]
        return slot(0, fq), slot(0, hq), slot(hq, hq)

    def own(q):
        for f in range(q * fq, q * fq + fq):
            v = ac[pl.ds(ne + f, nseq, stride=pitch), :].astype(BF)
            csend[f] = v
            call[f, me, :nseq, :] = v
        pc.spread(csend.at[pl.ds(q * fq, fq)], cslots(q)[0], ssem_c.at[q], rsem_c.at[q])

    def neighbours(q):
        pc.spread_relay(*cslots(q), ssem_c.at[q], rsem_c.at[q])
        if q + 2 < nchunk:
            own(q + 2)

    own(0)
    own(1)
    apack[me] = asend[me]
    pc.scatter_relay(aslot, arel, ssem_a, rsem_a)
    neighbours(0)
    padz = jnp.zeros((call.shape[1], call.shape[2] - nseq, nres), BF)

    def fill(f):
        call[f, :, nseq:, :] = padz
    loop(nf, fill)
    maskcol[:] = jnp.broadcast_to((rm_ref[:].astype(F32) - 1.0) * 1e4, (nres, nres)).T
    mbf = mask_ref[:].astype(F32).astype(BF)
    cbuf[:] = lax.dot_general(mbf, mbf, (((0,), (0,)), ((), ())), preferred_element_type=F32)
    w32[:] = wopm_ref[:].astype(F32)
    for g in range(nf // per):
        wt[:, part(g, nres)] = stack(*[w32[pl.ds(g * per + u, ne, stride=nf), :] for u in range(per)]).T.astype(BF)
    neighbours(1)
    pc.scatter_wait(aslot, rsem_a)

    def unpack(d):
        last = jnp.zeros((nres, nres), F32)
        for r in range(blocks - 1):
            v = apack[d, part(r, nres), :].astype(F32)
            aall[d, part(r, nres), :] = jnp.where(lane < nseq, v, 0.0).astype(BF)
            moved = pltpu.roll(v, (r + 1) * (nres - nseq), 1)
            last = last + jnp.where((lane >= r * (nres - nseq)) & (lane < (r + 1) * (nres - nseq)), moved, 0.0)
        aall[d, part(blocks - 1, nres), :] = last.astype(BF)
    loop(n, unpack)

    for q in range(nchunk):
        pc.spread_wait(*cslots(q), ssem_c.at[q], rsem_c.at[q])

        def outer(g):
            acc = None
            for kk in range(n // 2):
                rhs = jnp.concatenate(
                    [jnp.concatenate([call[q * fq + 2 * g + u, 2 * kk], call[q * fq + 2 * g + u, 2 * kk + 1]], axis=0) for u in range(2)],
                    axis=1)
                lhs = jnp.concatenate([aall[2 * kk], aall[2 * kk + 1]], axis=1)
                step = dot(lhs, rhs)
                acc = step if acc is None else acc + step
            ob = acc.astype(BF)
            for u in range(2):
                for i in range(rows):
                    osc[i, ds8((2 * g + u) * ne, ne, 32), :] = ob[i * ne:(i + 1) * ne, u * nres:(u + 1) * nres]
        loop(fq // 2, outer)

        def contract(g):
            rhs = jnp.concatenate([osc[2 * g], osc[2 * g + 1]], axis=1)
            step = dot(wt[:, part(q, fq * ne)], rhs)
            for u in range(2):
                v = step[:, part(u, nres)]
                upd[2 * g + u] = v if q == 0 else upd[2 * g + u] + v
        loop(rows // 2, contract, 2)
        if q + 2 < nchunk:
            neighbours(q + 2)

    def residual(i):
        u = upd[i] / (1e-3 + cbuf[pl.ds(me * rows + i, 1), :])
        z1[i] = (z_ref[i].astype(F32) + u.T).astype(BF)
    loop(rows, residual, 2)

    for zin, wb, wq, wo, ball, ts, zrel, zout, sems in (
            (z1, wb1_ref, wqkvg1_ref, wo1_ref, ball1, tsend1, zrel1, zmid, (ssem_b1, rsem_b1, ssem_t1, rsem_t1)),
            (zmid, wb2_ref, wqkvg2_ref, wo2_ref, ball2, tsend2, zrel2, zfin, (ssem_b2, rsem_b2, ssem_t2, rsem_t2))):
        tri_attend(pc, zin, wb, wq, wo, maskcol, zln, brow, ball, bias, proj, flat, wot, lbuf, mbuf, pbuf, rbuf, obuf, zrel, ts, zout, *sems)
    zo_ref[:] = zfin[:]
    pc.drain()


def pair_call(n, mask, x, z, rm, wproj, wopm, wb1, wqkvg1, wo1, wb2, wqkvg2, wo2):
    rows, nres, chan = z.shape
    nseq = 2 * x.shape[0]
    ne = wproj.shape[0] // 2
    heads = wb1.shape[0]
    nchunk = 4
    fq = ne // nchunk
    dma = pltpu.SemaphoreType.DMA((n,))
    dma9 = pltpu.SemaphoreType.DMA((9,))
    dmac = pltpu.SemaphoreType.DMA((nchunk, 9))
    pitch = rows + 8
    vz = pltpu.VMEM((rows, nres, chan), BF)
    fz = pltpu.VMEM((rows, chan, nres), F32)
    sq = pltpu.VMEM((nres, nres), F32)
    vb = pltpu.VMEM((heads, n * rows, nres), BF)
    vt = pltpu.VMEM((nres, rows, chan), BF)
    vr = pltpu.VMEM((2, rows, rows, chan), BF)
    apk = rows * ne * nseq // nres
    row8 = pltpu.VMEM((heads, 8, 2 * nres), F32)
    args = (mask, x, z, rm, wproj, wopm, wb1, wqkvg1, wo1, wb2, wqkvg2, wo2)
    return pl.pallas_call(
        functools.partial(pair_kernel, n, nchunk),
        name="pair",
        out_shape=jax.ShapeDtypeStruct(z.shape, BF),
        in_specs=[VM] * len(args),
        out_specs=VM,
        scratch_shapes=[
            pltpu.VMEM((nseq * (2 * ne + 8), nres), F32),
            pltpu.VMEM((nres * (ne + 8), nres), F32),
            pltpu.VMEM(wopm.shape, F32),
            pltpu.VMEM(wopm.shape[::-1], BF),
            sq,
            pltpu.VMEM((n, apk, nres), BF),
            pltpu.VMEM((ne, nseq, nres), BF),
            pltpu.VMEM((ne, n, nres, nres), BF),
            pltpu.VMEM((n, apk, nres), BF),
            pltpu.VMEM((2, apk, nres), BF),
            pltpu.VMEM((n, rows * ne, nres), BF),
            fz,
            pltpu.VMEM((rows, fq * ne, nres), BF),
            vz, vz,
            pltpu.VMEM((heads * pitch, nres), F32),
            vb, vb,
            pltpu.VMEM((nres, heads * nres), F32),
            pltpu.VMEM((rows, 4 * chan, nres), BF),
            pltpu.VMEM((nres * pitch, chan), F32),
            pltpu.VMEM((chan, chan), BF),
            pltpu.VMEM((heads, nres, 2 * nres), F32), row8, pltpu.VMEM((heads, nres, 2 * nres), BF), row8,
            fz, sq, vt, vt, vr, vr, vz, vz,
            dma9, dma9, dmac, dmac, dma, dma, dma9, dma9, dma, dma, dma9, dma9,
        ],
        compiler_params=pltpu.CompilerParams(vmem_limit_bytes=40 * 2 ** 20, collective_id=1, has_side_effects=True),
    )(*args)


def flat_t(w):
    return jnp.moveaxis(w, 0, -1).reshape(-1, w.shape[0])


def solution(mesh):
    n = mesh.shape["dap"]

    def block(msa, pair, msa_mask, res_mask, row_bias_w, row_qkvg_w, row_out_w, col_query_w, col_kv_w, col_gate_w, col_out_w,
              opm_proj_w, opm_out_w, start_bias_w, start_qkvg_w, start_out_w, end_bias_w, end_qkvg_w, end_out_w):
        nseq, nres, chan = msa.shape
        pdim = pair.shape[2]
        mt = jnp.transpose(msa, (0, 2, 1))
        m1, g2, o2 = msa_call(n, msa_mask, mt, pair, row_bias_w.T, flat_t(row_qkvg_w), row_out_w.reshape(chan, chan),
                              flat_t(col_query_w), flat_t(col_kv_w), flat_t(col_gate_w))
        m2, x3 = gate_call(m1, g2, o2, col_out_w.reshape(chan, chan))
        zo = pair_call(n, msa_mask, x3, pair, res_mask.reshape(1, nres), flat_t(opm_proj_w), opm_out_w.reshape(-1, pdim),
                       start_bias_w.T, flat_t(start_qkvg_w), start_out_w.reshape(pdim, pdim),
                       end_bias_w.T, flat_t(end_qkvg_w), end_out_w.reshape(pdim, pdim))
        return jnp.transpose(m2, (0, 2, 1)), zo

    row_spec = P(('data', 'dap'), None, None)
    in_specs = (row_spec, row_spec, P('data', None), P('data')) + (P(),) * 15
    return jax.shard_map(block, mesh=mesh, in_specs=in_specs, out_specs=(row_spec, row_spec), check_vma=False)
```

```python
import functools
import math

import jax
import jax.numpy as jnp
import numpy as np
from jax import lax
from jax.experimental import pallas as pl
from jax.experimental.pallas import tpu as pltpu
from jax.sharding import PartitionSpec as P

BF = jnp.bfloat16
F32 = jnp.float32
MESH = pl.DeviceIdType.MESH
LOG2E = math.log2(math.e)
VM = pl.BlockSpec(memory_space=pltpu.VMEM)


def dot(a, b):
    return lax.dot_general(a, b, (((1,), (0,)), ((), ())), preferred_element_type=F32)


def dot_nt(a, b):
    return lax.dot_general(a, b, (((1,), (1,)), ((), ())), preferred_element_type=F32)


def rnd(v):
    return v.astype(BF).astype(F32)


def norm(v, axis):
    mean = jnp.mean(v, axis=axis, keepdims=True)
    cen = v - mean
    var = jnp.mean(cen * cen, axis=axis, keepdims=True)
    return (cen * lax.rsqrt(var + 1e-5)).astype(BF)


def peak(v):
    return jnp.max(v, axis=0, keepdims=True)


def total(v):
    return jnp.sum(v, axis=0, keepdims=True)


def sigmoid(v):
    return 1.0 / (1.0 + jnp.exp(-v))


def split3(value):
    hi = float(np.asarray(value).astype(BF))
    mid = float(np.asarray(value - hi).astype(BF))
    return hi, mid, float(np.asarray(value - hi - mid).astype(BF))


def rcopy(src, dst, ssem, rsem, dev):
    return pltpu.make_async_remote_copy(src_ref=src, dst_ref=dst, send_sem=ssem, recv_sem=rsem, device_id={"dap": dev}, device_id_type=MESH)


def loop(count, body, unroll=1):
    lax.fori_loop(0, count, lambda t, c: (body(t), c)[-1], 0, unroll=unroll)


def cat(*v):
    return jnp.concatenate(v, axis=-1)


def stack(*v):
    return jnp.concatenate(v, axis=0)


def part(s, width):
    return slice(s * width, s * width + width)


class Place:
    def __init__(self, n):
        nx = n // 2
        self.n, self.me = n, lax.axis_index("dap")
        x, self.k = lax.div(self.me, 2), lax.rem(self.me, 2)
        self.rightc, self.leftc, self.farc = (lax.rem(x + d, nx) * 2 for d in (1, nx - 1, 2))
        self.right, self.left, self.far = (c + self.k for c in (self.rightc, self.leftc, self.farc))
        self.partner = self.other(self.me)
        self.sends = []

    def other(self, dev):
        return dev + 1 - 2 * self.k

    def signal(self):
        sem = pltpu.get_barrier_semaphore()
        for d in range(1, self.n):
            pl.semaphore_signal(sem, inc=1, device_id={"dap": lax.rem(self.me + d, self.n)}, device_id_type=MESH)

    def meet(self):
        pl.semaphore_wait(pltpu.get_barrier_semaphore(), self.n - 1)

    def go(self, src, dst, ssem, rsem, dev):
        cp = rcopy(src, dst, ssem, rsem, dev)
        cp.start()
        self.sends.append(cp)

    def got(self, dst, rsem):
        rcopy(dst, dst, rsem, rsem, self.me).wait_recv()

    def drain(self):
        for cp in self.sends:
            cp.wait_send()

    def to_all(self, src, slot, ssem, rsem):
        for d in sorted(range(1, self.n), key=lambda d: -min(d, self.n - d)):
            self.go(src, slot(self.me), ssem.at[d], rsem.at[d], lax.rem(self.me + d, self.n))

    def from_all(self, slot, rsem):
        for d in range(1, self.n):
            self.got(slot(lax.rem(self.me + self.n - d, self.n)), rsem.at[d])

    def scatter(self, blk, slot, rel, ssem, rsem):
        k, me = self.k, self.me
        self.go(blk(self.farc), rel.at[0], ssem.at[0], rsem.at[0], self.right)
        self.go(blk(self.farc + 1), rel.at[1], ssem.at[1], rsem.at[1], self.left)
        for j in range(2):
            self.go(blk(self.rightc + j), slot(me), ssem.at[2 + j], rsem.at[2 + k], self.rightc + j)
            self.go(blk(self.leftc + j), slot(me), ssem.at[4 + j], rsem.at[4 + k], self.leftc + j)
        self.go(blk(self.partner), slot(me), ssem.at[6], rsem.at[6], self.partner)

    def scatter_relay(self, slot, rel, ssem, rsem):
        self.got(rel.at[0], rsem.at[0])
        self.go(rel.at[0], slot(self.left), ssem.at[7], rsem.at[7 + self.k], self.rightc)
        self.got(rel.at[1], rsem.at[1])
        self.go(rel.at[1], slot(self.right), ssem.at[8], rsem.at[7 + self.k], self.leftc + 1)

    def scatter_wait(self, slot, rsem):
        for j in range(2):
            self.got(slot(self.leftc + j), rsem.at[2 + j])
            self.got(slot(self.rightc + j), rsem.at[4 + j])
            self.got(slot(self.farc + j), rsem.at[7 + j])
        self.got(slot(self.partner), rsem.at[6])

    def spread(self, src, slot, ssem, rsem):
        for i, dev in enumerate((self.right, self.left, self.partner)):
            self.go(src, slot(self.me), ssem.at[i], rsem.at[i], dev)

    def spread_relay(self, slot, lower, upper, ssem, rsem):
        left, right = self.left, self.right
        self.got(slot(left), rsem.at[0])
        self.go(lower(left), lower(left), ssem.at[3], rsem.at[3], right)
        self.go(slot(left), slot(left), ssem.at[5], rsem.at[5], self.partner)
        self.got(slot(right), rsem.at[1])
        self.go(upper(right), upper(right), ssem.at[4], rsem.at[4], left)
        self.go(slot(right), slot(right), ssem.at[6], rsem.at[6], self.partner)

    def spread_wait(self, slot, lower, upper, ssem, rsem):
        for i, half in enumerate((lower, upper)):
            self.got(half(self.far), rsem.at[3 + i])
            self.go(half(self.far), half(self.far), ssem.at[7 + i], rsem.at[7 + i], self.partner)
        self.got(slot(self.partner), rsem.at[2])
        self.got(slot(self.other(self.left)), rsem.at[5])
        self.got(slot(self.other(self.right)), rsem.at[6])
        for i, half in enumerate((lower, upper)):
            self.got(half(self.other(self.far)), rsem.at[7 + i])


def ds8(start, size, unit=8):
    return pl.ds(pl.multiple_of(start, unit), size)


def msa_kernel(n, nin, *refs):
    inputs, outputs, held = refs[:nin], refs[nin:nin + 3], refs[nin + 3:2 * nin + 3]
    msa_body(n, inputs, held, *outputs, *refs[2 * nin + 3:])


def msa_body(n, inputs, held,
               m1_ref, g2_ref, o2_ref, isem,
               ball, bias, brow, kv, lg, wot, qpart, ppart, tmp, x2_ref, xbuf, klhs, qblk, vbuf, gbuf, lbuf, mbuf, pbuf, rbuf, obuf,
               ssem_b, rsem_b, ssem_q, rsem_q, ssem_p, rsem_p):
    pc = Place(n)
    me = pc.me
    pc.signal()
    loads = [pltpu.make_async_copy(a, b, isem.at[i]) for i, (a, b) in enumerate(zip(inputs, held))]
    for cp in loads:
        cp.start()
    z_ref, wb_ref, mask_ref, m_ref, wqkvg_ref, wo_ref, wq2_ref, wkv_ref, wg2_ref = held
    loads[0].wait()
    loads[1].wait()
    nseq, chan, nres = m_ref.shape
    rows = z_ref.shape[0]
    heads = wb_ref.shape[0]
    hd = chan // heads
    scale = hd ** -0.5
    base = me * nseq

    pitch = rows + 8

    def bias_row(i):
        b = dot_nt(wb_ref[:], norm(z_ref[i].astype(F32), 1))
        brow[pl.ds(i, heads, stride=pitch), :] = b
    loop(rows, bias_row, rows)
    mine = ds8(me * rows, rows, 16)
    for h in range(heads):
        ball[h, mine, :] = brow[h * pitch:h * pitch + rows, :].astype(BF)
    def bslot(dev):
        return ball.at[:, ds8(dev * rows, rows, 16), :]

    pc.meet()
    pc.to_all(bslot(me), bslot, ssem_b, rsem_b)
    for cp in loads[2:]:
        cp.wait()
    wot[:] = wo_ref[:].astype(F32).T.astype(BF)
    rid = lax.broadcasted_iota(jnp.int32, (16, 2 * nres), 0)
    lid = lax.broadcasted_iota(jnp.int32, (16, 2 * nres), 1)
    diag = (rid < 8) == (lid < nres)

    def lnorm(t):
        xbuf[t] = norm(jnp.concatenate([m_ref[2 * t].astype(F32), m_ref[2 * t + 1].astype(F32)], axis=1), 0)
    loop(nseq // 2, lnorm, 4)

    def project(t):
        s0 = t * 2
        proj = dot(wqkvg_ref[:], xbuf[t])
        gbuf[t] = proj[3 * chan:4 * chan, :].astype(BF)
        for s in range(2):
            sl = part(s, nres)
            mk = mask_ref[pl.ds(base + s0 + s, 1), :].astype(F32) - 1.0
            kaug = jnp.concatenate([proj[chan:2 * chan, sl], jnp.broadcast_to(mk, (nres - chan, nres))], axis=0)
            klhs[s0 + s] = kaug.T.astype(BF)
            vbuf[s0 + s] = proj[2 * chan:3 * chan, sl].astype(BF)
            for p in range(heads // 2):
                q16 = proj[16 * p:16 * p + 16, sl]
                qblk[s0 + s, 16 * p:16 * p + 16, :] = jnp.where(diag, jnp.concatenate([q16, q16], axis=1), 0.0).astype(BF)
    loop(nseq // 2, project, 8)
    pc.from_all(bslot, rsem_b)
    for h in range(heads):
        bias[:, part(h, nres)] = ball[h].astype(F32).T * LOG2E

    hi, mid, lo = split3(1e4 / scale)
    rid = lax.broadcasted_iota(jnp.int32, (16, 2 * nres), 0)
    lid = lax.broadcasted_iota(jnp.int32, (16, 2 * nres), 1)
    aug = jnp.where(rid == 0, hi, jnp.where(rid == 1, mid, jnp.where(rid == 2, lo, 0.0))).astype(BF)

    npair = nseq // 2
    half = heads // 2
    wide = 2 * nres

    def qk(t, u):
        s, p = u // half, u % half
        parts = []
        if p > 0:
            parts.append(jnp.zeros((16 * p, wide), BF))
        parts.append(qblk[t * 2 + s, 16 * p:16 * p + 16, :])
        if chan - 16 * p - 16 > 0:
            parts.append(jnp.zeros((chan - 16 * p - 16, wide), BF))
        parts.append(aug)
        l = dot(klhs[t * 2 + s, :, :chan + 16], jnp.concatenate(parts, axis=0)) * (scale * LOG2E) + bias[:, part(p, wide)]
        lbuf[u] = l
        mbuf[u, 0:1, :] = peak(l)

    def ex(u):
        e = jnp.exp2(lbuf[u] - mbuf[u, 0:1, :])
        pbuf[u] = e.astype(BF)
        rbuf[u, 0:1, :] = 1.0 / total(e)

    def pv(t, u):
        s, p = u // half, u % half
        o = dot(vbuf[t * 2 + s, 16 * p:16 * p + 16, :], pbuf[u])
        sl = part(s, nres)
        obuf[t, 16 * p:16 * p + 8, sl] = o[:8, :nres] * rbuf[u, 0:1, :nres]
        obuf[t, 16 * p + 8:16 * p + 16, sl] = o[8:16, nres:] * rbuf[u, 0:1, nres:]

    units = 2 * half
    for u in range(units):
        qk(0, u)

    def row_pair(t):
        tn = jnp.minimum(t + 1, npair - 1)
        for u in range(units):
            ex(u)
            qk(tn, u)
            if u > 0:
                pv(t, u - 1)
        pv(t, units - 1)
    loop(npair, row_pair, 2)

    def finish(t):
        s0 = t * 2
        mv = jnp.concatenate([m_ref[s0].astype(F32), m_ref[s0 + 1].astype(F32)], axis=1)
        y = (sigmoid(gbuf[t].astype(F32)) * obuf[t]).astype(BF)
        m1 = (mv + dot(wot[:], y)).astype(BF)
        for s in range(2):
            m1_ref[s0 + s] = m1[:, part(s, nres)]
    loop(npair, finish, 16)

    def renorm(t, acc):
        s0 = t * 2
        m1 = jnp.concatenate([m1_ref[s0].astype(F32), m1_ref[s0 + 1].astype(F32)], axis=1)
        x2 = norm(m1, 0)
        for s in range(2):
            sl = part(s, nres)
            x2_ref[s0 + s] = x2[:, sl]
            acc = acc + mask_ref[pl.ds(base + s0 + s, 1), :].astype(F32) * x2[:, sl].astype(F32)
        return acc
    qpart[me] = lax.fori_loop(0, npair, renorm, jnp.zeros((chan, nres), F32), unroll=2)

    halfq = chan // 2
    qslots = (lambda dev: qpart.at[dev]), (lambda dev: qpart.at[dev, :halfq]), (lambda dev: qpart.at[dev, halfq:])
    pc.spread(qpart.at[me], qslots[0], ssem_q, rsem_q)

    def keyval(t):
        s0 = t * 2
        xv = jnp.concatenate([x2_ref[s0], x2_ref[s0 + 1]], axis=1)
        kvp = rnd(dot(wkv_ref[:], xv))
        g2_ref[t] = dot(wg2_ref[:], xv).astype(BF)
        for s in range(2):
            kv[s0 + s] = kvp[:, part(s, nres)]
    loop(npair, keyval, 8)
    count = total(mask_ref[:].astype(F32)) + 1e-10
    pc.spread_relay(*qslots, ssem_q, rsem_q)
    pc.spread_wait(*qslots, ssem_q, rsem_q)
    tot = qpart[0]
    for d in range(1, n):
        tot = tot + qpart[d]
    tmp[:] = rnd(dot(wq2_ref[:], (tot / count).astype(BF)))
    qd = [tmp[pl.ds(d, heads, stride=hd), :] for d in range(hd)]
    unroll = 8

    def logit(t, mx):
        for u in range(unroll):
            s = t * unroll + u
            row = kv.at[s]
            l = qd[0] * row[0:1, :]
            for d in range(1, hd):
                l = l + qd[d] * row[d:d + 1, :]
            l = l * scale + (mask_ref[pl.ds(base + s, 1), :].astype(F32) - 1.0) * 1e4
            lg[s] = l
            mx = jnp.maximum(mx, l)
        return mx
    mx = lax.fori_loop(0, nseq // unroll, logit, jnp.full((heads, nres), -jnp.inf, F32))

    def weigh(t, carry):
        ssum, acc = carry
        acc = list(acc)
        for u in range(unroll):
            s = t * unroll + u
            row = kv.at[s]
            e = jnp.exp(lg[s] - mx)
            ssum = ssum + e
            eb = rnd(e)
            for d in range(hd):
                acc[d] = acc[d] + eb * row[hd + d:hd + d + 1, :]
        return ssum, tuple(acc)
    zero = jnp.zeros((heads, nres), F32)
    ssum, acc = lax.fori_loop(0, nseq // unroll, weigh, (zero, (zero,) * hd))
    ppart[me, :8, :] = mx
    ppart[me, 8:16, :] = ssum
    for d in range(hd):
        ppart[me, 16 + 8 * d:24 + 8 * d, :] = acc[d]
    halfp = 8 + chan // 2
    pslots = (lambda dev: ppart.at[dev]), (lambda dev: ppart.at[dev, :halfp]), (lambda dev: ppart.at[dev, halfp:])
    pc.spread(ppart.at[me], pslots[0], ssem_p, rsem_p)
    pc.spread_relay(*pslots, ssem_p, rsem_p)
    pc.spread_wait(*pslots, ssem_p, rsem_p)
    top = ppart[0, :8, :]
    for d in range(1, n):
        top = jnp.maximum(top, ppart[d, :8, :])
    fac = [jnp.exp(ppart[d, :8, :] - top) for d in range(n)]
    den = fac[0] * ppart[0, 8:16, :]
    for d in range(1, n):
        den = den + fac[d] * ppart[d, 8:16, :]
    inv = 1.0 / den
    for c in range(hd):
        o = fac[0] * ppart[0, 16 + 8 * c:24 + 8 * c, :]
        for d in range(1, n):
            o = o + fac[d] * ppart[d, 16 + 8 * c:24 + 8 * c, :]
        o2_ref[pl.ds(c, heads, stride=hd), :] = o * inv
    pc.drain()


def msa_call(n, mask, mt, z, wb, wqkvg, wo, wq2, wkv, wg2):
    nseq, chan, nres = mt.shape
    rows = z.shape[0]
    heads = wb.shape[0]
    dma = pltpu.SemaphoreType.DMA((n,))
    dma9 = pltpu.SemaphoreType.DMA((9,))
    args = [pltpu.with_memory_space_constraint(v, pltpu.HBM) for v in (z, wb, mask, mt, wqkvg, wo, wq2, wkv, wg2)]
    return pl.pallas_call(
        functools.partial(msa_kernel, n, len(args)),
        name="msa",
        out_shape=[jax.ShapeDtypeStruct((nseq, chan, nres), BF), jax.ShapeDtypeStruct((nseq // 2, chan, 2 * nres), BF),
                   jax.ShapeDtypeStruct((chan, nres), F32)],
        in_specs=[pl.BlockSpec(memory_space=pltpu.HBM)] * len(args),
        out_specs=[VM] * 3,
        scratch_shapes=[pltpu.VMEM(v.shape, v.dtype) for v in args] + [
            dma9,
            pltpu.VMEM((heads, n * rows, nres), BF),
            pltpu.VMEM((nres, heads * nres), F32),
            pltpu.VMEM((heads * (rows + 8), nres), F32),
            pltpu.VMEM((nseq, wkv.shape[0], nres), F32),
            pltpu.VMEM((nseq, heads, nres), F32),
            pltpu.VMEM((chan, chan), BF),
            pltpu.VMEM((n, chan, nres), F32),
            pltpu.VMEM((n, chan + 16, nres), F32),
            pltpu.VMEM((chan, nres), F32),
            pltpu.VMEM((nseq, chan, nres), BF),
            pltpu.VMEM((nseq // 2, chan, 2 * nres), BF),
            pltpu.VMEM((nseq, nres, nres), BF),
            pltpu.VMEM((nseq, chan, 2 * nres), BF),
            pltpu.VMEM((nseq, chan, nres), BF),
            pltpu.VMEM((nseq // 2, chan, 2 * nres), BF),
            pltpu.VMEM((heads, nres, 2 * nres), F32),
            pltpu.VMEM((heads, 8, 2 * nres), F32),
            pltpu.VMEM((heads, nres, 2 * nres), BF),
            pltpu.VMEM((heads, 8, 2 * nres), F32),
            pltpu.VMEM((nseq // 2, chan, 2 * nres), F32),
            dma, dma, dma9, dma9, dma9, dma9,
        ],
        compiler_params=pltpu.CompilerParams(vmem_limit_bytes=36 * 2 ** 20, collective_id=0, has_side_effects=True),
    )(*args)


def gate_kernel(m1_ref, g2_ref, o2_ref, wo_ref, m2_ref, x_ref, wot):
    nseq, chan, nres = m1_ref.shape
    wot[:] = wo_ref[:].astype(F32).T.astype(BF)

    def gate(t):
        y = (sigmoid(g2_ref[t].astype(F32)) * cat(o2_ref[:], o2_ref[:])).astype(BF)
        m2 = (cat(m1_ref[2 * t].astype(F32), m1_ref[2 * t + 1].astype(F32)) + dot(wot[:], y)).astype(BF)
        for s in range(2):
            m2_ref[2 * t + s] = m2[:, part(s, nres)]
    loop(nseq // 2, gate, 16)

    def renorm(t):
        x_ref[t] = norm(cat(m2_ref[2 * t].astype(F32), m2_ref[2 * t + 1].astype(F32)), 0)
    loop(nseq // 2, renorm, 2)


def gate_call(m1, g2, o2, wo):
    nseq, chan, nres = m1.shape
    return pl.pallas_call(
        gate_kernel,
        name="gate",
        out_shape=[jax.ShapeDtypeStruct(m1.shape, BF), jax.ShapeDtypeStruct(g2.shape, BF)],
        in_specs=[VM] * 4,
        out_specs=[VM] * 2,
        scratch_shapes=[pltpu.VMEM((chan, chan), BF)],
        compiler_params=pltpu.CompilerParams(vmem_limit_bytes=16 * 2 ** 20),
    )(m1, g2, o2, wo)


def tri_attend(pc, zin, wb_ref, wqkvg_ref, wo_ref, maskcol, zln, brow, ball, bias, proj, flat, wot, lbuf, mbuf, pbuf, rbuf, obuf, zrel, tsend, zrecv,
               ssem_b, rsem_b, ssem_t, rsem_t):
    me = pc.me
    rows, nres, chan = zin.shape
    heads = wb_ref.shape[0]
    hd = chan // heads
    scale = hd ** -0.5
    pitch = rows + 8
    mine = ds8(me * rows, rows, 16)

    def bias_row(i):
        zl = norm(zin[i].astype(F32), 1)
        zln[i] = zl
        brow[pl.ds(i, heads, stride=pitch), :] = dot_nt(wb_ref[:], zl)
    loop(rows, bias_row, rows)
    for h in range(heads):
        ball[h, mine, :] = brow[h * pitch:h * pitch + rows, :].astype(BF)

    def bslot(dev):
        return ball.at[:, ds8(dev * rows, rows, 16), :]

    pc.to_all(bslot(me), bslot, ssem_b, rsem_b)
    wot[:] = wo_ref[:].astype(F32).T.astype(BF)

    def project(i):
        zl = zln[i]
        proj[i, :chan, :] = dot_nt(wqkvg_ref[:chan, :], zl).astype(BF)
        proj[i, chan:2 * chan, :] = dot_nt(zl, wqkvg_ref[chan:2 * chan, :]).astype(BF)
        proj[i, 2 * chan:4 * chan, :] = dot_nt(wqkvg_ref[2 * chan:4 * chan, :], zl).astype(BF)
    loop(rows, project, 8)
    pc.from_all(bslot, rsem_b)
    for h in range(heads):
        bias[:, part(h, nres)] = (ball[h].astype(F32).T + maskcol[:]) * LOG2E
    zero = jnp.zeros((hd, nres), BF)

    half = heads // 2
    wide = 2 * nres

    def qk(i, p, u):
        r0 = 2 * hd * p
        qa = proj[i, r0:r0 + hd, :]
        qb = proj[i, r0 + hd:r0 + 2 * hd, :]
        parts = [jnp.zeros((r0, wide), BF)] if p > 0 else []
        parts.append(jnp.concatenate([qa, zero], axis=1))
        parts.append(jnp.concatenate([zero, qb], axis=1))
        if chan - r0 - 2 * hd > 0:
            parts.append(jnp.zeros((chan - r0 - 2 * hd, wide), BF))
        l = dot(proj[i, chan:2 * chan, :], jnp.concatenate(parts, axis=0)) * (scale * LOG2E) + bias[:, part(p, wide)]
        lbuf[u] = l
        mbuf[u, 0:1, :] = peak(l)

    def ex(u):
        e = jnp.exp2(lbuf[u] - mbuf[u, 0:1, :])
        pbuf[u] = e.astype(BF)
        rbuf[u, 0:1, :] = 1.0 / total(e)

    def pv(i, p, u):
        r0 = 2 * hd * p
        o = dot(proj[i, 2 * chan + r0:2 * chan + r0 + 2 * hd, :], pbuf[u])
        obuf[i, r0:r0 + hd, :] = o[:hd, :nres] * rbuf[u, 0:1, :nres]
        obuf[i, r0 + hd:r0 + 2 * hd, :] = o[hd:, nres:] * rbuf[u, 0:1, nres:]

    units = [(i, p) for i in range(2) for p in range(half)]
    for u, (i, p) in enumerate(units):
        qk(i, p, u)

    def attend(t):
        nxt = jnp.minimum(2 * t + 2, rows - 2)
        for u, (i, p) in enumerate(units):
            ex(u)
            qk(nxt + i, p, u)
            if u > 0:
                pv(2 * t + units[u - 1][0], units[u - 1][1], u - 1)
        pv(2 * t + units[-1][0], units[-1][1], len(units) - 1)
    def finish(i):
        y = (sigmoid(proj[i, 3 * chan:4 * chan, :].astype(F32)) * obuf[i]).astype(BF)
        upd = dot(wot[:], y).T
        flat[pl.ds(i, nres, stride=pitch), :] = zin[i].astype(F32) + upd
    hrow = rows // 2

    def tblk(h):
        return lambda dev: tsend.at[h, pl.ds(dev * rows, rows)]

    def tslot(h):
        return lambda dev: zrecv.at[:, ds8(dev * rows + h * hrow, hrow), :]

    for h in range(2):
        loop(rows // 4, lambda t: attend(t + h * (rows // 4)), 4)
        loop(hrow, lambda i: finish(i + h * hrow), 8)

        def regroup(j):
            tsend[h, j] = flat[ds8(j * pitch + h * hrow, hrow), :].astype(BF)
        loop(nres, regroup, 8)
        pc.scatter(tblk(h), tslot(h), zrel.at[h], ssem_t.at[h], rsem_t.at[h])
    for h in range(2):
        zrecv[:, ds8(me * rows + h * hrow, hrow), :] = tsend[h, pl.ds(me * rows, rows)]
        pc.scatter_relay(tslot(h), zrel.at[h], ssem_t.at[h], rsem_t.at[h])
    for h in range(2):
        pc.scatter_wait(tslot(h), rsem_t.at[h])


def pair_kernel(n, sizes, mask_ref, x_ref, z_ref, rm_ref, wproj_ref, wopm_ref, wb1_ref, wqkvg1_ref, wo1_ref, wb2_ref, wqkvg2_ref, wo2_ref,
                zo_ref,
                ac, at, w32, wt, cbuf, asend, csend, call, apack, arel, aall, upd, osc, z1, zln, brow, ball1, ball2, bias, proj, flat, wot,
                lbuf, mbuf, pbuf, rbuf, obuf, maskcol, tsend1, tsend2, zrel1, zrel2, zmid, zfin,
                ssem_a, rsem_a, ssem_c, rsem_c, ssem_b1, rsem_b1, ssem_t1, rsem_t1, ssem_b2, rsem_b2, ssem_t2, rsem_t2):
    pc = Place(n)
    me = pc.me
    pc.signal()
    rows, nres, chan = z_ref.shape
    nf, nseq = csend.shape[0:2]
    ne = nf
    nchunk = len(sizes)
    first = [sum(sizes[:q]) for q in range(nchunk)]
    lane = lax.broadcasted_iota(jnp.int32, (nres, nres), 1)
    pitch = ac.shape[0] // nseq
    pitch2 = at.shape[0] // nres

    def project(t):
        pr = rnd(dot(wproj_ref[:], x_ref[t]))
        for s in range(2):
            mk = mask_ref[pl.ds(me * nseq + 2 * t + s, 1), :].astype(F32)
            ac[ds8((2 * t + s) * pitch, 2 * ne), :] = pr[:, part(s, nres)] * mk
    loop(nseq // 2, project, 16)

    def cslots(q):
        def slot(lo, size):
            return lambda dev: call.at[pl.ds(first[q] + lo, size), dev, :nseq, :]
        hq = sizes[q] // 2
        return slot(0, sizes[q]), slot(0, hq), slot(hq, hq)

    def own(q):
        for f in range(first[q], first[q] + sizes[q]):
            v = ac[pl.ds(ne + f, nseq, stride=pitch), :].astype(BF)
            csend[f] = v
            call[f, me, :nseq, :] = v
        pc.spread(csend.at[pl.ds(first[q], sizes[q])], cslots(q)[0], ssem_c.at[q], rsem_c.at[q])

    def neighbours(q):
        pc.spread_relay(*cslots(q), ssem_c.at[q], rsem_c.at[q])
        if q + 2 < nchunk:
            own(q + 2)

    pc.meet()
    own(0)
    pad = jnp.zeros((nres - nseq, nres), F32)

    def plane(e):
        at[pl.ds(e, nres, stride=pitch2), :] = stack(ac[pl.ds(e, nseq, stride=pitch), :], pad).T
    loop(ne, plane, 8)
    blocks = rows * ne // nres
    per = nres // ne

    def pack(d):
        v = [stack(*[at[ds8((d * rows + b * per + u) * pitch2, ne), :] for u in range(per)]) for b in range(blocks)]
        for r in range(blocks - 1):
            asend[d, part(r, nres), :] = jnp.where(lane >= nseq, pltpu.roll(v[-1], nseq - r * (nres - nseq), 1), v[r]).astype(BF)
    loop(n, pack, 4)

    def aslot(dev):
        return apack.at[dev]

    pc.scatter(lambda dev: asend.at[dev], aslot, arel, ssem_a, rsem_a)

    own(1)
    apack[me] = asend[me]
    pc.scatter_relay(aslot, arel, ssem_a, rsem_a)
    neighbours(0)
    padz = jnp.zeros((call.shape[1], call.shape[2] - nseq, nres), BF)

    def fill(f):
        call[f, :, nseq:, :] = padz
    loop(nf, fill)
    maskcol[:] = jnp.broadcast_to((rm_ref[:].astype(F32) - 1.0) * 1e4, (nres, nres)).T
    mbf = mask_ref[:].astype(F32).astype(BF)
    cbuf[:] = lax.dot_general(mbf, mbf, (((0,), (0,)), ((), ())), preferred_element_type=F32)
    w32[:] = wopm_ref[:].astype(F32)
    for g in range(nf // per):
        wt[:, part(g, nres)] = stack(*[w32[pl.ds(g * per + u, ne, stride=nf), :] for u in range(per)]).T.astype(BF)
    neighbours(1)
    pc.scatter_wait(aslot, rsem_a)

    def unpack(d):
        last = jnp.zeros((nres, nres), F32)
        for r in range(blocks - 1):
            v = apack[d, part(r, nres), :].astype(F32)
            aall[d, part(r, nres), :] = jnp.where(lane < nseq, v, 0.0).astype(BF)
            moved = pltpu.roll(v, (r + 1) * (nres - nseq), 1)
            last = last + jnp.where((lane >= r * (nres - nseq)) & (lane < (r + 1) * (nres - nseq)), moved, 0.0)
        aall[d, part(blocks - 1, nres), :] = last.astype(BF)
    loop(n, unpack, 2)

    for q in range(nchunk):
        pc.spread_wait(*cslots(q), ssem_c.at[q], rsem_c.at[q])

        def outer(g):
            acc = None
            f = first[q] + 2 * g
            for kk in range(n // 2):
                rhs = cat(*[stack(call[f + u, 2 * kk], call[f + u, 2 * kk + 1]) for u in range(2)])
                step = dot(cat(aall[2 * kk], aall[2 * kk + 1]), rhs)
                acc = step if acc is None else acc + step
            ob = acc.astype(BF)
            for u in range(2):
                for i in range(rows):
                    osc[i, ds8((2 * g + u) * ne, ne, 32), :] = ob[part(i, ne), part(u, nres)]
        loop(sizes[q] // 2, outer, 2)
        depth = sizes[q] * ne

        def contract(g):
            step = dot(wt[:, first[q] * ne:first[q] * ne + depth], cat(osc[2 * g, :depth, :], osc[2 * g + 1, :depth, :]))
            for u in range(2):
                v = step[:, part(u, nres)]
                upd[2 * g + u] = v if q == 0 else upd[2 * g + u] + v
        loop(rows // 2, contract, 8)
        if 0 < q + 2 < nchunk:
            neighbours(q + 2)

    def residual(i):
        u = upd[i] / (1e-3 + cbuf[pl.ds(me * rows + i, 1), :])
        z1[i] = (z_ref[i].astype(F32) + u.T).astype(BF)
    loop(rows, residual, 8)

    for zin, wb, wq, wo, ball, ts, zrel, zout, sems in (
            (z1, wb1_ref, wqkvg1_ref, wo1_ref, ball1, tsend1, zrel1, zmid, (ssem_b1, rsem_b1, ssem_t1, rsem_t1)),
            (zmid, wb2_ref, wqkvg2_ref, wo2_ref, ball2, tsend2, zrel2, zfin, (ssem_b2, rsem_b2, ssem_t2, rsem_t2))):
        tri_attend(pc, zin, wb, wq, wo, maskcol, zln, brow, ball, bias, proj, flat, wot, lbuf, mbuf, pbuf, rbuf, obuf, zrel, ts, zout, *sems)
    zo_ref[:] = zfin[:]
    pc.drain()


def pair_call(n, mask, x, z, rm, wproj, wopm, wb1, wqkvg1, wo1, wb2, wqkvg2, wo2):
    rows, nres, chan = z.shape
    nseq = 2 * x.shape[0]
    ne = wproj.shape[0] // 2
    heads = wb1.shape[0]
    sizes = (8, 8, 8, 4, 4)
    dma = pltpu.SemaphoreType.DMA((n,))
    dma9 = pltpu.SemaphoreType.DMA((9,))
    dmac = pltpu.SemaphoreType.DMA((len(sizes), 9))
    pitch = rows + 8
    vz = pltpu.VMEM((rows, nres, chan), BF)
    fz = pltpu.VMEM((rows, chan, nres), F32)
    sq = pltpu.VMEM((nres, nres), F32)
    vb = pltpu.VMEM((heads, n * rows, nres), BF)
    vt = pltpu.VMEM((2, nres, rows // 2, chan), BF)
    vr = pltpu.VMEM((2, 2, rows, rows // 2, chan), BF)
    dma29 = pltpu.SemaphoreType.DMA((2, 9))
    apk = rows * ne * nseq // nres
    row8 = pltpu.VMEM((heads, 8, 2 * nres), F32)
    args = (mask, x, z, rm, wproj, wopm, wb1, wqkvg1, wo1, wb2, wqkvg2, wo2)
    return pl.pallas_call(
        functools.partial(pair_kernel, n, sizes),
        name="pair",
        out_shape=jax.ShapeDtypeStruct(z.shape, BF),
        in_specs=[VM] * len(args),
        out_specs=VM,
        scratch_shapes=[
            pltpu.VMEM((nseq * (2 * ne + 8), nres), F32),
            pltpu.VMEM((nres * (ne + 8), nres), F32),
            pltpu.VMEM(wopm.shape, F32),
            pltpu.VMEM(wopm.shape[::-1], BF),
            sq,
            pltpu.VMEM((n, apk, nres), BF),
            pltpu.VMEM((ne, nseq, nres), BF),
            pltpu.VMEM((ne, n, nres, nres), BF),
            pltpu.VMEM((n, apk, nres), BF),
            pltpu.VMEM((2, apk, nres), BF),
            pltpu.VMEM((n, rows * ne, nres), BF),
            fz,
            pltpu.VMEM((rows, sizes[0] * ne, nres), BF),
            vz, vz,
            pltpu.VMEM((heads * pitch, nres), F32),
            vb, vb,
            pltpu.VMEM((nres, heads * nres), F32),
            pltpu.VMEM((rows, 4 * chan, nres), BF),
            pltpu.VMEM((nres * pitch, chan), F32),
            pltpu.VMEM((chan, chan), BF),
            pltpu.VMEM((heads, nres, 2 * nres), F32), row8, pltpu.VMEM((heads, nres, 2 * nres), BF), row8,
            fz, sq, vt, vt, vr, vr, vz, vz,
            dma9, dma9, dmac, dmac, dma, dma, dma29, dma29, dma, dma, dma29, dma29,
        ],
        compiler_params=pltpu.CompilerParams(vmem_limit_bytes=40 * 2 ** 20, collective_id=1, has_side_effects=True),
    )(*args)


def flat_t(w):
    return jnp.moveaxis(w, 0, -1).reshape(-1, w.shape[0])


def solution(mesh):
    n = mesh.shape["dap"]

    def block(msa, pair, msa_mask, res_mask, row_bias_w, row_qkvg_w, row_out_w, col_query_w, col_kv_w, col_gate_w, col_out_w,
              opm_proj_w, opm_out_w, start_bias_w, start_qkvg_w, start_out_w, end_bias_w, end_qkvg_w, end_out_w):
        nseq, nres, chan = msa.shape
        pdim = pair.shape[2]
        mt = jnp.transpose(msa, (0, 2, 1))
        m1, g2, o2 = msa_call(n, msa_mask, mt, pair, row_bias_w.T, flat_t(row_qkvg_w), row_out_w.reshape(chan, chan),
                              flat_t(col_query_w), flat_t(col_kv_w), flat_t(col_gate_w))
        m2, x3 = gate_call(m1, g2, o2, col_out_w.reshape(chan, chan))
        zo = pair_call(n, msa_mask, x3, pair, res_mask.reshape(1, nres), flat_t(opm_proj_w), opm_out_w.reshape(-1, pdim),
                       start_bias_w.T, flat_t(start_qkvg_w), start_out_w.reshape(pdim, pdim),
                       end_bias_w.T, flat_t(end_qkvg_w), end_out_w.reshape(pdim, pdim))
        return jnp.transpose(m2, (0, 2, 1)), zo

    row_spec = P(('data', 'dap'), None, None)
    in_specs = (row_spec, row_spec, P('data', None), P('data')) + (P(),) * 15
    return jax.shard_map(block, mesh=mesh, in_specs=in_specs, out_specs=(row_spec, row_spec), check_vma=False)
```

```python
import functools
import math

import jax
import jax.numpy as jnp
import numpy as np
from jax import lax
from jax.experimental import pallas as pl
from jax.experimental.pallas import tpu as pltpu
from jax.sharding import PartitionSpec as P

BF = jnp.bfloat16
F32 = jnp.float32
MESH = pl.DeviceIdType.MESH
LOG2E = math.log2(math.e)
VM = pl.BlockSpec(memory_space=pltpu.VMEM)


def dot(a, b):
    return lax.dot_general(a, b, (((1,), (0,)), ((), ())), preferred_element_type=F32)


def dot_nt(a, b):
    return lax.dot_general(a, b, (((1,), (1,)), ((), ())), preferred_element_type=F32)


def rnd(v):
    return v.astype(BF).astype(F32)


def norm(v, axis):
    mean = jnp.mean(v, axis=axis, keepdims=True)
    cen = v - mean
    var = jnp.mean(cen * cen, axis=axis, keepdims=True)
    return (cen * lax.rsqrt(var + 1e-5)).astype(BF)


def peak(v):
    return jnp.max(v, axis=0, keepdims=True)


def total(v):
    return jnp.sum(v, axis=0, keepdims=True)


def sigmoid(v):
    return 1.0 / (1.0 + jnp.exp(-v))


def split3(value):
    hi = float(np.asarray(value).astype(BF))
    mid = float(np.asarray(value - hi).astype(BF))
    return hi, mid, float(np.asarray(value - hi - mid).astype(BF))


def rcopy(src, dst, ssem, rsem, dev):
    return pltpu.make_async_remote_copy(src_ref=src, dst_ref=dst, send_sem=ssem, recv_sem=rsem, device_id={"dap": dev}, device_id_type=MESH)


def loop(count, body, unroll=1):
    lax.fori_loop(0, count, lambda t, c: (body(t), c)[-1], 0, unroll=unroll)


def cat(*v):
    return jnp.concatenate(v, axis=-1)


def stack(*v):
    return jnp.concatenate(v, axis=0)


def part(s, width):
    return slice(s * width, s * width + width)


class Place:
    def __init__(self, n):
        nx = n // 2
        self.n, self.me = n, lax.axis_index("dap")
        x, self.k = lax.div(self.me, 2), lax.rem(self.me, 2)
        self.rightc, self.leftc, self.farc = (lax.rem(x + d, nx) * 2 for d in (1, nx - 1, 2))
        self.right, self.left, self.far = (c + self.k for c in (self.rightc, self.leftc, self.farc))
        self.partner = self.other(self.me)
        self.sends = []

    def other(self, dev):
        return dev + 1 - 2 * self.k

    def signal(self):
        sem = pltpu.get_barrier_semaphore()
        for d in range(1, self.n):
            pl.semaphore_signal(sem, inc=1, device_id={"dap": lax.rem(self.me + d, self.n)}, device_id_type=MESH)

    def meet(self):
        pl.semaphore_wait(pltpu.get_barrier_semaphore(), self.n - 1)

    def go(self, src, dst, ssem, rsem, dev):
        cp = rcopy(src, dst, ssem, rsem, dev)
        cp.start()
        self.sends.append(cp)

    def got(self, dst, rsem):
        rcopy(dst, dst, rsem, rsem, self.me).wait_recv()

    def drain(self):
        for cp in self.sends:
            cp.wait_send()

    def to_all(self, src, slot, ssem, rsem):
        for d in sorted(range(1, self.n), key=lambda d: -min(d, self.n - d)):
            self.go(src, slot(self.me), ssem.at[d], rsem.at[d], lax.rem(self.me + d, self.n))

    def from_all(self, slot, rsem):
        for d in range(1, self.n):
            self.got(slot(lax.rem(self.me + self.n - d, self.n)), rsem.at[d])

    def scatter(self, blk, slot, rel, ssem, rsem):
        k, me = self.k, self.me
        self.go(blk(self.farc), rel.at[0], ssem.at[0], rsem.at[0], self.right)
        self.go(blk(self.farc + 1), rel.at[1], ssem.at[1], rsem.at[1], self.left)
        for j in range(2):
            self.go(blk(self.rightc + j), slot(me), ssem.at[2 + j], rsem.at[2 + k], self.rightc + j)
            self.go(blk(self.leftc + j), slot(me), ssem.at[4 + j], rsem.at[4 + k], self.leftc + j)
        self.go(blk(self.partner), slot(me), ssem.at[6], rsem.at[6], self.partner)

    def scatter_relay(self, slot, rel, ssem, rsem):
        self.got(rel.at[0], rsem.at[0])
        self.go(rel.at[0], slot(self.left), ssem.at[7], rsem.at[7 + self.k], self.rightc)
        self.got(rel.at[1], rsem.at[1])
        self.go(rel.at[1], slot(self.right), ssem.at[8], rsem.at[7 + self.k], self.leftc + 1)

    def scatter_wait(self, slot, rsem):
        for j in range(2):
            self.got(slot(self.leftc + j), rsem.at[2 + j])
            self.got(slot(self.rightc + j), rsem.at[4 + j])
            self.got(slot(self.farc + j), rsem.at[7 + j])
        self.got(slot(self.partner), rsem.at[6])

    def spread(self, src, slot, ssem, rsem):
        for i, dev in enumerate((self.right, self.left, self.partner)):
            self.go(src, slot(self.me), ssem.at[i], rsem.at[i], dev)

    def spread_relay(self, slot, lower, upper, ssem, rsem, both=False):
        left, right = self.left, self.right
        for i, (dev, half, onward) in enumerate(((left, lower, right), (right, upper, left))):
            self.got(slot(dev), rsem.at[i])
            self.go(half(dev), half(dev), ssem.at[3 + i], rsem.at[3 + i], onward)
            if both:
                self.go(half(dev), half(dev), ssem.at[7 + i], rsem.at[7 + i], self.other(onward))
            self.go(slot(dev), slot(dev), ssem.at[5 + i], rsem.at[5 + i], self.partner)

    def spread_wait(self, slot, lower, upper, ssem, rsem, both=False):
        for i, half in enumerate((lower, upper)):
            self.got(half(self.far), rsem.at[3 + i])
            if not both:
                self.go(half(self.far), half(self.far), ssem.at[7 + i], rsem.at[7 + i], self.partner)
        self.got(slot(self.partner), rsem.at[2])
        self.got(slot(self.other(self.left)), rsem.at[5])
        self.got(slot(self.other(self.right)), rsem.at[6])
        for i, half in enumerate((lower, upper)):
            self.got(half(self.other(self.far)), rsem.at[7 + i])


def ds8(start, size, unit=8):
    return pl.ds(pl.multiple_of(start, unit), size)


def msa_kernel(n, nin, *refs):
    inputs, outputs, held = refs[:nin], refs[nin:nin + 3], refs[nin + 3:2 * nin + 3]
    msa_body(n, inputs, held, *outputs, *refs[2 * nin + 3:])


def msa_body(n, inputs, held,
               m1_ref, g2_ref, o2_ref, isem,
               ball, bias, brow, kv, lg, wot, qpart, ppart, tmp, x2_ref, xbuf, klhs, qblk, vbuf, gbuf, lbuf, mbuf, pbuf, rbuf, obuf,
               ssem_b, rsem_b, ssem_q, rsem_q, ssem_p, rsem_p):
    pc = Place(n)
    me = pc.me
    pc.signal()
    loads = [pltpu.make_async_copy(a, b, isem.at[i]) for i, (a, b) in enumerate(zip(inputs, held))]
    for cp in loads:
        cp.start()
    z_ref, wb_ref, mask_ref, m_ref, wqkvg_ref, wo_ref, wq2_ref, wkv_ref, wg2_ref = held
    loads[0].wait()
    loads[1].wait()
    nseq, chan, nres = m_ref.shape
    rows = z_ref.shape[0]
    heads = wb_ref.shape[0]
    hd = chan // heads
    scale = hd ** -0.5
    base = me * nseq

    pitch = rows + 8

    def bias_row(i):
        b = dot_nt(wb_ref[:], norm(z_ref[i].astype(F32), 1))
        brow[pl.ds(i, heads, stride=pitch), :] = b
    loop(rows, bias_row, rows)
    mine = ds8(me * rows, rows, 16)
    for h in range(heads):
        ball[h, mine, :] = brow[h * pitch:h * pitch + rows, :].astype(BF)
    def bslot(dev):
        return ball.at[:, ds8(dev * rows, rows, 16), :]

    pc.meet()
    pc.to_all(bslot(me), bslot, ssem_b, rsem_b)
    for cp in loads[2:]:
        cp.wait()
    wot[:] = wo_ref[:].astype(F32).T.astype(BF)
    rid = lax.broadcasted_iota(jnp.int32, (16, 2 * nres), 0)
    lid = lax.broadcasted_iota(jnp.int32, (16, 2 * nres), 1)
    diag = (rid < 8) == (lid < nres)

    def lnorm(t):
        xbuf[t] = norm(jnp.concatenate([m_ref[2 * t].astype(F32), m_ref[2 * t + 1].astype(F32)], axis=1), 0)
    loop(nseq // 2, lnorm, 4)

    def project(t):
        s0 = t * 2
        proj = dot(wqkvg_ref[:], xbuf[t])
        gbuf[t] = sigmoid(rnd(proj[3 * chan:, :]))
        for s in range(2):
            sl = part(s, nres)
            mk = mask_ref[pl.ds(base + s0 + s, 1), :].astype(F32) - 1.0
            kaug = jnp.concatenate([proj[chan:2 * chan, sl], jnp.broadcast_to(mk, (nres - chan, nres))], axis=0)
            klhs[s0 + s] = kaug.T.astype(BF)
            vbuf[s0 + s] = proj[2 * chan:3 * chan, sl].astype(BF)
            for p in range(heads // 2):
                q16 = proj[16 * p:16 * p + 16, sl]
                qblk[s0 + s, 16 * p:16 * p + 16, :] = jnp.where(diag, jnp.concatenate([q16, q16], axis=1), 0.0).astype(BF)
    loop(nseq // 2, project, 8)
    pc.from_all(bslot, rsem_b)
    for h in range(heads):
        bias[:, part(h, nres)] = ball[h].astype(F32).T * LOG2E

    hi, mid, lo = split3(1e4 / scale)
    rid = lax.broadcasted_iota(jnp.int32, (16, 2 * nres), 0)
    lid = lax.broadcasted_iota(jnp.int32, (16, 2 * nres), 1)
    aug = jnp.where(rid == 0, hi, jnp.where(rid == 1, mid, jnp.where(rid == 2, lo, 0.0))).astype(BF)

    npair = nseq // 2
    half = heads // 2
    wide = 2 * nres

    def qk(t, u):
        s, p = u // half, u % half
        parts = []
        if p > 0:
            parts.append(jnp.zeros((16 * p, wide), BF))
        parts.append(qblk[t * 2 + s, 16 * p:16 * p + 16, :])
        if chan - 16 * p - 16 > 0:
            parts.append(jnp.zeros((chan - 16 * p - 16, wide), BF))
        parts.append(aug)
        l = dot(klhs[t * 2 + s, :, :chan + 16], jnp.concatenate(parts, axis=0)) * (scale * LOG2E) + bias[:, part(p, wide)]
        lbuf[u] = l
        mbuf[u, 0:1, :] = peak(l)

    def ex(u):
        e = jnp.exp2(lbuf[u] - mbuf[u, 0:1, :])
        pbuf[u] = e.astype(BF)
        rbuf[u, 0:1, :] = 1.0 / total(e)

    def pv(t, u):
        s, p = u // half, u % half
        o = dot(vbuf[t * 2 + s, 16 * p:16 * p + 16, :], pbuf[u])
        sl = part(s, nres)
        obuf[t, 16 * p:16 * p + 8, sl] = o[:8, :nres] * rbuf[u, 0:1, :nres]
        obuf[t, 16 * p + 8:16 * p + 16, sl] = o[8:16, nres:] * rbuf[u, 0:1, nres:]

    units = 2 * half
    for u in range(units):
        qk(0, u)

    def row_pair(t):
        tn = jnp.minimum(t + 1, npair - 1)
        for u in range(units):
            ex(u)
            qk(tn, u)
            if u > 0:
                pv(t, u - 1)
        pv(t, units - 1)
    loop(npair, row_pair, 2)

    def finish(t):
        s0 = t * 2
        mv = jnp.concatenate([m_ref[s0].astype(F32), m_ref[s0 + 1].astype(F32)], axis=1)
        y = (gbuf[t] * obuf[t]).astype(BF)
        m1 = (mv + dot(wot[:], y)).astype(BF)
        for s in range(2):
            m1_ref[s0 + s] = m1[:, part(s, nres)]
    loop(npair, finish, 16)

    def renorm(t, acc):
        s0 = t * 2
        m1 = jnp.concatenate([m1_ref[s0].astype(F32), m1_ref[s0 + 1].astype(F32)], axis=1)
        x2 = norm(m1, 0)
        for s in range(2):
            sl = part(s, nres)
            x2_ref[s0 + s] = x2[:, sl]
            acc = acc + mask_ref[pl.ds(base + s0 + s, 1), :].astype(F32) * x2[:, sl].astype(F32)
        return acc
    qpart[me] = lax.fori_loop(0, npair, renorm, jnp.zeros((chan, nres), F32), unroll=2)

    halfq = chan // 2
    qslots = (lambda dev: qpart.at[dev]), (lambda dev: qpart.at[dev, :halfq]), (lambda dev: qpart.at[dev, halfq:])
    pc.spread(qpart.at[me], qslots[0], ssem_q, rsem_q)

    def keyval(t):
        s0 = t * 2
        xv = jnp.concatenate([x2_ref[s0], x2_ref[s0 + 1]], axis=1)
        kvp = rnd(dot(wkv_ref[:], xv))
        g2_ref[t] = sigmoid(rnd(dot(wg2_ref[:], xv)))
        for s in range(2):
            kv[s0 + s] = kvp[:, part(s, nres)]
    loop(npair, keyval, 8)
    count = total(mask_ref[:].astype(F32)) + 1e-10
    pc.spread_relay(*qslots, ssem_q, rsem_q, True)
    pc.spread_wait(*qslots, ssem_q, rsem_q, True)
    tot = qpart[0]
    for d in range(1, n):
        tot = tot + qpart[d]
    tmp[:] = rnd(dot(wq2_ref[:], (tot / count).astype(BF)))
    qd = [tmp[pl.ds(d, heads, stride=hd), :] for d in range(hd)]
    unroll = 8

    def logit(t, mx):
        for u in range(unroll):
            s = t * unroll + u
            row = kv.at[s]
            l = qd[0] * row[0:1, :]
            for d in range(1, hd):
                l = l + qd[d] * row[d:d + 1, :]
            l = l * scale + (mask_ref[pl.ds(base + s, 1), :].astype(F32) - 1.0) * 1e4
            lg[s] = l
            mx = jnp.maximum(mx, l)
        return mx
    mx = lax.fori_loop(0, nseq // unroll, logit, jnp.full((heads, nres), -jnp.inf, F32))

    def weigh(t, carry):
        ssum, acc = carry
        acc = list(acc)
        for u in range(unroll):
            s = t * unroll + u
            row = kv.at[s]
            e = jnp.exp(lg[s] - mx)
            ssum = ssum + e
            eb = rnd(e)
            for d in range(hd):
                acc[d] = acc[d] + eb * row[hd + d:hd + d + 1, :]
        return ssum, tuple(acc)
    zero = jnp.zeros((heads, nres), F32)
    ssum, acc = lax.fori_loop(0, nseq // unroll, weigh, (zero, (zero,) * hd))
    ppart[me, :8, :] = mx
    ppart[me, 8:16, :] = ssum
    for d in range(hd):
        ppart[me, 16 + 8 * d:24 + 8 * d, :] = acc[d]
    halfp = 8 + chan // 2
    pslots = (lambda dev: ppart.at[dev]), (lambda dev: ppart.at[dev, :halfp]), (lambda dev: ppart.at[dev, halfp:])
    pc.spread(ppart.at[me], pslots[0], ssem_p, rsem_p)
    pc.spread_relay(*pslots, ssem_p, rsem_p, True)
    pc.spread_wait(*pslots, ssem_p, rsem_p, True)
    top = ppart[0, :8, :]
    for d in range(1, n):
        top = jnp.maximum(top, ppart[d, :8, :])
    fac = [jnp.exp(ppart[d, :8, :] - top) for d in range(n)]
    den = fac[0] * ppart[0, 8:16, :]
    for d in range(1, n):
        den = den + fac[d] * ppart[d, 8:16, :]
    inv = 1.0 / den
    for c in range(hd):
        o = fac[0] * ppart[0, 16 + 8 * c:24 + 8 * c, :]
        for d in range(1, n):
            o = o + fac[d] * ppart[d, 16 + 8 * c:24 + 8 * c, :]
        o2_ref[pl.ds(c, heads, stride=hd), :] = o * inv
    pc.drain()


def msa_call(n, mask, mt, z, wb, wqkvg, wo, wq2, wkv, wg2):
    nseq, chan, nres = mt.shape
    rows = z.shape[0]
    heads = wb.shape[0]
    dma = pltpu.SemaphoreType.DMA((n,))
    dma9 = pltpu.SemaphoreType.DMA((9,))
    args = [pltpu.with_memory_space_constraint(v, pltpu.HBM) for v in (z, wb, mask, mt, wqkvg, wo, wq2, wkv, wg2)]
    return pl.pallas_call(
        functools.partial(msa_kernel, n, len(args)),
        name="msa",
        out_shape=[jax.ShapeDtypeStruct((nseq, chan, nres), BF), jax.ShapeDtypeStruct((nseq // 2, chan, 2 * nres), F32),
                   jax.ShapeDtypeStruct((chan, nres), F32)],
        in_specs=[pl.BlockSpec(memory_space=pltpu.HBM)] * len(args),
        out_specs=[VM] * 3,
        scratch_shapes=[pltpu.VMEM(v.shape, v.dtype) for v in args] + [
            dma9,
            pltpu.VMEM((heads, n * rows, nres), BF),
            pltpu.VMEM((nres, heads * nres), F32),
            pltpu.VMEM((heads * (rows + 8), nres), F32),
            pltpu.VMEM((nseq, wkv.shape[0], nres), F32),
            pltpu.VMEM((nseq, heads, nres), F32),
            pltpu.VMEM((chan, chan), BF),
            pltpu.VMEM((n, chan, nres), F32),
            pltpu.VMEM((n, chan + 16, nres), F32),
            pltpu.VMEM((chan, nres), F32),
            pltpu.VMEM((nseq, chan, nres), BF),
            pltpu.VMEM((nseq // 2, chan, 2 * nres), BF),
            pltpu.VMEM((nseq, nres, nres), BF),
            pltpu.VMEM((nseq, chan, 2 * nres), BF),
            pltpu.VMEM((nseq, chan, nres), BF),
            pltpu.VMEM((nseq // 2, chan, 2 * nres), F32),
            pltpu.VMEM((heads, nres, 2 * nres), F32),
            pltpu.VMEM((heads, 8, 2 * nres), F32),
            pltpu.VMEM((heads, nres, 2 * nres), BF),
            pltpu.VMEM((heads, 8, 2 * nres), F32),
            pltpu.VMEM((nseq // 2, chan, 2 * nres), F32),
            dma, dma, dma9, dma9, dma9, dma9,
        ],
        compiler_params=pltpu.CompilerParams(vmem_limit_bytes=38 * 2 ** 20, collective_id=0, has_side_effects=True),
    )(*args)


def gate_kernel(m1_ref, g2_ref, o2_ref, wo_ref, m2_ref, x_ref, wot, m2, sem):
    nseq, chan, nres = m1_ref.shape
    wot[:] = wo_ref[:].astype(F32).T.astype(BF)
    pieces = sem.shape[0]
    size = nseq // pieces

    def gate(t):
        y = (g2_ref[t] * cat(o2_ref[:], o2_ref[:])).astype(BF)
        m = (cat(m1_ref[2 * t].astype(F32), m1_ref[2 * t + 1].astype(F32)) + dot(wot[:], y)).astype(BF)
        for s in range(2):
            m2[2 * t + s] = m[:, part(s, nres)]

    def renorm(t):
        x_ref[t] = norm(cat(m2[2 * t].astype(F32), m2[2 * t + 1].astype(F32)), 0)
    copies = []
    for p in range(pieces):
        loop(size // 2, lambda t: gate(t + p * (size // 2)), size // 2)
        piece = pl.ds(p * size, size)
        copies.append(pltpu.make_async_copy(m2.at[piece], m2_ref.at[piece], sem.at[p]))
        copies[-1].start()
    loop(nseq // 2, renorm, 2)
    for cp in copies:
        cp.wait()


def gate_call(m1, g2, o2, wo):
    nseq, chan, nres = m1.shape
    return pl.pallas_call(
        gate_kernel,
        name="gate",
        out_shape=[jax.ShapeDtypeStruct(m1.shape, BF), jax.ShapeDtypeStruct(g2.shape, BF)],
        in_specs=[VM] * 4,
        out_specs=[pl.BlockSpec(memory_space=pltpu.HBM), VM],
        scratch_shapes=[pltpu.VMEM((chan, chan), BF), pltpu.VMEM(m1.shape, BF), pltpu.SemaphoreType.DMA((3,))],
        compiler_params=pltpu.CompilerParams(vmem_limit_bytes=16 * 2 ** 20),
    )(m1, g2, o2, wo)


def tri_attend(pc, early, zin, wb_ref, wqkvg_ref, wo_ref, maskcol, zln, brow, ball, bias, proj, gate, flat, wot, lbuf, mbuf, pbuf, rbuf, obuf, zrel, tsend, zrecv,
               ssem_b, rsem_b, ssem_t, rsem_t):
    me = pc.me
    rows, nres, chan = zin.shape
    heads = wb_ref.shape[0]
    hd = chan // heads
    scale = hd ** -0.5
    pitch = rows + 8
    mine = ds8(me * rows, rows, 16)

    def bslot(buf):
        return lambda dev: buf.at[:, ds8(dev * rows, rows, 16), :]

    def make_bias(src, w_ref, buf, ssem, rsem):
        def bias_row(i):
            zl = norm(src[i].astype(F32), 1)
            zln[i] = zl
            brow[pl.ds(i, heads, stride=pitch), :] = dot_nt(w_ref[:], zl)
        loop(rows, bias_row, rows)
        for h in range(heads):
            buf[h, mine, :] = brow[h * pitch:h * pitch + rows, :].astype(BF)
        pc.to_all(bslot(buf)(me), bslot(buf), ssem, rsem)

    if early:
        make_bias(zin, wb_ref, ball, ssem_b, rsem_b)
    else:
        def renorm(i):
            zln[i] = norm(zin[i].astype(F32), 1)
        loop(rows, renorm, 8)
    wot[:] = wo_ref[:].astype(F32).T.astype(BF)

    def project(i):
        zl = zln[i]
        proj[i, :chan, :] = dot_nt(wqkvg_ref[:chan, :], zl).astype(BF)
        proj[i, chan:2 * chan, :] = dot_nt(zl, wqkvg_ref[chan:2 * chan, :]).astype(BF)
        proj[i, 2 * chan:, :] = dot_nt(wqkvg_ref[2 * chan:3 * chan, :], zl).astype(BF)
        gate[i] = sigmoid(rnd(dot_nt(wqkvg_ref[3 * chan:, :], zl)))
    loop(rows, project, 8)
    pc.from_all(bslot(ball), rsem_b)
    for h in range(heads):
        b = ball[h].astype(F32)
        bias[:, part(h, nres)] = ((b.T if early else b) + maskcol[:]) * LOG2E
    zero = jnp.zeros((hd, nres), BF)

    half = heads // 2
    wide = 2 * nres

    def qk(i, p, u):
        r0 = 2 * hd * p
        qa = proj[i, r0:r0 + hd, :]
        qb = proj[i, r0 + hd:r0 + 2 * hd, :]
        parts = [jnp.zeros((r0, wide), BF)] if p > 0 else []
        parts.append(jnp.concatenate([qa, zero], axis=1))
        parts.append(jnp.concatenate([zero, qb], axis=1))
        if chan - r0 - 2 * hd > 0:
            parts.append(jnp.zeros((chan - r0 - 2 * hd, wide), BF))
        l = dot(proj[i, chan:2 * chan, :], jnp.concatenate(parts, axis=0)) * (scale * LOG2E) + bias[:, part(p, wide)]
        lbuf[u] = l
        mbuf[u, 0:1, :] = peak(l)

    def ex(u):
        e = jnp.exp2(lbuf[u] - mbuf[u, 0:1, :])
        pbuf[u] = e.astype(BF)
        rbuf[u, 0:1, :] = 1.0 / total(e)

    def pv(i, p, u):
        r0 = 2 * hd * p
        o = dot(proj[i, 2 * chan + r0:2 * chan + r0 + 2 * hd, :], pbuf[u])
        obuf[i, r0:r0 + hd, :] = o[:hd, :nres] * rbuf[u, 0:1, :nres]
        obuf[i, r0 + hd:r0 + 2 * hd, :] = o[hd:, nres:] * rbuf[u, 0:1, nres:]

    units = [(i, p) for i in range(2) for p in range(half)]
    for u, (i, p) in enumerate(units):
        qk(i, p, u)

    def attend(t):
        nxt = jnp.minimum(2 * t + 2, rows - 2)
        for u, (i, p) in enumerate(units):
            ex(u)
            qk(nxt + i, p, u)
            if u > 0:
                pv(2 * t + units[u - 1][0], units[u - 1][1], u - 1)
        pv(2 * t + units[-1][0], units[-1][1], len(units) - 1)
    def finish(i):
        y = (gate[i] * obuf[i]).astype(BF)
        upd = dot(wot[:], y).T
        zn = zin[i].astype(F32) + upd
        flat[pl.ds(i, nres, stride=pitch), :] = zn
        if early:
            zin[i] = zn.astype(BF)
    hrow = rows // 2

    def tblk(h):
        return lambda dev: tsend.at[h, pl.ds(dev * rows, rows)]

    def tslot(h):
        return lambda dev: zrecv.at[:, ds8(dev * rows + h * hrow, hrow), :]

    for h in range(2):
        loop(rows // 4, lambda t: attend(t + h * (rows // 4)), 4)
        loop(hrow, lambda i: finish(i + h * hrow), 8)

        def regroup(j):
            tsend[h, j] = flat[ds8(j * pitch + h * hrow, hrow), :].astype(BF)
        loop(nres, regroup, 8)
        pc.scatter(tblk(h), tslot(h), zrel.at[h], ssem_t.at[h], rsem_t.at[h])
    for h in range(2):
        pc.scatter_relay(tslot(h), zrel.at[h], ssem_t.at[h], rsem_t.at[h])
        if early and h == 0:
            make_bias(zin, *early)
        zrecv[:, ds8(me * rows + h * hrow, hrow), :] = tsend[h, pl.ds(me * rows, rows)]
    for h in range(2):
        pc.scatter_wait(tslot(h), rsem_t.at[h])


def pair_kernel(n, sizes, mask_ref, x_ref, z_ref, rm_ref, wproj_ref, wopm_ref, wb1_ref, wqkvg1_ref, wo1_ref, wb2_ref, wqkvg2_ref, wo2_ref,
                zo_ref,
                ac, at, w32, wt, cbuf, asend, csend, call, apack, arel, aall, upd, osc, z1, zln, brow, ball1, ball2, bias, proj, gate, flat, wot,
                lbuf, mbuf, pbuf, rbuf, obuf, maskcol, tsend1, tsend2, zrel1, zrel2, zmid, zfin,
                ssem_a, rsem_a, ssem_c, rsem_c, ssem_b1, rsem_b1, ssem_t1, rsem_t1, ssem_b2, rsem_b2, ssem_t2, rsem_t2):
    pc = Place(n)
    me = pc.me
    pc.signal()
    rows, nres, chan = z_ref.shape
    nf, nseq = csend.shape[0:2]
    ne = nf
    nchunk = len(sizes)
    first = [sum(sizes[:q]) for q in range(nchunk)]
    lane = lax.broadcasted_iota(jnp.int32, (nres, nres), 1)
    pitch = ac.shape[0] // nseq
    pitch2 = at.shape[0] // nres

    def project(t):
        pr = rnd(dot(wproj_ref[:], x_ref[t]))
        for s in range(2):
            mk = mask_ref[pl.ds(me * nseq + 2 * t + s, 1), :].astype(F32)
            ac[ds8((2 * t + s) * pitch, 2 * ne), :] = pr[:, part(s, nres)] * mk
    loop(nseq // 2, project, 16)

    def cslots(q):
        def slot(lo, size):
            return lambda dev: call.at[pl.ds(first[q] + lo, size), dev, :nseq, :]
        hq = sizes[q] // 2
        return slot(0, sizes[q]), slot(0, hq), slot(hq, hq)

    def own(q):
        for f in range(first[q], first[q] + sizes[q]):
            v = ac[pl.ds(ne + f, nseq, stride=pitch), :].astype(BF)
            csend[f] = v
            call[f, me, :nseq, :] = v
        pc.spread(csend.at[pl.ds(first[q], sizes[q])], cslots(q)[0], ssem_c.at[q], rsem_c.at[q])

    def neighbours(q):
        pc.spread_relay(*cslots(q), ssem_c.at[q], rsem_c.at[q])
        if q + 2 < nchunk:
            own(q + 2)

    pc.meet()
    own(0)
    pad = jnp.zeros((nres - nseq, nres), F32)

    def plane(e):
        at[pl.ds(e, nres, stride=pitch2), :] = stack(ac[pl.ds(e, nseq, stride=pitch), :], pad).T
    loop(ne, plane, 8)
    blocks = rows * ne // nres
    per = nres // ne

    def pack(d):
        v = [stack(*[at[ds8((d * rows + b * per + u) * pitch2, ne), :] for u in range(per)]) for b in range(blocks)]
        for r in range(blocks - 1):
            asend[d, part(r, nres), :] = jnp.where(lane >= nseq, pltpu.roll(v[-1], nseq - r * (nres - nseq), 1), v[r]).astype(BF)
    loop(n, pack, 4)

    def aslot(dev):
        return apack.at[dev]

    pc.scatter(lambda dev: asend.at[dev], aslot, arel, ssem_a, rsem_a)

    own(1)
    apack[me] = asend[me]
    pc.scatter_relay(aslot, arel, ssem_a, rsem_a)
    neighbours(0)
    padz = jnp.zeros((call.shape[1], call.shape[2] - nseq, nres), BF)

    def fill(f):
        call[f, :, nseq:, :] = padz
    loop(nf, fill)
    maskcol[:] = jnp.broadcast_to((rm_ref[:].astype(F32) - 1.0) * 1e4, (nres, nres)).T
    mbf = mask_ref[:].astype(F32).astype(BF)
    cbuf[:] = lax.dot_general(mbf, mbf, (((0,), (0,)), ((), ())), preferred_element_type=F32)
    w32[:] = wopm_ref[:].astype(F32)
    for g in range(nf // per):
        wt[:, part(g, nres)] = stack(*[w32[pl.ds(g * per + u, ne, stride=nf), :] for u in range(per)]).T.astype(BF)
    neighbours(1)
    pc.scatter_wait(aslot, rsem_a)

    def unpack(d):
        last = jnp.zeros((nres, nres), F32)
        for r in range(blocks - 1):
            v = apack[d, part(r, nres), :].astype(F32)
            aall[d, part(r, nres), :] = jnp.where(lane < nseq, v, 0.0).astype(BF)
            moved = pltpu.roll(v, (r + 1) * (nres - nseq), 1)
            last = last + jnp.where((lane >= r * (nres - nseq)) & (lane < (r + 1) * (nres - nseq)), moved, 0.0)
        aall[d, part(blocks - 1, nres), :] = last.astype(BF)
    loop(n, unpack, 2)

    for q in range(nchunk):
        pc.spread_wait(*cslots(q), ssem_c.at[q], rsem_c.at[q])

        if q == nchunk - 3:
            neighbours(q + 2)

        def outer(g):
            acc = None
            f = first[q] + 2 * g
            for kk in range(n // 2):
                rhs = cat(*[stack(call[f + u, 2 * kk], call[f + u, 2 * kk + 1]) for u in range(2)])
                step = dot(cat(aall[2 * kk], aall[2 * kk + 1]), rhs)
                acc = step if acc is None else acc + step
            ob = acc.astype(BF)
            for u in range(2):
                for i in range(rows):
                    osc[i, ds8((2 * g + u) * ne, ne, 32), :] = ob[part(i, ne), part(u, nres)]
        loop(sizes[q] // 2, outer, 2)
        depth = sizes[q] * ne

        def contract(g):
            step = dot(wt[:, first[q] * ne:first[q] * ne + depth], cat(osc[2 * g, :depth, :], osc[2 * g + 1, :depth, :]))
            for u in range(2):
                v = step[:, part(u, nres)]
                upd[2 * g + u] = v if q == 0 else upd[2 * g + u] + v
        loop(rows // 2, contract, 8)
        if q + 3 < nchunk:
            neighbours(q + 2)

    def residual(i):
        u = upd[i] / (1e-3 + cbuf[pl.ds(me * rows + i, 1), :])
        z1[i] = (z_ref[i].astype(F32) + u.T).astype(BF)
    loop(rows, residual, 8)

    for early, zin, wb, wq, wo, ball, ts, zrel, zout, sems in (
            ((wb2_ref, ball2, ssem_b2, rsem_b2), z1, wb1_ref, wqkvg1_ref, wo1_ref, ball1, tsend1, zrel1, zmid, (ssem_b1, rsem_b1, ssem_t1, rsem_t1)),
            (None, zmid, wb2_ref, wqkvg2_ref, wo2_ref, ball2, tsend2, zrel2, zfin, (ssem_b2, rsem_b2, ssem_t2, rsem_t2))):
        tri_attend(pc, early, zin, wb, wq, wo, maskcol, zln, brow, ball, bias, proj, gate, flat, wot, lbuf, mbuf, pbuf, rbuf, obuf, zrel, ts, zout, *sems)
    zo_ref[:] = zfin[:]
    pc.drain()


def pair_call(n, mask, x, z, rm, wproj, wopm, wb1, wqkvg1, wo1, wb2, wqkvg2, wo2):
    rows, nres, chan = z.shape
    nseq = 2 * x.shape[0]
    ne = wproj.shape[0] // 2
    heads = wb1.shape[0]
    sizes = (8, 8, 8, 4, 4)
    dma = pltpu.SemaphoreType.DMA((n,))
    dma9 = pltpu.SemaphoreType.DMA((9,))
    dmac = pltpu.SemaphoreType.DMA((len(sizes), 9))
    pitch = rows + 8
    vz = pltpu.VMEM((rows, nres, chan), BF)
    fz = pltpu.VMEM((rows, chan, nres), F32)
    sq = pltpu.VMEM((nres, nres), F32)
    vb = pltpu.VMEM((heads, n * rows, nres), BF)
    vt = pltpu.VMEM((2, nres, rows // 2, chan), BF)
    vr = pltpu.VMEM((2, 2, rows, rows // 2, chan), BF)
    dma29 = pltpu.SemaphoreType.DMA((2, 9))
    apk = rows * ne * nseq // nres
    row8 = pltpu.VMEM((heads, 8, 2 * nres), F32)
    args = (mask, x, z, rm, wproj, wopm, wb1, wqkvg1, wo1, wb2, wqkvg2, wo2)
    return pl.pallas_call(
        functools.partial(pair_kernel, n, sizes),
        name="pair",
        out_shape=jax.ShapeDtypeStruct(z.shape, BF),
        in_specs=[VM] * len(args),
        out_specs=VM,
        scratch_shapes=[
            pltpu.VMEM((nseq * (2 * ne + 8), nres), F32),
            pltpu.VMEM((nres * (ne + 8), nres), F32),
            pltpu.VMEM(wopm.shape, F32),
            pltpu.VMEM(wopm.shape[::-1], BF),
            sq,
            pltpu.VMEM((n, apk, nres), BF),
            pltpu.VMEM((ne, nseq, nres), BF),
            pltpu.VMEM((ne, n, nres, nres), BF),
            pltpu.VMEM((n, apk, nres), BF),
            pltpu.VMEM((2, apk, nres), BF),
            pltpu.VMEM((n, rows * ne, nres), BF),
            fz,
            pltpu.VMEM((rows, sizes[0] * ne, nres), BF),
            vz, vz,
            pltpu.VMEM((heads * pitch, nres), F32),
            vb, vb,
            pltpu.VMEM((nres, heads * nres), F32),
            pltpu.VMEM((rows, 3 * chan, nres), BF), fz,
            pltpu.VMEM((nres * pitch, chan), F32),
            pltpu.VMEM((chan, chan), BF),
            pltpu.VMEM((heads, nres, 2 * nres), F32), row8, pltpu.VMEM((heads, nres, 2 * nres), BF), row8,
            fz, sq, vt, vt, vr, vr, vz, vz,
            dma9, dma9, dmac, dmac, dma, dma, dma29, dma29, dma, dma, dma29, dma29,
        ],
        compiler_params=pltpu.CompilerParams(vmem_limit_bytes=40 * 2 ** 20, collective_id=1, has_side_effects=True),
    )(*args)


def flat_t(w):
    return jnp.moveaxis(w, 0, -1).reshape(-1, w.shape[0])


def solution(mesh):
    n = mesh.shape["dap"]

    def block(msa, pair, msa_mask, res_mask, row_bias_w, row_qkvg_w, row_out_w, col_query_w, col_kv_w, col_gate_w, col_out_w,
              opm_proj_w, opm_out_w, start_bias_w, start_qkvg_w, start_out_w, end_bias_w, end_qkvg_w, end_out_w):
        nseq, nres, chan = msa.shape
        pdim = pair.shape[2]
        mt = jnp.transpose(msa, (0, 2, 1))
        m1, g2, o2 = msa_call(n, msa_mask, mt, pair, row_bias_w.T, flat_t(row_qkvg_w), row_out_w.reshape(chan, chan),
                              flat_t(col_query_w), flat_t(col_kv_w), flat_t(col_gate_w))
        m2, x3 = gate_call(m1, g2, o2, col_out_w.reshape(chan, chan))
        zo = pair_call(n, msa_mask, x3, pair, res_mask.reshape(1, nres), flat_t(opm_proj_w), opm_out_w.reshape(-1, pdim),
                       start_bias_w.T, flat_t(start_qkvg_w), start_out_w.reshape(pdim, pdim),
                       end_bias_w.T, flat_t(end_qkvg_w), end_out_w.reshape(pdim, pdim))
        return jnp.transpose(m2, (0, 2, 1)), zo

    row_spec = P(('data', 'dap'), None, None)
    in_specs = (row_spec, row_spec, P('data', None), P('data')) + (P(),) * 15
    return jax.shard_map(block, mesh=mesh, in_specs=in_specs, out_specs=(row_spec, row_spec), check_vma=False)
```

```python
import functools
import math

import jax
import jax.numpy as jnp
import numpy as np
from jax import lax
from jax.experimental import pallas as pl
from jax.experimental.pallas import tpu as pltpu
from jax.sharding import PartitionSpec as P

BF = jnp.bfloat16
F32 = jnp.float32
MESH = pl.DeviceIdType.MESH
LOG2E = math.log2(math.e)
VM = pl.BlockSpec(memory_space=pltpu.VMEM)


def dot(a, b):
    return lax.dot_general(a, b, (((1,), (0,)), ((), ())), preferred_element_type=F32)


def dot_nt(a, b):
    return lax.dot_general(a, b, (((1,), (1,)), ((), ())), preferred_element_type=F32)


def rnd(v):
    return v.astype(BF).astype(F32)


def norm(v, axis):
    mean = jnp.mean(v, axis=axis, keepdims=True)
    cen = v - mean
    var = jnp.mean(cen * cen, axis=axis, keepdims=True)
    return (cen * lax.rsqrt(var + 1e-5)).astype(BF)


def peak(v):
    return jnp.max(v, axis=0, keepdims=True)


def total(v):
    return jnp.sum(v, axis=0, keepdims=True)


def sigmoid(v):
    return 1.0 / (1.0 + jnp.exp(-v))


def split3(value):
    hi = float(np.asarray(value).astype(BF))
    mid = float(np.asarray(value - hi).astype(BF))
    return hi, mid, float(np.asarray(value - hi - mid).astype(BF))


def rcopy(src, dst, ssem, rsem, dev):
    return pltpu.make_async_remote_copy(src_ref=src, dst_ref=dst, send_sem=ssem, recv_sem=rsem, device_id={"dap": dev}, device_id_type=MESH)


def loop(count, body, unroll=1):
    lax.fori_loop(0, count, lambda t, c: (body(t), c)[-1], 0, unroll=unroll)


def cat(*v):
    return jnp.concatenate(v, axis=-1)


def stack(*v):
    return jnp.concatenate(v, axis=0)


def part(s, width):
    return slice(s * width, s * width + width)


class Place:
    def __init__(self, n):
        nx = n // 2
        self.n, self.me = n, lax.axis_index("dap")
        x, self.k = lax.div(self.me, 2), lax.rem(self.me, 2)
        self.rightc, self.leftc, self.farc = (lax.rem(x + d, nx) * 2 for d in (1, nx - 1, 2))
        self.right, self.left, self.far = (c + self.k for c in (self.rightc, self.leftc, self.farc))
        self.partner = self.other(self.me)
        self.sends = []

    def other(self, dev):
        return dev + 1 - 2 * self.k

    def signal(self):
        sem = pltpu.get_barrier_semaphore()
        for d in range(1, self.n):
            pl.semaphore_signal(sem, inc=1, device_id={"dap": lax.rem(self.me + d, self.n)}, device_id_type=MESH)

    def meet(self):
        pl.semaphore_wait(pltpu.get_barrier_semaphore(), self.n - 1)

    def go(self, src, dst, ssem, rsem, dev):
        cp = rcopy(src, dst, ssem, rsem, dev)
        cp.start()
        self.sends.append(cp)

    def got(self, dst, rsem):
        rcopy(dst, dst, rsem, rsem, self.me).wait_recv()

    def drain(self):
        for cp in self.sends:
            cp.wait_send()

    def to_all(self, src, slot, ssem, rsem):
        for d in sorted(range(1, self.n), key=lambda d: -min(d, self.n - d)):
            self.go(src, slot(self.me), ssem.at[d], rsem.at[d], lax.rem(self.me + d, self.n))

    def from_all(self, slot, rsem):
        for d in range(1, self.n):
            self.got(slot(lax.rem(self.me + self.n - d, self.n)), rsem.at[d])

    def scatter(self, blk, slot, ssem, rsem, rel=None):
        k, me = self.k, self.me
        for j, onward in enumerate((self.right, self.left)):
            if rel is None:
                self.go(blk(self.farc + j), slot(me), ssem.at[j], rsem.at[7 + k], self.farc + j)
            else:
                self.go(blk(self.farc + j), rel.at[j], ssem.at[j], rsem.at[j], onward)
        for j in range(2):
            self.go(blk(self.rightc + j), slot(me), ssem.at[2 + j], rsem.at[2 + k], self.rightc + j)
            self.go(blk(self.leftc + j), slot(me), ssem.at[4 + j], rsem.at[4 + k], self.leftc + j)
        self.go(blk(self.partner), slot(me), ssem.at[6], rsem.at[6], self.partner)

    def scatter_relay(self, slot, rel, ssem, rsem):
        for j, (dev, onward) in enumerate(((self.left, self.rightc), (self.right, self.leftc + 1))):
            self.got(rel.at[j], rsem.at[j])
            self.go(rel.at[j], slot(dev), ssem.at[7 + j], rsem.at[7 + self.k], onward)

    def scatter_wait(self, slot, rsem):
        for j in range(2):
            self.got(slot(self.leftc + j), rsem.at[2 + j])
            self.got(slot(self.rightc + j), rsem.at[4 + j])
            self.got(slot(self.farc + j), rsem.at[7 + j])
        self.got(slot(self.partner), rsem.at[6])

    def spread(self, src, slot, ssem, rsem):
        for i, dev in enumerate((self.right, self.left, self.partner)):
            self.go(src, slot(self.me), ssem.at[i], rsem.at[i], dev)

    def spread_relay(self, slot, lower, upper, ssem, rsem, both=False):
        left, right = self.left, self.right
        for i, (dev, half, onward) in enumerate(((left, lower, right), (right, upper, left))):
            self.got(slot(dev), rsem.at[i])
            self.go(half(dev), half(dev), ssem.at[3 + i], rsem.at[3 + i], onward)
            if both:
                self.go(half(dev), half(dev), ssem.at[7 + i], rsem.at[7 + i], self.other(onward))
            self.go(slot(dev), slot(dev), ssem.at[5 + i], rsem.at[5 + i], self.partner)

    def spread_wait(self, slot, lower, upper, ssem, rsem, both=False):
        for i, half in enumerate((lower, upper)):
            self.got(half(self.far), rsem.at[3 + i])
            if not both:
                self.go(half(self.far), half(self.far), ssem.at[7 + i], rsem.at[7 + i], self.partner)
        self.got(slot(self.partner), rsem.at[2])
        self.got(slot(self.other(self.left)), rsem.at[5])
        self.got(slot(self.other(self.right)), rsem.at[6])
        for i, half in enumerate((lower, upper)):
            self.got(half(self.other(self.far)), rsem.at[7 + i])


def ds8(start, size, unit=8):
    return pl.ds(pl.multiple_of(start, unit), size)


def msa_kernel(n, nin, *refs):
    inputs, outputs, held = refs[:nin], refs[nin:nin + 3], refs[nin + 3:2 * nin + 3]
    msa_body(n, inputs, held, *outputs, *refs[2 * nin + 3:])


def msa_body(n, inputs, held,
               m1_ref, g2_ref, o2_ref, isem,
               ball, bias, brow, kv, lg, wot, qpart, ppart, tmp, x2_ref, xbuf, klhs, qblk, vbuf, gbuf, lbuf, mbuf, pbuf, rbuf, obuf,
               ssem_b, rsem_b, ssem_q, rsem_q, ssem_p, rsem_p):
    pc = Place(n)
    me = pc.me
    pc.signal()
    loads = [pltpu.make_async_copy(a, b, isem.at[i]) for i, (a, b) in enumerate(zip(inputs, held))]
    for cp in loads:
        cp.start()
    z_ref, wb_ref, mask_ref, m_ref, wqkvg_ref, wo_ref, wq2_ref, wkv_ref, wg2_ref = held
    loads[0].wait()
    loads[1].wait()
    nseq, chan, nres = m_ref.shape
    rows = z_ref.shape[0]
    heads = wb_ref.shape[0]
    hd = chan // heads
    scale = hd ** -0.5
    base = me * nseq

    pitch = rows + 8

    def bias_row(i):
        b = dot_nt(wb_ref[:], norm(z_ref[i].astype(F32), 1))
        brow[pl.ds(i, heads, stride=pitch), :] = b
    loop(rows, bias_row, rows)
    mine = ds8(me * rows, rows, 16)
    for h in range(heads):
        ball[h, mine, :] = brow[h * pitch:h * pitch + rows, :].astype(BF)
    def bslot(dev):
        return ball.at[:, ds8(dev * rows, rows, 16), :]

    pc.meet()
    pc.to_all(bslot(me), bslot, ssem_b, rsem_b)
    for cp in loads[2:]:
        cp.wait()
    wot[:] = wo_ref[:].astype(F32).T.astype(BF)
    rid = lax.broadcasted_iota(jnp.int32, (16, 2 * nres), 0)
    lid = lax.broadcasted_iota(jnp.int32, (16, 2 * nres), 1)
    diag = (rid < 8) == (lid < nres)

    def lnorm(t):
        xbuf[t] = norm(jnp.concatenate([m_ref[2 * t].astype(F32), m_ref[2 * t + 1].astype(F32)], axis=1), 0)
    loop(nseq // 2, lnorm, 4)

    def project(t):
        s0 = t * 2
        proj = dot(wqkvg_ref[:], xbuf[t])
        gbuf[t] = sigmoid(rnd(proj[3 * chan:, :]))
        for s in range(2):
            sl = part(s, nres)
            mk = mask_ref[pl.ds(base + s0 + s, 1), :].astype(F32) - 1.0
            kaug = jnp.concatenate([proj[chan:2 * chan, sl], jnp.broadcast_to(mk, (nres - chan, nres))], axis=0)
            klhs[s0 + s] = kaug.T.astype(BF)
            vbuf[s0 + s] = proj[2 * chan:3 * chan, sl].astype(BF)
            for p in range(heads // 2):
                q16 = proj[16 * p:16 * p + 16, sl]
                qblk[s0 + s, 16 * p:16 * p + 16, :] = jnp.where(diag, jnp.concatenate([q16, q16], axis=1), 0.0).astype(BF)
    loop(nseq // 2, project, 8)
    pc.from_all(bslot, rsem_b)
    for h in range(heads):
        bias[:, part(h, nres)] = ball[h].astype(F32).T * LOG2E

    hi, mid, lo = split3(1e4 / scale)
    rid = lax.broadcasted_iota(jnp.int32, (16, 2 * nres), 0)
    lid = lax.broadcasted_iota(jnp.int32, (16, 2 * nres), 1)
    aug = jnp.where(rid == 0, hi, jnp.where(rid == 1, mid, jnp.where(rid == 2, lo, 0.0))).astype(BF)

    npair = nseq // 2
    half = heads // 2
    wide = 2 * nres

    def qk(t, u):
        s, p = u // half, u % half
        parts = []
        if p > 0:
            parts.append(jnp.zeros((16 * p, wide), BF))
        parts.append(qblk[t * 2 + s, 16 * p:16 * p + 16, :])
        if chan - 16 * p - 16 > 0:
            parts.append(jnp.zeros((chan - 16 * p - 16, wide), BF))
        parts.append(aug)
        l = dot(klhs[t * 2 + s, :, :chan + 16], jnp.concatenate(parts, axis=0)) * (scale * LOG2E) + bias[:, part(p, wide)]
        lbuf[u] = l
        mbuf[u, 0:1, :] = peak(l)

    def ex(u):
        e = jnp.exp2(lbuf[u] - mbuf[u, 0:1, :])
        pbuf[u] = e.astype(BF)
        rbuf[u, 0:1, :] = 1.0 / total(e)

    def pv(t, u):
        s, p = u // half, u % half
        o = dot(vbuf[t * 2 + s, 16 * p:16 * p + 16, :], pbuf[u])
        sl = part(s, nres)
        obuf[t, 16 * p:16 * p + 8, sl] = o[:8, :nres] * rbuf[u, 0:1, :nres]
        obuf[t, 16 * p + 8:16 * p + 16, sl] = o[8:16, nres:] * rbuf[u, 0:1, nres:]

    units = 2 * half
    for u in range(units):
        qk(0, u)

    def row_pair(t):
        tn = jnp.minimum(t + 1, npair - 1)
        for u in range(units):
            ex(u)
            qk(tn, u)
            if u > 0:
                pv(t, u - 1)
        pv(t, units - 1)
    loop(npair, row_pair, 2)

    def finish(t):
        s0 = t * 2
        mv = jnp.concatenate([m_ref[s0].astype(F32), m_ref[s0 + 1].astype(F32)], axis=1)
        y = (gbuf[t] * obuf[t]).astype(BF)
        m1 = (mv + dot(wot[:], y)).astype(BF)
        for s in range(2):
            m1_ref[s0 + s] = m1[:, part(s, nres)]
    loop(npair, finish, 16)

    def renorm(t, acc):
        s0 = t * 2
        m1 = jnp.concatenate([m1_ref[s0].astype(F32), m1_ref[s0 + 1].astype(F32)], axis=1)
        x2 = norm(m1, 0)
        for s in range(2):
            sl = part(s, nres)
            x2_ref[s0 + s] = x2[:, sl]
            acc = acc + mask_ref[pl.ds(base + s0 + s, 1), :].astype(F32) * x2[:, sl].astype(F32)
        return acc
    qpart[me] = lax.fori_loop(0, npair, renorm, jnp.zeros((chan, nres), F32), unroll=2)


    def qslots(dev):
        return qpart.at[dev]

    pc.to_all(qpart.at[me], qslots, ssem_q, rsem_q)

    def keyval(t):
        s0 = t * 2
        xv = jnp.concatenate([x2_ref[s0], x2_ref[s0 + 1]], axis=1)
        kvp = rnd(dot(wkv_ref[:], xv))
        g2_ref[t] = sigmoid(rnd(dot(wg2_ref[:], xv)))
        for s in range(2):
            kv[s0 + s] = kvp[:, part(s, nres)]
    loop(npair, keyval, 8)
    count = total(mask_ref[:].astype(F32)) + 1e-10
    pc.from_all(qslots, rsem_q)
    tot = qpart[0]
    for d in range(1, n):
        tot = tot + qpart[d]
    tmp[:] = rnd(dot(wq2_ref[:], (tot / count).astype(BF)))
    qd = [tmp[pl.ds(d, heads, stride=hd), :] for d in range(hd)]
    unroll = 8

    def logit(t, mx):
        for u in range(unroll):
            s = t * unroll + u
            row = kv.at[s]
            l = qd[0] * row[0:1, :]
            for d in range(1, hd):
                l = l + qd[d] * row[d:d + 1, :]
            l = l * scale + (mask_ref[pl.ds(base + s, 1), :].astype(F32) - 1.0) * 1e4
            lg[s] = l
            mx = jnp.maximum(mx, l)
        return mx
    mx = lax.fori_loop(0, nseq // unroll, logit, jnp.full((heads, nres), -jnp.inf, F32))

    def weigh(t, carry):
        ssum, acc = carry
        acc = list(acc)
        for u in range(unroll):
            s = t * unroll + u
            row = kv.at[s]
            e = jnp.exp(lg[s] - mx)
            ssum = ssum + e
            eb = rnd(e)
            for d in range(hd):
                acc[d] = acc[d] + eb * row[hd + d:hd + d + 1, :]
        return ssum, tuple(acc)
    zero = jnp.zeros((heads, nres), F32)
    ssum, acc = lax.fori_loop(0, nseq // unroll, weigh, (zero, (zero,) * hd))
    ppart[me, :8, :] = mx
    ppart[me, 8:16, :] = ssum
    for d in range(hd):
        ppart[me, 16 + 8 * d:24 + 8 * d, :] = acc[d]

    def pslots(dev):
        return ppart.at[dev]

    pc.to_all(ppart.at[me], pslots, ssem_p, rsem_p)
    pc.from_all(pslots, rsem_p)
    top = ppart[0, :8, :]
    for d in range(1, n):
        top = jnp.maximum(top, ppart[d, :8, :])
    fac = [jnp.exp(ppart[d, :8, :] - top) for d in range(n)]
    den = fac[0] * ppart[0, 8:16, :]
    for d in range(1, n):
        den = den + fac[d] * ppart[d, 8:16, :]
    inv = 1.0 / den
    for c in range(hd):
        o = fac[0] * ppart[0, 16 + 8 * c:24 + 8 * c, :]
        for d in range(1, n):
            o = o + fac[d] * ppart[d, 16 + 8 * c:24 + 8 * c, :]
        o2_ref[pl.ds(c, heads, stride=hd), :] = o * inv
    pc.drain()


def msa_call(n, mask, mt, z, wb, wqkvg, wo, wq2, wkv, wg2):
    nseq, chan, nres = mt.shape
    rows = z.shape[0]
    heads = wb.shape[0]
    dma = pltpu.SemaphoreType.DMA((n,))
    dma9 = pltpu.SemaphoreType.DMA((9,))
    args = [pltpu.with_memory_space_constraint(v, pltpu.HBM) for v in (z, wb, mask, mt, wqkvg, wo, wq2, wkv, wg2)]
    return pl.pallas_call(
        functools.partial(msa_kernel, n, len(args)),
        name="msa",
        out_shape=[jax.ShapeDtypeStruct((nseq, chan, nres), BF), jax.ShapeDtypeStruct((nseq // 2, chan, 2 * nres), F32),
                   jax.ShapeDtypeStruct((chan, nres), F32)],
        in_specs=[pl.BlockSpec(memory_space=pltpu.HBM)] * len(args),
        out_specs=[VM] * 3,
        scratch_shapes=[pltpu.VMEM(v.shape, v.dtype) for v in args] + [
            dma9,
            pltpu.VMEM((heads, n * rows, nres), BF),
            pltpu.VMEM((nres, heads * nres), F32),
            pltpu.VMEM((heads * (rows + 8), nres), F32),
            pltpu.VMEM((nseq, wkv.shape[0], nres), F32),
            pltpu.VMEM((nseq, heads, nres), F32),
            pltpu.VMEM((chan, chan), BF),
            pltpu.VMEM((n, chan, nres), F32),
            pltpu.VMEM((n, chan + 16, nres), F32),
            pltpu.VMEM((chan, nres), F32),
            pltpu.VMEM((nseq, chan, nres), BF),
            pltpu.VMEM((nseq // 2, chan, 2 * nres), BF),
            pltpu.VMEM((nseq, nres, nres), BF),
            pltpu.VMEM((nseq, chan, 2 * nres), BF),
            pltpu.VMEM((nseq, chan, nres), BF),
            pltpu.VMEM((nseq // 2, chan, 2 * nres), F32),
            pltpu.VMEM((heads, nres, 2 * nres), F32),
            pltpu.VMEM((heads, 8, 2 * nres), F32),
            pltpu.VMEM((heads, nres, 2 * nres), BF),
            pltpu.VMEM((heads, 8, 2 * nres), F32),
            pltpu.VMEM((nseq // 2, chan, 2 * nres), F32),
            dma, dma, dma, dma, dma, dma,
        ],
        compiler_params=pltpu.CompilerParams(vmem_limit_bytes=38 * 2 ** 20, collective_id=0, has_side_effects=True),
    )(*args)


def gate_kernel(m1_ref, g2_ref, o2_ref, wo_ref, m2_ref, x_ref, wot, m2, sem):
    nseq, chan, nres = m1_ref.shape
    wot[:] = wo_ref[:].astype(F32).T.astype(BF)
    pieces = sem.shape[0]
    size = nseq // pieces

    def gate(t):
        y = (g2_ref[t] * cat(o2_ref[:], o2_ref[:])).astype(BF)
        m = (cat(m1_ref[2 * t].astype(F32), m1_ref[2 * t + 1].astype(F32)) + dot(wot[:], y)).astype(BF)
        for s in range(2):
            m2[2 * t + s] = m[:, part(s, nres)]

    def renorm(t):
        x_ref[t] = norm(cat(m2[2 * t].astype(F32), m2[2 * t + 1].astype(F32)), 0)
    copies = []
    for p in range(pieces):
        loop(size // 2, lambda t: gate(t + p * (size // 2)), size // 2)
        piece = pl.ds(p * size, size)
        copies.append(pltpu.make_async_copy(m2.at[piece], m2_ref.at[piece], sem.at[p]))
        copies[-1].start()
    loop(nseq // 2, renorm, 2)
    for cp in copies:
        cp.wait()


def gate_call(m1, g2, o2, wo):
    nseq, chan, nres = m1.shape
    return pl.pallas_call(
        gate_kernel,
        name="gate",
        out_shape=[jax.ShapeDtypeStruct(m1.shape, BF), jax.ShapeDtypeStruct(g2.shape, BF)],
        in_specs=[VM] * 4,
        out_specs=[pl.BlockSpec(memory_space=pltpu.HBM), VM],
        scratch_shapes=[pltpu.VMEM((chan, chan), BF), pltpu.VMEM(m1.shape, BF), pltpu.SemaphoreType.DMA((3,))],
        compiler_params=pltpu.CompilerParams(vmem_limit_bytes=16 * 2 ** 20),
    )(m1, g2, o2, wo)


def tri_attend(pc, early, zin, wb_ref, wqkvg_ref, wo_ref, maskcol, zln, brow, ball, bias, proj, gate, flat, wot, lbuf, mbuf, pbuf, rbuf, obuf, tsend, zrecv,
               ssem_b, rsem_b, ssem_t, rsem_t):
    me = pc.me
    rows, nres, chan = zin.shape
    heads = wb_ref.shape[0]
    hd = chan // heads
    scale = hd ** -0.5
    pitch = rows + 8
    mine = ds8(me * rows, rows, 16)

    def bslot(buf):
        return lambda dev: buf.at[:, ds8(dev * rows, rows, 16), :]

    def make_bias(src, w_ref, buf, ssem, rsem):
        def bias_row(i):
            zl = norm(src[i].astype(F32), 1)
            zln[i] = zl
            brow[pl.ds(i, heads, stride=pitch), :] = dot_nt(w_ref[:], zl)
        loop(rows, bias_row, rows)
        for h in range(heads):
            buf[h, mine, :] = brow[h * pitch:h * pitch + rows, :].astype(BF)
        pc.to_all(bslot(buf)(me), bslot(buf), ssem, rsem)

    if early:
        make_bias(zin, wb_ref, ball, ssem_b, rsem_b)
    else:
        def renorm(i):
            zln[i] = norm(zin[i].astype(F32), 1)
        loop(rows, renorm, 8)
    wot[:] = wo_ref[:].astype(F32).T.astype(BF)

    def project(i):
        zl = zln[i]
        proj[i, :chan, :] = dot_nt(wqkvg_ref[:chan, :], zl).astype(BF)
        proj[i, chan:2 * chan, :] = dot_nt(zl, wqkvg_ref[chan:2 * chan, :]).astype(BF)
        proj[i, 2 * chan:, :] = dot_nt(wqkvg_ref[2 * chan:3 * chan, :], zl).astype(BF)
        gate[i] = sigmoid(rnd(dot_nt(wqkvg_ref[3 * chan:, :], zl)))
    loop(rows, project, 8)
    pc.from_all(bslot(ball), rsem_b)
    for h in range(heads):
        b = ball[h].astype(F32)
        bias[:, part(h, nres)] = ((b.T if early else b) + maskcol[:]) * LOG2E
    zero = jnp.zeros((hd, nres), BF)

    half = heads // 2
    wide = 2 * nres

    def qk(i, p, u):
        r0 = 2 * hd * p
        qa = proj[i, r0:r0 + hd, :]
        qb = proj[i, r0 + hd:r0 + 2 * hd, :]
        parts = [jnp.zeros((r0, wide), BF)] if p > 0 else []
        parts.append(jnp.concatenate([qa, zero], axis=1))
        parts.append(jnp.concatenate([zero, qb], axis=1))
        if chan - r0 - 2 * hd > 0:
            parts.append(jnp.zeros((chan - r0 - 2 * hd, wide), BF))
        l = dot(proj[i, chan:2 * chan, :], jnp.concatenate(parts, axis=0)) * (scale * LOG2E) + bias[:, part(p, wide)]
        lbuf[u] = l
        mbuf[u, 0:1, :] = peak(l)

    def ex(u):
        e = jnp.exp2(lbuf[u] - mbuf[u, 0:1, :])
        pbuf[u] = e.astype(BF)
        rbuf[u, 0:1, :] = 1.0 / total(e)

    def pv(i, p, u):
        r0 = 2 * hd * p
        o = dot(proj[i, 2 * chan + r0:2 * chan + r0 + 2 * hd, :], pbuf[u])
        obuf[i, r0:r0 + hd, :] = o[:hd, :nres] * rbuf[u, 0:1, :nres]
        obuf[i, r0 + hd:r0 + 2 * hd, :] = o[hd:, nres:] * rbuf[u, 0:1, nres:]

    units = [(i, p) for i in range(2) for p in range(half)]
    for u, (i, p) in enumerate(units):
        qk(i, p, u)

    def attend(t):
        nxt = jnp.minimum(2 * t + 2, rows - 2)
        for u, (i, p) in enumerate(units):
            ex(u)
            qk(nxt + i, p, u)
            if u > 0:
                pv(2 * t + units[u - 1][0], units[u - 1][1], u - 1)
        pv(2 * t + units[-1][0], units[-1][1], len(units) - 1)
    def finish(i):
        y = (gate[i] * obuf[i]).astype(BF)
        upd = dot(wot[:], y).T
        zn = zin[i].astype(F32) + upd
        flat[pl.ds(i, nres, stride=pitch), :] = zn
        if early:
            zin[i] = zn.astype(BF)
    hrow = rows // 2

    def tblk(h):
        return lambda dev: tsend.at[h, pl.ds(dev * rows, rows)]

    def tslot(h):
        return lambda dev: zrecv.at[:, ds8(dev * rows + h * hrow, hrow), :]

    for h in range(2):
        loop(rows // 4, lambda t: attend(t + h * (rows // 4)), 4)
        loop(hrow, lambda i: finish(i + h * hrow), 8)

        def regroup(j):
            tsend[h, j] = flat[ds8(j * pitch + h * hrow, hrow), :].astype(BF)
        loop(nres, regroup, 8)
        pc.scatter(tblk(h), tslot(h), ssem_t.at[h], rsem_t.at[h])
    for h in range(2):
        if early and h == 0:
            make_bias(zin, *early)
        zrecv[:, ds8(me * rows + h * hrow, hrow), :] = tsend[h, pl.ds(me * rows, rows)]
    for h in range(2):
        pc.scatter_wait(tslot(h), rsem_t.at[h])


def pair_kernel(n, sizes, mask_ref, x_ref, z_ref, rm_ref, wproj_ref, wopm_ref, wb1_ref, wqkvg1_ref, wo1_ref, wb2_ref, wqkvg2_ref, wo2_ref,
                zo_ref,
                ac, at, w32, wt, cbuf, asend, csend, call, apack, arel, aall, upd, osc, z1, zln, brow, ball1, ball2, bias, proj, gate, flat, wot,
                lbuf, mbuf, pbuf, rbuf, obuf, maskcol, tsend1, tsend2, zmid, zfin,
                ssem_a, rsem_a, ssem_c, rsem_c, ssem_b1, rsem_b1, ssem_t1, rsem_t1, ssem_b2, rsem_b2, ssem_t2, rsem_t2):
    pc = Place(n)
    me = pc.me
    pc.signal()
    rows, nres, chan = z_ref.shape
    nf, nseq = csend.shape[0:2]
    ne = nf
    nchunk = len(sizes)
    first = [sum(sizes[:q]) for q in range(nchunk)]
    lane = lax.broadcasted_iota(jnp.int32, (nres, nres), 1)
    pitch = ac.shape[0] // nseq
    pitch2 = at.shape[0] // nres

    def project(t):
        pr = rnd(dot(wproj_ref[:], x_ref[t]))
        for s in range(2):
            mk = mask_ref[pl.ds(me * nseq + 2 * t + s, 1), :].astype(F32)
            ac[ds8((2 * t + s) * pitch, 2 * ne), :] = pr[:, part(s, nres)] * mk
    loop(nseq // 2, project, 16)

    def cslots(q):
        def slot(lo, size):
            return lambda dev: call.at[pl.ds(first[q] + lo, size), dev, :nseq, :]
        hq = sizes[q] // 2
        return slot(0, sizes[q]), slot(0, hq), slot(hq, hq)

    def own(q):
        for f in range(first[q], first[q] + sizes[q]):
            v = ac[pl.ds(ne + f, nseq, stride=pitch), :].astype(BF)
            csend[f] = v
            call[f, me, :nseq, :] = v
        pc.spread(csend.at[pl.ds(first[q], sizes[q])], cslots(q)[0], ssem_c.at[q], rsem_c.at[q])

    def neighbours(q):
        pc.spread_relay(*cslots(q), ssem_c.at[q], rsem_c.at[q])
        if q + 2 < nchunk:
            own(q + 2)

    pc.meet()
    own(0)
    pad = jnp.zeros((nres - nseq, nres), F32)

    def plane(e):
        at[pl.ds(e, nres, stride=pitch2), :] = stack(ac[pl.ds(e, nseq, stride=pitch), :], pad).T
    loop(ne, plane, 8)
    blocks = rows * ne // nres
    per = nres // ne

    def pack(d):
        v = [stack(*[at[ds8((d * rows + b * per + u) * pitch2, ne), :] for u in range(per)]) for b in range(blocks)]
        for r in range(blocks - 1):
            asend[d, part(r, nres), :] = jnp.where(lane >= nseq, pltpu.roll(v[-1], nseq - r * (nres - nseq), 1), v[r]).astype(BF)
    loop(n, pack, 4)

    def aslot(dev):
        return apack.at[dev]

    pc.scatter(lambda dev: asend.at[dev], aslot, ssem_a, rsem_a, arel)

    own(1)
    apack[me] = asend[me]
    pc.scatter_relay(aslot, arel, ssem_a, rsem_a)
    neighbours(0)
    padz = jnp.zeros((call.shape[1], call.shape[2] - nseq, nres), BF)

    def fill(f):
        call[f, :, nseq:, :] = padz
    loop(nf, fill)
    maskcol[:] = jnp.broadcast_to((rm_ref[:].astype(F32) - 1.0) * 1e4, (nres, nres)).T
    mbf = mask_ref[:].astype(F32).astype(BF)
    cbuf[:] = lax.dot_general(mbf, mbf, (((0,), (0,)), ((), ())), preferred_element_type=F32)
    w32[:] = wopm_ref[:].astype(F32)
    for g in range(nf // per):
        wt[:, part(g, nres)] = stack(*[w32[pl.ds(g * per + u, ne, stride=nf), :] for u in range(per)]).T.astype(BF)
    neighbours(1)
    pc.scatter_wait(aslot, rsem_a)

    def unpack(d):
        last = jnp.zeros((nres, nres), F32)
        for r in range(blocks - 1):
            v = apack[d, part(r, nres), :].astype(F32)
            aall[d, part(r, nres), :] = jnp.where(lane < nseq, v, 0.0).astype(BF)
            moved = pltpu.roll(v, (r + 1) * (nres - nseq), 1)
            last = last + jnp.where((lane >= r * (nres - nseq)) & (lane < (r + 1) * (nres - nseq)), moved, 0.0)
        aall[d, part(blocks - 1, nres), :] = last.astype(BF)
    loop(n, unpack, 2)

    for q in range(nchunk):
        pc.spread_wait(*cslots(q), ssem_c.at[q], rsem_c.at[q])

        if q == nchunk - 3:
            neighbours(q + 2)

        def outer(g):
            acc = None
            f = first[q] + 2 * g
            for kk in range(n // 2):
                rhs = cat(*[stack(call[f + u, 2 * kk], call[f + u, 2 * kk + 1]) for u in range(2)])
                step = dot(cat(aall[2 * kk], aall[2 * kk + 1]), rhs)
                acc = step if acc is None else acc + step
            ob = acc.astype(BF)
            for u in range(2):
                for i in range(rows):
                    osc[i, ds8((2 * g + u) * ne, ne, 32), :] = ob[part(i, ne), part(u, nres)]
        loop(sizes[q] // 2, outer, 2)
        depth = sizes[q] * ne

        def contract(g):
            step = dot(wt[:, first[q] * ne:first[q] * ne + depth], cat(osc[2 * g, :depth, :], osc[2 * g + 1, :depth, :]))
            for u in range(2):
                v = step[:, part(u, nres)]
                upd[2 * g + u] = v if q == 0 else upd[2 * g + u] + v
        loop(rows // 2, contract, 8)
        if q + 3 < nchunk:
            neighbours(q + 2)

    def residual(i):
        u = upd[i] / (1e-3 + cbuf[pl.ds(me * rows + i, 1), :])
        z1[i] = (z_ref[i].astype(F32) + u.T).astype(BF)
    loop(rows, residual, 8)

    for early, zin, wb, wq, wo, ball, ts, zout, sems in (
            ((wb2_ref, ball2, ssem_b2, rsem_b2), z1, wb1_ref, wqkvg1_ref, wo1_ref, ball1, tsend1, zmid, (ssem_b1, rsem_b1, ssem_t1, rsem_t1)),
            (None, zmid, wb2_ref, wqkvg2_ref, wo2_ref, ball2, tsend2, zfin, (ssem_b2, rsem_b2, ssem_t2, rsem_t2))):
        tri_attend(pc, early, zin, wb, wq, wo, maskcol, zln, brow, ball, bias, proj, gate, flat, wot, lbuf, mbuf, pbuf, rbuf, obuf, ts, zout, *sems)
    zo_ref[:] = zfin[:]
    pc.drain()


def pair_call(n, mask, x, z, rm, wproj, wopm, wb1, wqkvg1, wo1, wb2, wqkvg2, wo2):
    rows, nres, chan = z.shape
    nseq = 2 * x.shape[0]
    ne = wproj.shape[0] // 2
    heads = wb1.shape[0]
    sizes = (8, 8, 8, 4, 4)
    dma = pltpu.SemaphoreType.DMA((n,))
    dma9 = pltpu.SemaphoreType.DMA((9,))
    dmac = pltpu.SemaphoreType.DMA((len(sizes), 9))
    pitch = rows + 8
    vz = pltpu.VMEM((rows, nres, chan), BF)
    fz = pltpu.VMEM((rows, chan, nres), F32)
    sq = pltpu.VMEM((nres, nres), F32)
    vb = pltpu.VMEM((heads, n * rows, nres), BF)
    vt = pltpu.VMEM((2, nres, rows // 2, chan), BF)
    dma29 = pltpu.SemaphoreType.DMA((2, 9))
    apk = rows * ne * nseq // nres
    row8 = pltpu.VMEM((heads, 8, 2 * nres), F32)
    args = (mask, x, z, rm, wproj, wopm, wb1, wqkvg1, wo1, wb2, wqkvg2, wo2)
    return pl.pallas_call(
        functools.partial(pair_kernel, n, sizes),
        name="pair",
        out_shape=jax.ShapeDtypeStruct(z.shape, BF),
        in_specs=[VM] * len(args),
        out_specs=VM,
        scratch_shapes=[
            pltpu.VMEM((nseq * (2 * ne + 8), nres), F32),
            pltpu.VMEM((nres * (ne + 8), nres), F32),
            pltpu.VMEM(wopm.shape, F32),
            pltpu.VMEM(wopm.shape[::-1], BF),
            sq,
            pltpu.VMEM((n, apk, nres), BF),
            pltpu.VMEM((ne, nseq, nres), BF),
            pltpu.VMEM((ne, n, nres, nres), BF),
            pltpu.VMEM((n, apk, nres), BF),
            pltpu.VMEM((2, apk, nres), BF),
            pltpu.VMEM((n, rows * ne, nres), BF),
            fz,
            pltpu.VMEM((rows, sizes[0] * ne, nres), BF),
            vz, vz,
            pltpu.VMEM((heads * pitch, nres), F32),
            vb, vb,
            pltpu.VMEM((nres, heads * nres), F32),
            pltpu.VMEM((rows, 3 * chan, nres), BF), fz,
            pltpu.VMEM((nres * pitch, chan), F32),
            pltpu.VMEM((chan, chan), BF),
            pltpu.VMEM((heads, nres, 2 * nres), F32), row8, pltpu.VMEM((heads, nres, 2 * nres), BF), row8,
            fz, sq, vt, vt, vz, vz,
            dma9, dma9, dmac, dmac, dma, dma, dma29, dma29, dma, dma, dma29, dma29,
        ],
        compiler_params=pltpu.CompilerParams(vmem_limit_bytes=40 * 2 ** 20, collective_id=1, has_side_effects=True),
    )(*args)


def flat_t(w):
    return jnp.moveaxis(w, 0, -1).reshape(-1, w.shape[0])


def solution(mesh):
    n = mesh.shape["dap"]

    def block(msa, pair, msa_mask, res_mask, row_bias_w, row_qkvg_w, row_out_w, col_query_w, col_kv_w, col_gate_w, col_out_w,
              opm_proj_w, opm_out_w, start_bias_w, start_qkvg_w, start_out_w, end_bias_w, end_qkvg_w, end_out_w):
        nseq, nres, chan = msa.shape
        pdim = pair.shape[2]
        mt = jnp.transpose(msa, (0, 2, 1))
        m1, g2, o2 = msa_call(n, msa_mask, mt, pair, row_bias_w.T, flat_t(row_qkvg_w), row_out_w.reshape(chan, chan),
                              flat_t(col_query_w), flat_t(col_kv_w), flat_t(col_gate_w))
        m2, x3 = gate_call(m1, g2, o2, col_out_w.reshape(chan, chan))
        zo = pair_call(n, msa_mask, x3, pair, res_mask.reshape(1, nres), flat_t(opm_proj_w), opm_out_w.reshape(-1, pdim),
                       start_bias_w.T, flat_t(start_qkvg_w), start_out_w.reshape(pdim, pdim),
                       end_bias_w.T, flat_t(end_qkvg_w), end_out_w.reshape(pdim, pdim))
        return jnp.transpose(m2, (0, 2, 1)), zo

    row_spec = P(('data', 'dap'), None, None)
    in_specs = (row_spec, row_spec, P('data', None), P('data')) + (P(),) * 15
    return jax.shard_map(block, mesh=mesh, in_specs=in_specs, out_specs=(row_spec, row_spec), check_vma=False)
```

```python
import functools
import math

import jax
import jax.numpy as jnp
import numpy as np
from jax import lax
from jax.experimental import pallas as pl
from jax.experimental.pallas import tpu as pltpu
from jax.sharding import PartitionSpec as P

BF = jnp.bfloat16
F32 = jnp.float32
MESH = pl.DeviceIdType.MESH
LOG2E = math.log2(math.e)
VM = pl.BlockSpec(memory_space=pltpu.VMEM)


def dot(a, b):
    return lax.dot_general(a, b, (((1,), (0,)), ((), ())), preferred_element_type=F32)


def dot_nt(a, b):
    return lax.dot_general(a, b, (((1,), (1,)), ((), ())), preferred_element_type=F32)


def rnd(v):
    return v.astype(BF).astype(F32)


def norm(v, axis):
    mean = jnp.mean(v, axis=axis, keepdims=True)
    cen = v - mean
    var = jnp.mean(cen * cen, axis=axis, keepdims=True)
    return (cen * lax.rsqrt(var + 1e-5)).astype(BF)


def peak(v):
    return jnp.max(v, axis=0, keepdims=True)


def total(v):
    return jnp.sum(v, axis=0, keepdims=True)


def sigmoid(v):
    return 1.0 / (1.0 + jnp.exp(-v))


def split3(value):
    hi = float(np.asarray(value).astype(BF))
    mid = float(np.asarray(value - hi).astype(BF))
    return hi, mid, float(np.asarray(value - hi - mid).astype(BF))


def rcopy(src, dst, ssem, rsem, dev):
    return pltpu.make_async_remote_copy(src_ref=src, dst_ref=dst, send_sem=ssem, recv_sem=rsem, device_id={"dap": dev}, device_id_type=MESH)


def loop(count, body, unroll=1):
    lax.fori_loop(0, count, lambda t, c: (body(t), c)[-1], 0, unroll=unroll)


def cat(*v):
    return jnp.concatenate(v, axis=-1)


def stack(*v):
    return jnp.concatenate(v, axis=0)


def part(s, width):
    return slice(s * width, s * width + width)


class Place:
    def __init__(self, n):
        nx = n // 2
        self.n, self.me = n, lax.axis_index("dap")
        x, self.k = lax.div(self.me, 2), lax.rem(self.me, 2)
        self.rightc, self.leftc, self.farc = (lax.rem(x + d, nx) * 2 for d in (1, nx - 1, 2))
        self.right, self.left, self.far = (c + self.k for c in (self.rightc, self.leftc, self.farc))
        self.partner = self.other(self.me)
        self.sends = []

    def other(self, dev):
        return dev + 1 - 2 * self.k

    def signal(self):
        sem = pltpu.get_barrier_semaphore()
        for d in range(1, self.n):
            pl.semaphore_signal(sem, inc=1, device_id={"dap": lax.rem(self.me + d, self.n)}, device_id_type=MESH)

    def meet(self):
        pl.semaphore_wait(pltpu.get_barrier_semaphore(), self.n - 1)

    def go(self, src, dst, ssem, rsem, dev):
        cp = rcopy(src, dst, ssem, rsem, dev)
        cp.start()
        self.sends.append(cp)

    def got(self, dst, rsem):
        rcopy(dst, dst, rsem, rsem, self.me).wait_recv()

    def drain(self):
        for cp in self.sends:
            cp.wait_send()

    def to_all(self, src, slot, ssem, rsem):
        for d in sorted(range(1, self.n), key=lambda d: -min(d, self.n - d)):
            self.go(src, slot(self.me), ssem.at[d], rsem.at[d], lax.rem(self.me + d, self.n))

    def from_all(self, slot, rsem):
        for d in range(1, self.n):
            self.got(slot(lax.rem(self.me + self.n - d, self.n)), rsem.at[d])

    def scatter(self, blk, slot, ssem, rsem, rel=None):
        k, me = self.k, self.me
        for j, onward in enumerate((self.right, self.left)):
            if rel is None:
                self.go(blk(self.farc + j), slot(me), ssem.at[j], rsem.at[7 + k], self.farc + j)
            else:
                self.go(blk(self.farc + j), rel.at[j], ssem.at[j], rsem.at[j], onward)
        for j in range(2):
            self.go(blk(self.rightc + j), slot(me), ssem.at[2 + j], rsem.at[2 + k], self.rightc + j)
            self.go(blk(self.leftc + j), slot(me), ssem.at[4 + j], rsem.at[4 + k], self.leftc + j)
        self.go(blk(self.partner), slot(me), ssem.at[6], rsem.at[6], self.partner)

    def scatter_relay(self, slot, rel, ssem, rsem):
        for j, (dev, onward) in enumerate(((self.left, self.rightc), (self.right, self.leftc + 1))):
            self.got(rel.at[j], rsem.at[j])
            self.go(rel.at[j], slot(dev), ssem.at[7 + j], rsem.at[7 + self.k], onward)

    def scatter_wait(self, slot, rsem):
        for j in range(2):
            self.got(slot(self.leftc + j), rsem.at[2 + j])
            self.got(slot(self.rightc + j), rsem.at[4 + j])
            self.got(slot(self.farc + j), rsem.at[7 + j])
        self.got(slot(self.partner), rsem.at[6])

    def spread(self, src, slot, ssem, rsem):
        for i, dev in enumerate((self.right, self.left, self.partner)):
            self.go(src, slot(self.me), ssem.at[i], rsem.at[i], dev)

    def spread_relay(self, slot, lower, upper, ssem, rsem, both=False):
        left, right = self.left, self.right
        for i, (dev, half, onward) in enumerate(((left, lower, right), (right, upper, left))):
            self.got(slot(dev), rsem.at[i])
            self.go(half(dev), half(dev), ssem.at[3 + i], rsem.at[3 + i], onward)
            if both:
                self.go(half(dev), half(dev), ssem.at[7 + i], rsem.at[7 + i], self.other(onward))
            self.go(slot(dev), slot(dev), ssem.at[5 + i], rsem.at[5 + i], self.partner)

    def spread_wait(self, slot, lower, upper, ssem, rsem, both=False):
        for i, half in enumerate((lower, upper)):
            self.got(half(self.far), rsem.at[3 + i])
            if not both:
                self.go(half(self.far), half(self.far), ssem.at[7 + i], rsem.at[7 + i], self.partner)
        self.got(slot(self.partner), rsem.at[2])
        self.got(slot(self.other(self.left)), rsem.at[5])
        self.got(slot(self.other(self.right)), rsem.at[6])
        for i, half in enumerate((lower, upper)):
            self.got(half(self.other(self.far)), rsem.at[7 + i])


def ds8(start, size, unit=8):
    return pl.ds(pl.multiple_of(start, unit), size)


def msa_kernel(n, nin, *refs):
    inputs, outputs, held = refs[:nin], refs[nin:nin + 3], refs[nin + 3:2 * nin + 3]
    msa_body(n, inputs, held, *outputs, *refs[2 * nin + 3:])


def msa_body(n, inputs, held,
               m1_ref, g2_ref, o2_ref, isem,
               ball, bias, brow, kv, lg, wot, qpart, ppart, tmp, x2_ref, xbuf, klhs, qblk, vbuf, gbuf, lbuf, mbuf, pbuf, rbuf, obuf,
               ssem_b, rsem_b, ssem_q, rsem_q, ssem_p, rsem_p):
    pc = Place(n)
    me = pc.me
    pc.signal()
    loads = [pltpu.make_async_copy(a, b, isem.at[i]) for i, (a, b) in enumerate(zip(inputs, held))]
    for cp in loads:
        cp.start()
    z_ref, wb_ref, mask_ref, m_ref, wqkvg_ref, wo_ref, wq2_ref, wkv_ref, wg2_ref = held
    loads[0].wait()
    loads[1].wait()
    nseq, chan, nres = m_ref.shape
    rows = z_ref.shape[0]
    heads = wb_ref.shape[0]
    hd = chan // heads
    scale = hd ** -0.5
    base = me * nseq

    pitch = rows + 8

    def bias_row(i):
        b = dot_nt(wb_ref[:], norm(z_ref[i].astype(F32), 1))
        brow[pl.ds(i, heads, stride=pitch), :] = b
    loop(rows, bias_row, rows)
    mine = ds8(me * rows, rows, 16)
    for h in range(heads):
        ball[h, mine, :] = brow[h * pitch:h * pitch + rows, :].astype(BF)
    def bslot(dev):
        return ball.at[:, ds8(dev * rows, rows, 16), :]

    pc.meet()
    pc.to_all(bslot(me), bslot, ssem_b, rsem_b)
    for cp in loads[2:]:
        cp.wait()
    wot[:] = wo_ref[:].astype(F32).T.astype(BF)
    rid = lax.broadcasted_iota(jnp.int32, (16, 2 * nres), 0)
    lid = lax.broadcasted_iota(jnp.int32, (16, 2 * nres), 1)
    diag = (rid < 8) == (lid < nres)

    def lnorm(t):
        xbuf[t] = norm(jnp.concatenate([m_ref[2 * t].astype(F32), m_ref[2 * t + 1].astype(F32)], axis=1), 0)
    loop(nseq // 2, lnorm, 4)

    def project(t):
        s0 = t * 2
        proj = dot(wqkvg_ref[:], xbuf[t])
        gbuf[t] = sigmoid(rnd(proj[3 * chan:, :]))
        for s in range(2):
            sl = part(s, nres)
            mk = mask_ref[pl.ds(base + s0 + s, 1), :].astype(F32) - 1.0
            kaug = jnp.concatenate([proj[chan:2 * chan, sl], jnp.broadcast_to(mk, (nres - chan, nres))], axis=0)
            klhs[s0 + s] = kaug.T.astype(BF)
            vbuf[s0 + s] = proj[2 * chan:3 * chan, sl].astype(BF)
            for p in range(heads // 2):
                q16 = proj[16 * p:16 * p + 16, sl]
                qblk[s0 + s, 16 * p:16 * p + 16, :] = jnp.where(diag, jnp.concatenate([q16, q16], axis=1), 0.0).astype(BF)
    loop(nseq // 2, project, 8)
    pc.from_all(bslot, rsem_b)
    for h in range(heads):
        bias[:, part(h, nres)] = ball[h].astype(F32).T * LOG2E

    hi, mid, lo = split3(1e4 / scale)
    rid = lax.broadcasted_iota(jnp.int32, (16, 2 * nres), 0)
    lid = lax.broadcasted_iota(jnp.int32, (16, 2 * nres), 1)
    aug = jnp.where(rid == 0, hi, jnp.where(rid == 1, mid, jnp.where(rid == 2, lo, 0.0))).astype(BF)

    npair = nseq // 2
    half = heads // 2
    wide = 2 * nres

    def qk(t, u):
        s, p = u // half, u % half
        parts = []
        if p > 0:
            parts.append(jnp.zeros((16 * p, wide), BF))
        parts.append(qblk[t * 2 + s, 16 * p:16 * p + 16, :])
        if chan - 16 * p - 16 > 0:
            parts.append(jnp.zeros((chan - 16 * p - 16, wide), BF))
        parts.append(aug)
        l = dot(klhs[t * 2 + s, :, :chan + 16], jnp.concatenate(parts, axis=0)) * (scale * LOG2E) + bias[:, part(p, wide)]
        lbuf[u] = l
        mbuf[u, 0:1, :] = peak(l)

    def ex(u):
        e = jnp.exp2(lbuf[u] - mbuf[u, 0:1, :])
        pbuf[u] = e.astype(BF)
        rbuf[u, 0:1, :] = 1.0 / total(e)

    def pv(t, u):
        s, p = u // half, u % half
        o = dot(vbuf[t * 2 + s, 16 * p:16 * p + 16, :], pbuf[u])
        sl = part(s, nres)
        obuf[t, 16 * p:16 * p + 8, sl] = o[:8, :nres] * rbuf[u, 0:1, :nres]
        obuf[t, 16 * p + 8:16 * p + 16, sl] = o[8:16, nres:] * rbuf[u, 0:1, nres:]

    units = 2 * half
    for u in range(units):
        qk(0, u)

    def row_pair(t):
        tn = jnp.minimum(t + 1, npair - 1)
        for u in range(units):
            ex(u)
            qk(tn, u)
            if u > 0:
                pv(t, u - 1)
        pv(t, units - 1)
    loop(npair, row_pair, 4)

    def finish(t):
        s0 = t * 2
        mv = jnp.concatenate([m_ref[s0].astype(F32), m_ref[s0 + 1].astype(F32)], axis=1)
        y = (gbuf[t] * obuf[t]).astype(BF)
        m1 = (mv + dot(wot[:], y)).astype(BF)
        for s in range(2):
            m1_ref[s0 + s] = m1[:, part(s, nres)]
    loop(npair, finish, 16)

    def renorm(t, acc):
        s0 = t * 2
        m1 = jnp.concatenate([m1_ref[s0].astype(F32), m1_ref[s0 + 1].astype(F32)], axis=1)
        x2 = norm(m1, 0)
        for s in range(2):
            sl = part(s, nres)
            x2_ref[s0 + s] = x2[:, sl]
            acc = acc + mask_ref[pl.ds(base + s0 + s, 1), :].astype(F32) * x2[:, sl].astype(F32)
        return acc
    qpart[me] = lax.fori_loop(0, npair, renorm, jnp.zeros((chan, nres), F32), unroll=2)


    def qslots(dev):
        return qpart.at[dev]

    pc.to_all(qpart.at[me], qslots, ssem_q, rsem_q)

    def keyval(t):
        s0 = t * 2
        xv = jnp.concatenate([x2_ref[s0], x2_ref[s0 + 1]], axis=1)
        kvp = rnd(dot(wkv_ref[:], xv))
        g2_ref[t] = sigmoid(rnd(dot(wg2_ref[:], xv)))
        for s in range(2):
            kv[s0 + s] = kvp[:, part(s, nres)]
    loop(npair, keyval, 8)
    count = total(mask_ref[:].astype(F32)) + 1e-10
    pc.from_all(qslots, rsem_q)
    tot = qpart[0]
    for d in range(1, n):
        tot = tot + qpart[d]
    tmp[:] = rnd(dot(wq2_ref[:], (tot / count).astype(BF)))
    qd = [tmp[pl.ds(d, heads, stride=hd), :] for d in range(hd)]
    unroll = 16

    def logit(t, mx):
        for u in range(unroll):
            s = t * unroll + u
            row = kv.at[s]
            l = qd[0] * row[0:1, :]
            for d in range(1, hd):
                l = l + qd[d] * row[d:d + 1, :]
            l = l * scale + (mask_ref[pl.ds(base + s, 1), :].astype(F32) - 1.0) * 1e4
            lg[s] = l
            mx = jnp.maximum(mx, l)
        return mx
    mx = lax.fori_loop(0, nseq // unroll, logit, jnp.full((heads, nres), -jnp.inf, F32))

    def weigh(t, carry):
        ssum, acc = carry
        acc = list(acc)
        for u in range(unroll):
            s = t * unroll + u
            row = kv.at[s]
            e = jnp.exp(lg[s] - mx)
            ssum = ssum + e
            eb = rnd(e)
            for d in range(hd):
                acc[d] = acc[d] + eb * row[hd + d:hd + d + 1, :]
        return ssum, tuple(acc)
    zero = jnp.zeros((heads, nres), F32)
    ssum, acc = lax.fori_loop(0, nseq // unroll, weigh, (zero, (zero,) * hd))
    ppart[me, :8, :] = mx
    ppart[me, 8:16, :] = ssum
    for d in range(hd):
        ppart[me, 16 + 8 * d:24 + 8 * d, :] = acc[d]

    def pslots(dev):
        return ppart.at[dev]

    pc.to_all(ppart.at[me], pslots, ssem_p, rsem_p)
    pc.from_all(pslots, rsem_p)
    top = ppart[0, :8, :]
    for d in range(1, n):
        top = jnp.maximum(top, ppart[d, :8, :])
    fac = [jnp.exp(ppart[d, :8, :] - top) for d in range(n)]
    den = fac[0] * ppart[0, 8:16, :]
    for d in range(1, n):
        den = den + fac[d] * ppart[d, 8:16, :]
    inv = 1.0 / den
    for c in range(hd):
        o = fac[0] * ppart[0, 16 + 8 * c:24 + 8 * c, :]
        for d in range(1, n):
            o = o + fac[d] * ppart[d, 16 + 8 * c:24 + 8 * c, :]
        o2_ref[pl.ds(c, heads, stride=hd), :] = o * inv
    pc.drain()


def msa_call(n, mask, mt, z, wb, wqkvg, wo, wq2, wkv, wg2):
    nseq, chan, nres = mt.shape
    rows = z.shape[0]
    heads = wb.shape[0]
    dma = pltpu.SemaphoreType.DMA((n,))
    dma9 = pltpu.SemaphoreType.DMA((9,))
    args = [pltpu.with_memory_space_constraint(v, pltpu.HBM) for v in (z, wb, mask, mt, wqkvg, wo, wq2, wkv, wg2)]
    return pl.pallas_call(
        functools.partial(msa_kernel, n, len(args)),
        name="msa",
        out_shape=[jax.ShapeDtypeStruct((nseq, chan, nres), BF), jax.ShapeDtypeStruct((nseq // 2, chan, 2 * nres), F32),
                   jax.ShapeDtypeStruct((chan, nres), F32)],
        in_specs=[pl.BlockSpec(memory_space=pltpu.HBM)] * len(args),
        out_specs=[VM] * 3,
        scratch_shapes=[pltpu.VMEM(v.shape, v.dtype) for v in args] + [
            dma9,
            pltpu.VMEM((heads, n * rows, nres), BF),
            pltpu.VMEM((nres, heads * nres), F32),
            pltpu.VMEM((heads * (rows + 8), nres), F32),
            pltpu.VMEM((nseq, wkv.shape[0], nres), F32),
            pltpu.VMEM((nseq, heads, nres), F32),
            pltpu.VMEM((chan, chan), BF),
            pltpu.VMEM((n, chan, nres), F32),
            pltpu.VMEM((n, chan + 16, nres), F32),
            pltpu.VMEM((chan, nres), F32),
            pltpu.VMEM((nseq, chan, nres), BF),
            pltpu.VMEM((nseq // 2, chan, 2 * nres), BF),
            pltpu.VMEM((nseq, nres, nres), BF),
            pltpu.VMEM((nseq, chan, 2 * nres), BF),
            pltpu.VMEM((nseq, chan, nres), BF),
            pltpu.VMEM((nseq // 2, chan, 2 * nres), F32),
            pltpu.VMEM((heads, nres, 2 * nres), F32),
            pltpu.VMEM((heads, 8, 2 * nres), F32),
            pltpu.VMEM((heads, nres, 2 * nres), BF),
            pltpu.VMEM((heads, 8, 2 * nres), F32),
            pltpu.VMEM((nseq // 2, chan, 2 * nres), F32),
            dma, dma, dma, dma, dma, dma,
        ],
        compiler_params=pltpu.CompilerParams(vmem_limit_bytes=38 * 2 ** 20, collective_id=0, has_side_effects=True),
    )(*args)


def gate_kernel(m1_ref, g2_ref, o2_ref, wo_ref, m2_ref, x_ref, wot, m2, sem):
    nseq, chan, nres = m1_ref.shape
    wot[:] = wo_ref[:].astype(F32).T.astype(BF)
    pieces = sem.shape[0]
    size = nseq // pieces

    def gate(t):
        y = (g2_ref[t] * cat(o2_ref[:], o2_ref[:])).astype(BF)
        m = (cat(m1_ref[2 * t].astype(F32), m1_ref[2 * t + 1].astype(F32)) + dot(wot[:], y)).astype(BF)
        for s in range(2):
            m2[2 * t + s] = m[:, part(s, nres)]

    def renorm(t):
        x_ref[t] = norm(cat(m2[2 * t].astype(F32), m2[2 * t + 1].astype(F32)), 0)
    copies = []
    for p in range(pieces):
        loop(size // 2, lambda t: gate(t + p * (size // 2)), size // 2)
        piece = pl.ds(p * size, size)
        copies.append(pltpu.make_async_copy(m2.at[piece], m2_ref.at[piece], sem.at[p]))
        copies[-1].start()
    loop(nseq // 2, renorm, 2)
    for cp in copies:
        cp.wait()


def gate_call(m1, g2, o2, wo):
    nseq, chan, nres = m1.shape
    return pl.pallas_call(
        gate_kernel,
        name="gate",
        out_shape=[jax.ShapeDtypeStruct(m1.shape, BF), jax.ShapeDtypeStruct(g2.shape, BF)],
        in_specs=[VM] * 4,
        out_specs=[pl.BlockSpec(memory_space=pltpu.HBM), VM],
        scratch_shapes=[pltpu.VMEM((chan, chan), BF), pltpu.VMEM(m1.shape, BF), pltpu.SemaphoreType.DMA((3,))],
        compiler_params=pltpu.CompilerParams(vmem_limit_bytes=16 * 2 ** 20),
    )(m1, g2, o2, wo)


def tri_attend(pc, early, zin, wb_ref, wqkvg_ref, wo_ref, maskcol, zln, brow, ball, bias, proj, gate, flat, wot, lbuf, mbuf, pbuf, rbuf, obuf, tsend, zrecv,
               ssem_b, rsem_b, ssem_t, rsem_t):
    me = pc.me
    rows, nres, chan = zin.shape
    heads = wb_ref.shape[0]
    hd = chan // heads
    scale = hd ** -0.5
    pitch = rows + 8
    mine = ds8(me * rows, rows, 16)

    def bslot(buf):
        return lambda dev: buf.at[:, ds8(dev * rows, rows, 16), :]

    def make_bias(src, w_ref, buf, ssem, rsem):
        def bias_row(i):
            zl = norm(src[i].astype(F32), 1)
            zln[i] = zl
            brow[pl.ds(i, heads, stride=pitch), :] = dot_nt(w_ref[:], zl)
        loop(rows, bias_row, rows)
        for h in range(heads):
            buf[h, mine, :] = brow[h * pitch:h * pitch + rows, :].astype(BF)
        pc.to_all(bslot(buf)(me), bslot(buf), ssem, rsem)

    if early:
        make_bias(zin, wb_ref, ball, ssem_b, rsem_b)
    else:
        def renorm(i):
            zln[i] = norm(zin[i].astype(F32), 1)
        loop(rows, renorm, 8)
    wot[:] = wo_ref[:].astype(F32).T.astype(BF)

    def project(i):
        zl = zln[i]
        proj[i, :chan, :] = dot_nt(wqkvg_ref[:chan, :], zl).astype(BF)
        proj[i, chan:2 * chan, :] = dot_nt(zl, wqkvg_ref[chan:2 * chan, :]).astype(BF)
        proj[i, 2 * chan:, :] = dot_nt(wqkvg_ref[2 * chan:3 * chan, :], zl).astype(BF)
        gate[i] = sigmoid(rnd(dot_nt(wqkvg_ref[3 * chan:, :], zl)))
    loop(rows, project, 8)
    pc.from_all(bslot(ball), rsem_b)
    for h in range(heads):
        b = ball[h].astype(F32)
        bias[:, part(h, nres)] = ((b.T if early else b) + maskcol[:]) * LOG2E
    zero = jnp.zeros((hd, nres), BF)

    half = heads // 2
    wide = 2 * nres

    def qk(i, p, u):
        r0 = 2 * hd * p
        qa = proj[i, r0:r0 + hd, :]
        qb = proj[i, r0 + hd:r0 + 2 * hd, :]
        parts = [jnp.zeros((r0, wide), BF)] if p > 0 else []
        parts.append(jnp.concatenate([qa, zero], axis=1))
        parts.append(jnp.concatenate([zero, qb], axis=1))
        if chan - r0 - 2 * hd > 0:
            parts.append(jnp.zeros((chan - r0 - 2 * hd, wide), BF))
        l = dot(proj[i, chan:2 * chan, :], jnp.concatenate(parts, axis=0)) * (scale * LOG2E) + bias[:, part(p, wide)]
        lbuf[u] = l
        mbuf[u, 0:1, :] = peak(l)

    def ex(u):
        e = jnp.exp2(lbuf[u] - mbuf[u, 0:1, :])
        pbuf[u] = e.astype(BF)
        rbuf[u, 0:1, :] = 1.0 / total(e)

    def pv(i, p, u):
        r0 = 2 * hd * p
        o = dot(proj[i, 2 * chan + r0:2 * chan + r0 + 2 * hd, :], pbuf[u])
        obuf[i, r0:r0 + hd, :] = o[:hd, :nres] * rbuf[u, 0:1, :nres]
        obuf[i, r0 + hd:r0 + 2 * hd, :] = o[hd:, nres:] * rbuf[u, 0:1, nres:]

    units = [(i, p) for i in range(2) for p in range(half)]
    for u, (i, p) in enumerate(units):
        qk(i, p, u)

    def attend(t):
        nxt = jnp.minimum(2 * t + 2, rows - 2)
        for u, (i, p) in enumerate(units):
            ex(u)
            qk(nxt + i, p, u)
            if u > 0:
                pv(2 * t + units[u - 1][0], units[u - 1][1], u - 1)
        pv(2 * t + units[-1][0], units[-1][1], len(units) - 1)
    def finish(i):
        y = (gate[i] * obuf[i]).astype(BF)
        upd = dot(wot[:], y).T
        zn = zin[i].astype(F32) + upd
        flat[pl.ds(i, nres, stride=pitch), :] = zn
        if early:
            zin[i] = zn.astype(BF)
    hrow = rows // 2

    def tblk(h):
        return lambda dev: tsend.at[h, pl.ds(dev * rows, rows)]

    def tslot(h):
        return lambda dev: zrecv.at[:, ds8(dev * rows + h * hrow, hrow), :]

    for h in range(2):
        loop(rows // 4, lambda t: attend(t + h * (rows // 4)), 4)
        loop(hrow, lambda i: finish(i + h * hrow), 8)

        def regroup(j):
            tsend[h, j] = flat[ds8(j * pitch + h * hrow, hrow), :].astype(BF)
        loop(nres, regroup, 8)
        pc.scatter(tblk(h), tslot(h), ssem_t.at[h], rsem_t.at[h])
    for h in range(2):
        if early and h == 0:
            make_bias(zin, *early)
        zrecv[:, ds8(me * rows + h * hrow, hrow), :] = tsend[h, pl.ds(me * rows, rows)]
    for h in range(2):
        pc.scatter_wait(tslot(h), rsem_t.at[h])


def pair_kernel(n, sizes, mask_ref, x_ref, z_ref, rm_ref, wproj_ref, wopm_ref, wb1_ref, wqkvg1_ref, wo1_ref, wb2_ref, wqkvg2_ref, wo2_ref,
                zo_ref,
                ac, at, w32, wt, cbuf, asend, csend, call, apack, arel, aall, upd, osc, z1, zln, brow, ball1, ball2, bias, proj, gate, flat, wot,
                lbuf, mbuf, pbuf, rbuf, obuf, maskcol, tsend1, tsend2, zmid, zfin,
                ssem_a, rsem_a, ssem_c, rsem_c, ssem_b1, rsem_b1, ssem_t1, rsem_t1, ssem_b2, rsem_b2, ssem_t2, rsem_t2):
    pc = Place(n)
    me = pc.me
    pc.signal()
    rows, nres, chan = z_ref.shape
    nf, nseq = csend.shape[0:2]
    ne = nf
    nchunk = len(sizes)
    first = [sum(sizes[:q]) for q in range(nchunk)]
    lane = lax.broadcasted_iota(jnp.int32, (nres, nres), 1)
    pitch = ac.shape[0] // nseq
    pitch2 = at.shape[0] // nres

    def project(t):
        pr = rnd(dot(wproj_ref[:], x_ref[t]))
        for s in range(2):
            mk = mask_ref[pl.ds(me * nseq + 2 * t + s, 1), :].astype(F32)
            ac[ds8((2 * t + s) * pitch, 2 * ne), :] = pr[:, part(s, nres)] * mk
    loop(nseq // 2, project, 16)

    def cslots(q):
        def slot(lo, size):
            return lambda dev: call.at[pl.ds(first[q] + lo, size), dev, :nseq, :]
        hq = sizes[q] // 2
        return slot(0, sizes[q]), slot(0, hq), slot(hq, hq)

    def own(q):
        for f in range(first[q], first[q] + sizes[q]):
            v = ac[pl.ds(ne + f, nseq, stride=pitch), :].astype(BF)
            csend[f] = v
            call[f, me, :nseq, :] = v
        pc.spread(csend.at[pl.ds(first[q], sizes[q])], cslots(q)[0], ssem_c.at[q], rsem_c.at[q])

    def neighbours(q):
        pc.spread_relay(*cslots(q), ssem_c.at[q], rsem_c.at[q])
        if q + 2 < nchunk:
            own(q + 2)

    pc.meet()
    own(0)
    pad = jnp.zeros((nres - nseq, nres), F32)

    def plane(e):
        at[pl.ds(e, nres, stride=pitch2), :] = stack(ac[pl.ds(e, nseq, stride=pitch), :], pad).T
    loop(ne, plane, 8)
    blocks = rows * ne // nres
    per = nres // ne

    def pack(d):
        v = [stack(*[at[ds8((d * rows + b * per + u) * pitch2, ne), :] for u in range(per)]) for b in range(blocks)]
        for r in range(blocks - 1):
            asend[d, part(r, nres), :] = jnp.where(lane >= nseq, pltpu.roll(v[-1], nseq - r * (nres - nseq), 1), v[r]).astype(BF)
    loop(n, pack, 4)

    def aslot(dev):
        return apack.at[dev]

    pc.scatter(lambda dev: asend.at[dev], aslot, ssem_a, rsem_a, arel)

    own(1)
    apack[me] = asend[me]
    pc.scatter_relay(aslot, arel, ssem_a, rsem_a)
    neighbours(0)
    padz = jnp.zeros((call.shape[1], call.shape[2] - nseq, nres), BF)

    def fill(f):
        call[f, :, nseq:, :] = padz
    loop(nf, fill)
    maskcol[:] = jnp.broadcast_to((rm_ref[:].astype(F32) - 1.0) * 1e4, (nres, nres)).T
    mbf = mask_ref[:].astype(F32).astype(BF)
    cbuf[:] = lax.dot_general(mbf, mbf, (((0,), (0,)), ((), ())), preferred_element_type=F32)
    w32[:] = wopm_ref[:].astype(F32)
    for g in range(nf // per):
        wt[:, part(g, nres)] = stack(*[w32[pl.ds(g * per + u, ne, stride=nf), :] for u in range(per)]).T.astype(BF)
    neighbours(1)
    pc.scatter_wait(aslot, rsem_a)

    def unpack(d):
        last = jnp.zeros((nres, nres), F32)
        for r in range(blocks - 1):
            v = apack[d, part(r, nres), :].astype(F32)
            aall[d, part(r, nres), :] = jnp.where(lane < nseq, v, 0.0).astype(BF)
            moved = pltpu.roll(v, (r + 1) * (nres - nseq), 1)
            last = last + jnp.where((lane >= r * (nres - nseq)) & (lane < (r + 1) * (nres - nseq)), moved, 0.0)
        aall[d, part(blocks - 1, nres), :] = last.astype(BF)
    loop(n, unpack, 2)

    for q in range(nchunk):
        pc.spread_wait(*cslots(q), ssem_c.at[q], rsem_c.at[q])

        if q == nchunk - 3:
            neighbours(q + 2)

        def outer(g):
            acc = None
            f = first[q] + 2 * g
            for kk in range(n // 2):
                rhs = cat(*[stack(call[f + u, 2 * kk], call[f + u, 2 * kk + 1]) for u in range(2)])
                step = dot(cat(aall[2 * kk], aall[2 * kk + 1]), rhs)
                acc = step if acc is None else acc + step
            ob = acc.astype(BF)
            for u in range(2):
                for i in range(rows):
                    osc[i, ds8((2 * g + u) * ne, ne, 32), :] = ob[part(i, ne), part(u, nres)]
        loop(sizes[q] // 2, outer, 2)
        depth = sizes[q] * ne

        def contract(g):
            step = dot(wt[:, first[q] * ne:first[q] * ne + depth], cat(osc[2 * g, :depth, :], osc[2 * g + 1, :depth, :]))
            for u in range(2):
                v = step[:, part(u, nres)]
                upd[2 * g + u] = v if q == 0 else upd[2 * g + u] + v
        loop(rows // 2, contract, 8)
        if q + 3 < nchunk:
            neighbours(q + 2)

    def residual(i):
        u = upd[i] / (1e-3 + cbuf[pl.ds(me * rows + i, 1), :])
        z1[i] = (z_ref[i].astype(F32) + u.T).astype(BF)
    loop(rows, residual, 8)

    for early, zin, wb, wq, wo, ball, ts, zout, sems in (
            ((wb2_ref, ball2, ssem_b2, rsem_b2), z1, wb1_ref, wqkvg1_ref, wo1_ref, ball1, tsend1, zmid, (ssem_b1, rsem_b1, ssem_t1, rsem_t1)),
            (None, zmid, wb2_ref, wqkvg2_ref, wo2_ref, ball2, tsend2, zfin, (ssem_b2, rsem_b2, ssem_t2, rsem_t2))):
        tri_attend(pc, early, zin, wb, wq, wo, maskcol, zln, brow, ball, bias, proj, gate, flat, wot, lbuf, mbuf, pbuf, rbuf, obuf, ts, zout, *sems)
    zo_ref[:] = zfin[:]
    pc.drain()


def pair_call(n, mask, x, z, rm, wproj, wopm, wb1, wqkvg1, wo1, wb2, wqkvg2, wo2):
    rows, nres, chan = z.shape
    nseq = 2 * x.shape[0]
    ne = wproj.shape[0] // 2
    heads = wb1.shape[0]
    sizes = (8, 8, 4, 4, 4, 4)
    dma = pltpu.SemaphoreType.DMA((n,))
    dma9 = pltpu.SemaphoreType.DMA((9,))
    dmac = pltpu.SemaphoreType.DMA((len(sizes), 9))
    pitch = rows + 8
    vz = pltpu.VMEM((rows, nres, chan), BF)
    fz = pltpu.VMEM((rows, chan, nres), F32)
    sq = pltpu.VMEM((nres, nres), F32)
    vb = pltpu.VMEM((heads, n * rows, nres), BF)
    vt = pltpu.VMEM((2, nres, rows // 2, chan), BF)
    dma29 = pltpu.SemaphoreType.DMA((2, 9))
    apk = rows * ne * nseq // nres
    row8 = pltpu.VMEM((heads, 8, 2 * nres), F32)
    args = (mask, x, z, rm, wproj, wopm, wb1, wqkvg1, wo1, wb2, wqkvg2, wo2)
    return pl.pallas_call(
        functools.partial(pair_kernel, n, sizes),
        name="pair",
        out_shape=jax.ShapeDtypeStruct(z.shape, BF),
        in_specs=[VM] * len(args),
        out_specs=VM,
        scratch_shapes=[
            pltpu.VMEM((nseq * (2 * ne + 8), nres), F32),
            pltpu.VMEM((nres * (ne + 8), nres), F32),
            pltpu.VMEM(wopm.shape, F32),
            pltpu.VMEM(wopm.shape[::-1], BF),
            sq,
            pltpu.VMEM((n, apk, nres), BF),
            pltpu.VMEM((ne, nseq, nres), BF),
            pltpu.VMEM((ne, n, nres, nres), BF),
            pltpu.VMEM((n, apk, nres), BF),
            pltpu.VMEM((2, apk, nres), BF),
            pltpu.VMEM((n, rows * ne, nres), BF),
            fz,
            pltpu.VMEM((rows, sizes[0] * ne, nres), BF),
            vz, vz,
            pltpu.VMEM((heads * pitch, nres), F32),
            vb, vb,
            pltpu.VMEM((nres, heads * nres), F32),
            pltpu.VMEM((rows, 3 * chan, nres), BF), fz,
            pltpu.VMEM((nres * pitch, chan), F32),
            pltpu.VMEM((chan, chan), BF),
            pltpu.VMEM((heads, nres, 2 * nres), F32), row8, pltpu.VMEM((heads, nres, 2 * nres), BF), row8,
            fz, sq, vt, vt, vz, vz,
            dma9, dma9, dmac, dmac, dma, dma, dma29, dma29, dma, dma, dma29, dma29,
        ],
        compiler_params=pltpu.CompilerParams(vmem_limit_bytes=40 * 2 ** 20, collective_id=1, has_side_effects=True),
    )(*args)


def flat_t(w):
    return jnp.moveaxis(w, 0, -1).reshape(-1, w.shape[0])


def solution(mesh):
    n = mesh.shape["dap"]

    def block(msa, pair, msa_mask, res_mask, row_bias_w, row_qkvg_w, row_out_w, col_query_w, col_kv_w, col_gate_w, col_out_w,
              opm_proj_w, opm_out_w, start_bias_w, start_qkvg_w, start_out_w, end_bias_w, end_qkvg_w, end_out_w):
        nseq, nres, chan = msa.shape
        pdim = pair.shape[2]
        mt = jnp.transpose(msa, (0, 2, 1))
        m1, g2, o2 = msa_call(n, msa_mask, mt, pair, row_bias_w.T, flat_t(row_qkvg_w), row_out_w.reshape(chan, chan),
                              flat_t(col_query_w), flat_t(col_kv_w), flat_t(col_gate_w))
        m2, x3 = gate_call(m1, g2, o2, col_out_w.reshape(chan, chan))
        zo = pair_call(n, msa_mask, x3, pair, res_mask.reshape(1, nres), flat_t(opm_proj_w), opm_out_w.reshape(-1, pdim),
                       start_bias_w.T, flat_t(start_qkvg_w), start_out_w.reshape(pdim, pdim),
                       end_bias_w.T, flat_t(end_qkvg_w), end_out_w.reshape(pdim, pdim))
        return jnp.transpose(m2, (0, 2, 1)), zo

    row_spec = P(('data', 'dap'), None, None)
    in_specs = (row_spec, row_spec, P('data', None), P('data')) + (P(),) * 15
    return jax.shard_map(block, mesh=mesh, in_specs=in_specs, out_specs=(row_spec, row_spec), check_vma=False)
```
